8 devices in a mesh: dp: 1 (over z), tp: 8 (over y, x, core).
Axes of the slice: x: 2, y: 2, z: 1, core: 2. Of those that a mesh axis runs over, the one named last changes fastest.
Arguments:
- tokens: bfloat16 [8, 2048, 1536], P('dp', 'tp')
- pad_mask: int32 [8, 2048], P('dp')
- rel_table: float32 [32, 16], P(None, 'tp')
- w_query: bfloat16 [2, 1536, 1024], P(None, None, 'tp')
- w_key: bfloat16 [2, 1536, 1024], P(None, None, 'tp')
- w_value: bfloat16 [2, 1536, 1024], P(None, None, 'tp')
- w_out: bfloat16 [2, 1024, 1536], P(None, 'tp')
- w_act: bfloat16 [2, 1536, 3840], P(None, None, 'tp')
- w_lin: bfloat16 [2, 1536, 3840], P(None, None, 'tp')
- w_down: bfloat16 [2, 3840, 1536], P(None, 'tp')
- norm_attn: float32 [2, 1536], replicated
- norm_mlp: float32 [2, 1536], replicated
Outputs:
- output: bfloat16 [8, 2048, 1536], P('dp', 'tp')
All inputs are finite; a program needn't handle non-finite values.
Results may differ from the reference program's by a relative error of at most 0.02.
Values are sent between devices in bfloat16 or wider.
A program may use at most 1 GiB of HBM per device.

```python
import jax
import jax.numpy as jnp
from jax import lax

BATCH_SIZE = 8
SEQ_LEN = 2048
MODEL_DIM = 1536
NUM_HEADS = 16
HEAD_DIM = 64
FF_DIM = 3840
NUM_LAYERS = 2
NUM_BUCKETS = 32
INNER_DIM = NUM_HEADS * HEAD_DIM


def rel_bucket(offsets):
    side = jnp.where(offsets > 0, 16, 0)
    distance = jnp.minimum(jnp.abs(offsets), 128)
    limits = 64 * 2 ** jnp.arange(1, 8)
    steps = jnp.sum((distance[:, None] * distance[:, None] >= limits[None, :]).astype(jnp.int32), axis=1)
    return side + jnp.where(distance < 8, distance, 8 + steps)


def rms_norm(rows_in, gain_vec):
    rows32 = rows_in.astype(jnp.float32)
    inv_rms = lax.rsqrt(jnp.mean(rows32 * rows32, axis=-1, keepdims=True) + 1e-6)
    return (rows32 * inv_rms * gain_vec).astype(jnp.bfloat16)


def setup_inputs(seed: int = 0, part: int = 0) -> dict:
    root_key = jax.random.key(seed)
    subkeys = jax.random.split(root_key, 10)
    part_keys = jax.random.split(jax.random.fold_in(root_key, part), 3)

    def weight(rng_key, dims, fan_in, factor):
        normal_draw = jax.random.normal(rng_key, dims, jnp.float32)
        return (normal_draw * (factor * fan_in ** -0.5)).astype(jnp.bfloat16)

    tokens = jax.random.normal(part_keys[0], (BATCH_SIZE, SEQ_LEN, MODEL_DIM), jnp.float32).astype(jnp.bfloat16)
    lengths = jax.random.randint(part_keys[1], (BATCH_SIZE,), SEQ_LEN // 8, SEQ_LEN + 1)
    full_row = jax.random.randint(part_keys[2], (), 0, BATCH_SIZE)
    lengths = jnp.where(jnp.arange(BATCH_SIZE) == full_row, SEQ_LEN, lengths)
    pad_mask = (jnp.arange(SEQ_LEN)[None, :] < lengths[:, None]).astype(jnp.int32)
    attn_dims = (NUM_LAYERS, MODEL_DIM, INNER_DIM)
    ff_dims = (NUM_LAYERS, MODEL_DIM, FF_DIM)
    return {
        'tokens': tokens,
        'pad_mask': pad_mask,
        'rel_table': jax.random.normal(subkeys[0], (NUM_BUCKETS, NUM_HEADS), jnp.float32),
        'w_query': weight(subkeys[1], attn_dims, MODEL_DIM * HEAD_DIM, 2.5),
        'w_key': weight(subkeys[2], attn_dims, MODEL_DIM, 1.0),
        'w_value': weight(subkeys[3], attn_dims, MODEL_DIM, 1.0),
        'w_out': weight(subkeys[4], (NUM_LAYERS, INNER_DIM, MODEL_DIM), INNER_DIM, 1.0),
        'w_act': weight(subkeys[5], ff_dims, MODEL_DIM, 1.0),
        'w_lin': weight(subkeys[6], ff_dims, MODEL_DIM, 1.0),
        'w_down': weight(subkeys[7], (NUM_LAYERS, FF_DIM, MODEL_DIM), FF_DIM, 1.0),
        'norm_attn': jax.random.uniform(subkeys[8], (NUM_LAYERS, MODEL_DIM), jnp.float32, 0.5, 1.5),
        'norm_mlp': jax.random.uniform(subkeys[9], (NUM_LAYERS, MODEL_DIM), jnp.float32, 0.5, 1.5),
    }


def reference(tokens, pad_mask, rel_table, w_query, w_key, w_value, w_out, w_act, w_lin, w_down, norm_attn, norm_mlp):
    offsets = jnp.arange(2 * SEQ_LEN - 1) - (SEQ_LEN - 1)
    dist_table = rel_table[rel_bucket(offsets)]
    positions = jnp.arange(SEQ_LEN)
    index = positions[None, :] - positions[:, None] + (SEQ_LEN - 1)
    key_bias = jnp.where(pad_mask == 1, 0.0, -1e9).astype(jnp.float32)
    token_rows = BATCH_SIZE * SEQ_LEN

    def head_attn(operands):
        q_head, k_head, v_head, table_col = operands
        scores = jnp.einsum('bqe,bke->bqk', q_head.astype(jnp.float32), k_head.astype(jnp.float32))
        scores = scores + table_col[index][None] + key_bias[:, None, :]
        attn_probs = jax.nn.softmax(scores, axis=-1).astype(jnp.bfloat16)
        context = jnp.einsum('bqk,bke->bqe', attn_probs.astype(jnp.float32), v_head.astype(jnp.float32))
        return context.astype(jnp.bfloat16)

    def layer(residual, params):
        lay_query, lay_key, lay_value, lay_out, lay_act, lay_lin, lay_down, lay_norm1, lay_norm2 = params
        normed = rms_norm(residual, lay_norm1)

        def project(weight_mat):
            projected = jnp.dot(normed, weight_mat, preferred_element_type=jnp.float32).astype(jnp.bfloat16)
            return projected.reshape(BATCH_SIZE, SEQ_LEN, NUM_HEADS, HEAD_DIM).transpose(2, 0, 1, 3)

        context = lax.map(head_attn, (project(lay_query), project(lay_key), project(lay_value), dist_table.T))
        context = context.transpose(1, 2, 0, 3).reshape(token_rows, INNER_DIM)
        attn_out = jnp.dot(context, lay_out, preferred_element_type=jnp.float32)
        mid_resid = (residual.astype(jnp.float32) + attn_out).astype(jnp.bfloat16)
        normed_mlp = rms_norm(mid_resid, lay_norm2)
        act_proj = jnp.dot(normed_mlp, lay_act, preferred_element_type=jnp.float32)
        lin_proj = jnp.dot(normed_mlp, lay_lin, preferred_element_type=jnp.float32)
        gated = (jax.nn.gelu(act_proj, approximate=True) * lin_proj).astype(jnp.bfloat16)
        ffn_out = jnp.dot(gated, lay_down, preferred_element_type=jnp.float32)
        return (mid_resid.astype(jnp.float32) + ffn_out).astype(jnp.bfloat16), None

    stacked = (w_query, w_key, w_value, w_out, w_act, w_lin, w_down, norm_attn, norm_mlp)
    final_rows, no_out = lax.scan(layer, tokens.reshape(token_rows, MODEL_DIM), stacked)
    return final_rows.reshape(BATCH_SIZE, SEQ_LEN, MODEL_DIM)
```

```python
import functools

import jax
import jax.numpy as jnp
from jax import lax
from jax.experimental import pallas as pl
from jax.experimental.pallas import tpu as pltpu
from jax.sharding import PartitionSpec as P

LOG2E = 1.4426950408889634
S=2048; H=16; D=64; KC=256

def split3(x):
    a = x.astype(jnp.bfloat16); r = x - a.astype(jnp.float32)
    b = r.astype(jnp.bfloat16); r = r - b.astype(jnp.float32)
    return a, b, r.astype(jnp.bfloat16)

def att_kernel(q_ref, kt_ref, v_ref, ka_ref, qa_ref, f_ref, o_ref, s_ref, w_ref, m_ref, *, bq, order):
    lane = lax.broadcasted_iota(jnp.int32, (1,128), 1)
    lo_half = lane < 64
    nq = S // bq
    nsub = bq // 256
    nu = H * nq
    ones = jnp.ones((KC,128), jnp.bfloat16)
    @pl.loop(0, H)
    def _(h):
        row = f_ref[pl.ds(h,1), :]
        full = pltpu.roll(jnp.broadcast_to(row, (256,1024)), 0, 1, stride=1, stride_axis=0)
        for d in range(3):
            w_ref[h, d] = full[:, d*256:(d+1)*256]
    w_ref[0, 3] = jnp.zeros((256,256), jnp.float32)
    def qk_setup(u):
        h = u // nq; i = u % nq
        pair = h // 2; odd = h % 2
        return h, i, pair, odd
    def qaug(u):
        h, i, pair, odd = qk_setup(u)
        qv = q_ref[pl.ds(i*bq, bq), pl.ds(pl.multiple_of(pair*128,128),128)]
        q32 = qv.astype(jnp.float32) * LOG2E
        hi = q32.astype(jnp.bfloat16).astype(jnp.float32)
        lo = q32 - hi
        mine = (lane // 64) == odd
        qa = jnp.concatenate([jnp.broadcast_to(qa_ref[h, pl.ds(i*nsub+r,1), :], (256,128)) for r in range(nsub)], axis=0)
        hi = jnp.where(mine, hi, 0.0).astype(jnp.bfloat16)
        lo = jnp.where(mine, lo, qa).astype(jnp.bfloat16)
        return jnp.concatenate([hi, lo], axis=1)
    def qk_chunk(u, qv, t, slot, m):
        h, i, pair, odd = qk_setup(u)
        c = (i*nsub - 1 + t + 8) % 8
        off = pl.multiple_of(c*KC, KC)
        kp = kt_ref[pl.ds(pl.multiple_of(pair*128,128),128), pl.ds(off,KC)]
        ka = ka_ref[:, pl.ds(off,KC)]
        rowi = lax.broadcasted_iota(jnp.int32, (128,1), 0)
        sel = jnp.where((rowi // 64) == odd, kp.astype(jnp.float32), ka.astype(jnp.float32)).astype(jnp.bfloat16)
        kk = jnp.concatenate([kp, sel], axis=0)
        s = jnp.dot(qv, kk, preferred_element_type=jnp.float32)
        ms = []
        for r in range(nsub):
            sr = s[r*256:(r+1)*256]
            d = t - r
            if 0 <= d <= 2:
                qb = i*nsub + r
                valid = jnp.logical_and(qb - 1 + d >= 0, qb - 1 + d <= 7)
                w = w_ref[h, d]
                if (d == 0 and r == 0) or (d == 2 and r == nsub-1):
                    w = jnp.where(valid, w, 0.0)
                sr = sr + w
            s_ref[slot, r*256:(r+1)*256, t*KC:(t+1)*KC] = sr
            mm = jnp.maximum(sr[:, :128], sr[:, 128:])
            ms.append(mm if m is None else jnp.maximum(m[r], mm))
        return ms
    def pv_chunk(u, t, slot, mr, acc):
        h, i, pair, odd = qk_setup(u)
        c = (i*nsub - 1 + t + 8) % 8
        off = pl.multiple_of(c*KC, KC)
        p = jnp.exp2(s_ref[slot, :, t*KC:(t+1)*KC] - mr).astype(jnp.bfloat16)
        vv = jnp.concatenate([v_ref[pl.ds(off,KC), pl.ds(pl.multiple_of(pair*128,128),128)], ones], axis=1)
        a = jnp.dot(p, vv, preferred_element_type=jnp.float32)
        return a if acc is None else acc + a
    def finish_max(m, slot):
        for r in range(nsub):
            m_ref[slot, r*256:(r+1)*256] = jnp.broadcast_to(jnp.max(m[r], axis=1, keepdims=True), (256,128))
    def store(u, acc):
        h, i, pair, odd = qk_setup(u)
        out = acc[:, :128] / acc[:, 128:]
        col = pl.ds(pl.multiple_of(pair*128,128),128)
        mine = (lane // 64) == odd
        old = o_ref[pl.ds(i*bq,bq), col]
        o_ref[pl.ds(i*bq,bq), col] = jnp.where(mine, out, old.astype(jnp.float32)).astype(jnp.bfloat16)
    qv = qaug(0); m=None
    for t in range(8): m = qk_chunk(0, qv, t, 0, m)
    finish_max(m, 0)
    def body(u, slot, last=False):
        nxt = 1 - slot
        un = jnp.minimum(u+1, nu-1)
        acc = None; m = None
        mr = jnp.concatenate([m_ref[slot], m_ref[slot]], axis=1)
        qv = qaug(un)
        for kind, t in order:
            if kind == 'q': m = qk_chunk(un, qv, t, nxt, m)
            elif kind == 'm': finish_max(m, nxt)
            else: acc = pv_chunk(u, t, slot, mr, acc)
        store(u, acc)
    @pl.loop(0, nu//2)
    def _(j):
        body(2*j, 0)
        body(2*j+1, 1)

def att(q, kt, v, ka, qa, f, bq=512, order=None, vmem=60*2**20, flags=None):
    return pl.pallas_call(
        functools.partial(att_kernel, bq=bq, order=order),
        in_specs=[pl.BlockSpec(memory_space=pltpu.VMEM)]*6,
        out_specs=pl.BlockSpec(memory_space=pltpu.VMEM),
        out_shape=jax.ShapeDtypeStruct((S, H*D), jnp.bfloat16),
        scratch_shapes=[pltpu.VMEM((2,bq,S), jnp.float32), pltpu.VMEM((H,4,256,256), jnp.float32), pltpu.VMEM((2,bq,128), jnp.float32)],
        compiler_params=pltpu.CompilerParams(vmem_limit_bytes=vmem, flags=flags),
    )(q,kt,v,ka,qa,f)


def tables(pad_row, rel):
    neg = jnp.where(pad_row == 1, 0.0, -1e9).astype(jnp.float32) * LOG2E
    m3 = split3(neg)
    chunk = jnp.arange(S)//256
    rows = [ (chunk == c).astype(jnp.bfloat16) for c in range(8) for _ in range(3)] + list(m3)
    ka = jnp.stack(rows + [jnp.zeros((S,), jnp.bfloat16)]*(64-len(rows)))
    ka = jnp.concatenate([ka, ka], axis=0)
    relT = rel.T * LOG2E
    right = relT[:,31]; left = relT[:,15]
    qb = jnp.arange(8)[:,None]; cc = jnp.arange(8)[None,:]
    cst = jnp.where((cc-qb)[None] >= 2, right[:,None,None], jnp.where((cc-qb)[None] <= -2, left[:,None,None], 0.0))
    c3 = jnp.stack(split3(cst), axis=-1).reshape(16,8,24).astype(jnp.float32)
    qa = jnp.concatenate([c3, jnp.ones((16,8,3),jnp.float32), jnp.zeros((16,8,37),jnp.float32)], axis=-1)
    qa = jnp.concatenate([qa,qa],axis=-1)
    t = jnp.arange(1024); n = jnp.where(t < 768, t-256, t-1024-256)
    r = jnp.minimum(jnp.abs(n),128)
    limits = 64 * 2 ** jnp.arange(1, 8)
    steps = jnp.sum((r[:,None]*r[:,None] >= limits[None,:]).astype(jnp.int32), axis=1)
    bucket = jnp.where(n>0,16,0) + jnp.where(r<8, r, 8+steps)
    f = jnp.sum(jnp.where(bucket[None,:,None] == jnp.arange(32)[None,None,:], relT[:,None,:], 0.0), axis=-1)
    return ka, qa, f


ORDER = [x for t in range(8) for x in (('q', t), ('p', t))] + [('m', 0)]


def rms_norm(rows_in, gain_vec):
    rows32 = rows_in.astype(jnp.float32)
    inv_rms = lax.rsqrt(jnp.mean(rows32 * rows32, axis=-1, keepdims=True) + 1e-6)
    return (rows32 * inv_rms * gain_vec).astype(jnp.bfloat16)


def solution(mesh):
    col_spec = P(None, None, 'tp')
    row_spec = P(None, 'tp', None)

    def local_fn(tokens, pad_mask, rel_table, w_query, w_key, w_value, w_out, w_act, w_lin, w_down, norm_attn, norm_mlp):
        me = lax.axis_index('tp')
        x = lax.all_to_all(tokens, 'tp', split_axis=0, concat_axis=1, tiled=True)[0]
        pad_row = lax.dynamic_index_in_dim(pad_mask, me, 0, keepdims=False)
        rel = lax.all_gather(rel_table, 'tp', axis=1, tiled=True)
        ka, qa, f = tables(pad_row, rel)
        gath = []
        for l in range(2):
            t = lambda w: w[l].T
            g1 = lax.all_gather(jnp.stack([t(w_query), t(w_key), t(w_value), w_out[l]]), 'tp', axis=1, tiled=True)
            g2 = lax.all_gather(jnp.stack([t(w_act), t(w_lin), w_down[l]]), 'tp', axis=1, tiled=True)
            gath.append((g1, g2))
        f32 = jnp.float32
        for l in range(2):
            g1, g2 = gath[l]
            h = rms_norm(x, norm_attn[l])
            q = jnp.einsum('sd,nd->sn', h, g1[0], preferred_element_type=f32).astype(jnp.bfloat16)
            kt = jnp.einsum('sd,nd->ns', h, g1[1], preferred_element_type=f32).astype(jnp.bfloat16)
            v = jnp.einsum('sd,nd->sn', h, g1[2], preferred_element_type=f32).astype(jnp.bfloat16)
            c = att(q, kt, v, ka, qa, f, bq=512, order=ORDER)
            x = (x.astype(f32) + jnp.dot(c, g1[3], preferred_element_type=f32)).astype(jnp.bfloat16)
            h = rms_norm(x, norm_mlp[l])
            act = jnp.einsum('sd,fd->sf', h, g2[0], preferred_element_type=f32)
            lin = jnp.einsum('sd,fd->sf', h, g2[1], preferred_element_type=f32)
            g = (jax.nn.gelu(act, approximate=True) * lin).astype(jnp.bfloat16)
            x = (x.astype(f32) + jnp.dot(g, g2[2], preferred_element_type=f32)).astype(jnp.bfloat16)
        return lax.all_to_all(x[None], 'tp', split_axis=1, concat_axis=0, tiled=True)

    in_specs = (P('dp', 'tp', None), P('dp', None), P(None, 'tp'), col_spec, col_spec, col_spec, row_spec,
                col_spec, col_spec, row_spec, P(None, None), P(None, None))
    return jax.shard_map(local_fn, mesh=mesh, in_specs=in_specs, out_specs=P('dp', 'tp', None), check_vma=False)
```

```python
import jax
import jax.numpy as jnp
from jax import lax
from jax.experimental import pallas as pl
from jax.experimental.pallas import tpu as pltpu
from jax.sharding import PartitionSpec as P

LOG2E = 1.4426950408889634
MESH = pl.DeviceIdType.MESH
F32, BF16 = jnp.float32, jnp.bfloat16
NT = (((1,), (1,)), ((), ()))

SEQ, DM, NH, NDEV, LAYERS = 2048, 1536, 16, 8, 2
LANES = 128
HD = 64
PART = SEQ // NDEV
KC = 256
NT_K = SEQ // KC
BQ = 512
NB = SEQ // BQ
NSUB = BQ // KC
HROWS = LANES
QROWS = 3 * HROWS
SHARD = 480
FR = 96
NG = SHARD // FR
GF = NDEV * FR
NF = 3 * NG
LEAD = 5
LAG = 5
VMEM_BYTES = 67043328

SEQUENCE = []
for _l in range(LAYERS):
    SEQUENCE += [('q', 3 * _l + i) for i in range(3)] + [('o', _l)] + [('f', NF * _l + i) for i in range(NF)]
NSEQ = len(SEQUENCE)
PER = NSEQ // LAYERS
ROWS = {'q': HROWS, 'o': HROWS, 'f': FR}
EVERY = tuple(range(NDEV))
LATE = (13, 14) + tuple(range(25, 30))
O_SEQ, F_SEQ = 3, 4


def split3(x):
    a = x.astype(BF16).astype(F32)
    b = (x - a).astype(BF16).astype(F32)
    return a, b, x - a - b


def gelu(x):
    return 0.5 * x * (1.0 + jnp.tanh(0.7978845608028654 * (x + 0.044715 * (x * x * x))))


def span(start, size, unit=LANES):
    return pl.ds(pl.multiple_of(start, unit), size)


def start(cps):
    for c in cps:
        c.start()


def wait(cps):
    for c in cps:
        c.wait()


def mega_kernel(tok, pad, rel, wq, wk, wv, wo, wa, wl, wd, n1, n2,
                out, gq, go, gf, xs,
                X, U, B, W, wb, F, Fo, ka_ref, qa_ref, mx, rawq,
                near_q, near_o, near_f, far_q, far_o, far_f, mate_q, mate_o, mate_f, sent_q, sent_o, sent_f,
                ts, tr, fts, ftr, ys, yr, ls, gs, vs, ps, rl):
    me = lax.axis_index('tp')
    core, chip = me % 2, me // 2
    cx, cy = chip % 2, chip // 2
    nx = cy * 4 + (1 - cx) * 2 + core
    ny = (1 - cy) * 4 + cx * 2 + core
    nd = (1 - cy) * 4 + (1 - cx) * 2 + core

    def other(d):
        return d + 1 - 2 * (d % 2)

    mate = other(me)

    def remote(src, dst, ss, rs, dev):
        return pltpu.make_async_remote_copy(src_ref=src, dst_ref=dst, send_sem=ss, recv_sem=rs,
                                            device_id={'tp': dev}, device_id_type=MESH)

    local = pltpu.make_async_copy

    def place(kind, k, owner, r0, r):
        if kind == 'q':
            return gq.at[k // 3, pl.ds(owner * QROWS + (k % 3) * HROWS + r0, r)]
        if kind == 'o':
            return go.at[k, pl.ds(owner * HROWS + r0, r)]
        return gf.at[k, pl.ds(owner * FR + r0, r)]

    def drained(ref, sem):
        local(ref, ref, sem).wait()

    def hop(kind, k, slot):
        r = ROWS[kind]
        owner, r0, rr, dev = ((me, 0, r, nx), (me, 0, r, ny), (me, 0, r, mate), (nx, 0, r // 2, ny),
                              (ny, r // 2, r // 2, nx), (nx, 0, r, mate), (ny, 0, r, mate), (nd, 0, r, mate))[slot]
        ref = place(kind, k, owner, r0, rr)
        near, far, via, sent = {'q': (near_q, far_q, mate_q, sent_q), 'o': (near_o, far_o, mate_o, sent_o),
                                'f': (near_f, far_f, mate_f, sent_f)}[kind]
        if slot < 2:
            got = near.at[k, slot]
        elif slot in (3, 4):
            got = far.at[k // 3 if kind == 'q' else k]
        elif kind == 'q':
            got = via.at[k // 3, max(slot - 4, 0)]
        else:
            got = via.at[k // 3 if kind == 'f' else k]
        return remote(ref, ref, sent.at[k // 3 if kind != 'o' else k], got, dev)

    def send_own(kind, k):
        start(hop(kind, k, slot) for slot in EVERY[:3])

    def forward(kind, k):
        for near in EVERY[:2]:
            hop(kind, k, near).wait_recv()
            start(hop(kind, k, near + step) for step in (3, 5))

    def forward_far(kind, k):
        if kind == 'q':
            drained(gq.at[k // 3, :QROWS], far_q.at[k // 3])
            start(hop(kind, k + i, EVERY[-1]) for i in range(3))
        else:
            drained(place(kind, k, 0, 0, ROWS[kind]), (far_o if kind == 'o' else far_f).at[k])
            hop(kind, k, EVERY[-1]).start()

    def tick(s):
        forward(*SEQUENCE[s])
        if s >= O_SEQ:
            kind, k = SEQUENCE[max(s - LAG, 0)]
            if kind == 'o' or kind == 'f' and k not in LATE:
                forward_far(kind, k)
            if s + LEAD < NSEQ:
                send_own(*SEQUENCE[s + LEAD])

    def tick_f(k):
        forward('f', k)

        @pl.when(k % NF == LAG - 1)
        def _():
            forward_far('o', k // NF)

        @pl.when(k % NF >= LAG)
        def _():
            forward_far('f', k - LAG)

        @pl.when(k < LAYERS * NF - LEAD)
        def _():
            send_own('f', k + LEAD)

    REST = slice(QROWS, BQ + 3 * SHARD)

    def load_raw(l):
        cps = [local(w.at[l], rawq.at[l, i], rl.at[l, 0]) for i, w in enumerate((wq, wk, wv))]
        cps += [local(wo.at[l], B.at[l, QROWS:BQ], rl.at[l, 1])]
        return cps + [local(w.at[l], B.at[l, BQ + SHARD * i:BQ + SHARD * (i + 1)], rl.at[l, 1])
                      for i, w in enumerate((wa, wl, wd))]

    def store_own(l):
        cps = [local(B.at[l, :QROWS], gq.at[l, pl.ds(me * QROWS, QROWS)], ps.at[l, 0]),
               local(B.at[l, QROWS:BQ], go.at[l, pl.ds(me * HROWS, HROWS)], ps.at[l, 1])]
        for m in range(3):
            for g in range(NG):
                r0 = BQ + SHARD * m + FR * g
                cps.append(local(B.at[l, r0:r0 + FR], gf.at[NF * l + 3 * g + m, pl.ds(me * FR, FR)], ps.at[l, 1]))
        return cps

    barrier = pltpu.get_barrier_semaphore()
    for o in EVERY[1:]:
        pl.semaphore_signal(barrier, inc=1, device_id={'tp': (me + o) % NDEV}, device_id_type=MESH)
    stores = [store_own(l) for l in range(LAYERS)]
    for l in range(LAYERS):
        start(load_raw(l))
    pl.semaphore_wait(barrier, NDEV - 1)

    peers = [nd, other(nd), nx, other(nx), ny, other(ny), mate]
    fcp = [remote(Fo, F.at[me], fts.at[0], ftr.at[0], d) for d in peers]
    tcp = [remote(tok.at[d], X.at[pl.ds(me * PART, PART)], ts.at[0], tr.at[i], d) for i, d in enumerate(peers)]
    own_tok = local(tok.at[me], X.at[pl.ds(me * PART, PART)], vs.at[NDEV])
    start((tcp[0], tcp[4], tcp[1], tcp[6], own_tok))

    t = lax.broadcasted_iota(jnp.int32, (1, 4 * KC), 1)
    n = jnp.where(t < 3 * KC, t, t - 4 * KC) - KC
    dist = jnp.minimum(jnp.abs(n), 128)
    steps = sum((dist * dist >= 64 * 2 ** i).astype(jnp.int32) for i in range(1, 8))
    bucket = jnp.where(n > 0, 16, 0) + jnp.where(dist < 8, dist, 8 + steps)
    for h in range(2):
        row = jnp.zeros((1, 4 * KC), F32)
        for b in range(32):
            row = jnp.where(bucket == b, rel[h, b] * LOG2E, row)
        Fo[pl.ds(h, 1), :] = row
    Fo[2:, :] = jnp.zeros((NDEV - 2, 4 * KC), F32)

    for l in range(LAYERS):
        drained(rawq.at[l], rl.at[l, 0])
        for i in range(3):
            for cb in range(DM // LANES):
                at = slice(LANES * cb, LANES * (cb + 1))
                B[l, HROWS * i:HROWS * (i + 1), at] = rawq[l, i, at, :].T
        if l == 0:
            start(fcp)
            start((tcp[5], tcp[2], tcp[3]))
            F[me] = Fo[:, :]
        stores[l][0].start()
        if l == 0:
            stores[l][0].wait()
            for k in range(O_SEQ):
                send_own('q', k)
        drained(B.at[l, REST], rl.at[l, 1])
        start(stores[l][1:])

    m3 = split3(jnp.where(pad[pl.ds(me, 1), :] == 1, 0.0, -1e9).astype(F32) * LOG2E)
    rowi = lax.broadcasted_iota(jnp.int32, (LANES, 1), 0) % HD
    for c in range(NT_K):
        col = slice(c * KC, (c + 1) * KC)
        v = jnp.where(jnp.logical_and(rowi >= 3 * c, rowi < 3 * c + 3), 1.0, jnp.zeros((LANES, KC), F32))
        for p in range(3):
            v = jnp.where(rowi == 3 * NT_K + p, m3[p][:, col], v)
        ka_ref[:, col] = v.astype(BF16)

    drained(F.at[:NDEV - 1], fts.at[0])
    drained(F.at[:NDEV - 1], ftr.at[0])
    lane8 = lax.broadcasted_iota(jnp.int32, (NT_K, LANES), 1) % HD
    qrow8 = lax.broadcasted_iota(jnp.int32, (NT_K, LANES), 0)

    @pl.loop(0, NH)
    def _(h):
        row = F[h // 2, pl.ds(h % 2, 1), :]
        full = pltpu.roll(jnp.broadcast_to(row, (KC, 4 * KC)), 0, 1, stride=1, stride_axis=0)
        for d in range(3):
            W[h, d] = full[:, d * KC:(d + 1) * KC]
        left, right = split3(row[:, :1]), split3(row[:, 2 * KC:2 * KC + 1])
        v = jnp.where(lane8 - 3 * NT_K < 3, 1.0, 0.0)
        for c in range(NT_K):
            for p in range(3):
                far = jnp.where(qrow8 <= c - 2, right[p], jnp.where(qrow8 >= c + 2, left[p], 0.0))
                v = jnp.where(lane8 == 3 * c + p, far, v)
        qa_ref[h] = jnp.where(lane8 < 3 * NT_K + 3, v, 0.0)

    stores[1][0].wait()
    for l in range(LAYERS):
        drained(B.at[l, REST], ps.at[l, 1])

    def norm_rows(src, r0, rows, gain):
        @pl.loop(0, rows // HD)
        def _(i):
            r = span(r0 + i * HD, HD, HD)
            v = src[r, :].astype(F32)
            inv = lax.rsqrt(jnp.mean(v * v, axis=-1, keepdims=True) + 1e-6)
            X[r, :] = (v * inv * gain).astype(BF16)

    def save(d, i):
        r = pl.ds(d * PART, PART)
        return local(X.at[r], xs.at[r], vs.at[i])

    def q_cols(pair):
        return span(pair * LANES, LANES)

    def v_cols(pair):
        return span(1024 * (1 - pair // 4) + LANES * (pair % 4), LANES)

    def k_at(pair, key, size):
        half = SEQ // 2
        return span((key // half) * half + pair * LANES, LANES), span(BQ + key % half, size)

    def qkv_step(p, slot):
        @pl.loop(0, NB)
        def _(m):
            rows = span(m * BQ, BQ)
            res = lax.dot_general(X[rows, :], wb[slot], NT, preferred_element_type=F32)
            for o in range(2):
                pair = 2 * p + o
                q, k, v = (res[:, QROWS * o + LANES * i:QROWS * o + LANES * (i + 1)] for i in range(3))
                B[0, rows, q_cols(pair)] = q.astype(BF16)
                kr, kc = k_at(pair, m * BQ, BQ)
                B[1, kr, kc] = k.T.astype(BF16)
                B[p // 2, rows, v_cols(pair)] = v.astype(BF16)

    def qkv(l):
        order = [chip, nx // 2, ny // 2, nd // 2]
        loads = [local(gq.at[l, pl.ds(p * GF, GF)], wb.at[i % 2], ls.at[i % 2]) for i, p in enumerate(order)]

        def fetch(i):
            if i == 1:
                if l == 0:
                    for s in range(O_SEQ):
                        tick(s)
                    for s in range(O_SEQ, O_SEQ + LEAD):
                        send_own(*SEQUENCE[s])
            if l == 1 and i > 0:
                tick(PER + O_SEQ + i)
            if i == 3:
                forward_far('q', O_SEQ * l)
            drained(gq.at[l, :QROWS], mate_q.at[l, i])
            loads[i].start()

        early = (2,) if l == 0 else (1, 2, 3)
        fetch(0)
        for i, p in enumerate(order):
            loads[i].wait()
            if i + 1 in early:
                fetch(i + 1)
            qkv_step(p, i % 2)
            if i + 1 < NB and i + 1 not in early:
                fetch(i + 1)
        tick((O_SEQ, PER + F_SEQ + 3)[l])

    lane = lax.broadcasted_iota(jnp.int32, (1, LANES), 1)
    krow = lax.broadcasted_iota(jnp.int32, (LANES, 1), 0)
    NU = NH * NB
    ones = jnp.ones((KC, LANES), BF16)

    def sblock(slot, t):
        b = slot * NT_K + t
        wide = DM // KC
        return (b // wide) * BQ, (b % wide) * KC

    def parts(u):
        h = u // NB
        return h, u % NB, h // 2, h % 2

    def tile_at(i, t):
        return (i * NSUB - 1 + t + NT_K) % NT_K

    def q_operand(u):
        h, i, pair, odd = parts(u)
        q32 = B[0, span(i * BQ, BQ), q_cols(pair)].astype(F32) * LOG2E
        hi = q32.astype(BF16).astype(F32)
        mine = (lane // HD) == odd
        qa = jnp.concatenate([jnp.broadcast_to(qa_ref[h, pl.ds(i * NSUB + r, 1), :], (KC, LANES)) for r in range(NSUB)])
        return jnp.concatenate([jnp.where(mine, hi, 0.0).astype(BF16), jnp.where(mine, q32 - hi, qa).astype(BF16)], axis=1)

    def score_tile(u, qv, t, slot, m):
        h, i, pair, odd = parts(u)
        c = tile_at(i, t)
        kr, kc = k_at(pair, c * KC, KC)
        kp = B[1, kr, kc]
        kx = ka_ref[:, span(c * KC, KC)]
        sel = jnp.where((krow // HD) == odd, kp.astype(F32), kx.astype(F32)).astype(BF16)
        s = jnp.dot(qv, jnp.concatenate([kp, sel]), preferred_element_type=F32)
        r0, c0 = sblock(slot, t)
        ms = []
        for r in range(NSUB):
            sr = s[r * KC:(r + 1) * KC]
            d = t - r
            if 0 <= d < 3:
                w = W[h, d]
                if (d, r) in ((0, 0), (2, NSUB - 1)):
                    at = i * NSUB + r - 1 + d
                    w = jnp.where(jnp.logical_and(at >= 0, at < NT_K), w, 0.0)
                sr = sr + w
            U[r0 + r * KC:r0 + (r + 1) * KC, c0:c0 + KC] = sr
            mm = jnp.maximum(sr[:, :LANES], sr[:, LANES:])
            ms.append(jnp.maximum(m[r], mm) if m else mm)
        return ms

    def value_tile(u, t, slot, mr, acc):
        h, i, pair, odd = parts(u)
        r0, c0 = sblock(slot, t)
        p = jnp.exp2(U[r0:r0 + BQ, c0:c0 + KC] - mr).astype(BF16)
        v = B[pair // 4, span(tile_at(i, t) * KC, KC), v_cols(pair)]
        a = jnp.dot(p, jnp.concatenate([v, ones], axis=1), preferred_element_type=F32)
        return a if t == 0 else acc + a

    def row_max(m, slot):
        for r in range(NSUB):
            mx[slot, r * KC:(r + 1) * KC] = jnp.broadcast_to(jnp.max(m[r], axis=1, keepdims=True), (KC, LANES))

    def context(u, acc):
        h, i, pair, odd = parts(u)
        rows, col = span(i * BQ, BQ), q_cols(pair)
        res = acc[:, :LANES] / acc[:, LANES:]
        B[0, rows, col] = jnp.where((lane // HD) == odd, res, B[0, rows, col].astype(F32)).astype(BF16)

    def unit(u, slot):
        nxt = 1 - slot
        un = jnp.minimum(u + 1, NU - 1)
        acc, m = (), ()
        mr = jnp.concatenate([mx[slot], mx[slot]], axis=1)
        qv = q_operand(un)
        for t in range(NT_K):
            m = score_tile(un, qv, t, nxt, m)
            acc = value_tile(u, t, slot, mr, acc)
        row_max(m, nxt)
        context(u, acc)

    def attention(l):
        qv, m = q_operand(0), ()
        for t in range(NT_K):
            m = score_tile(0, qv, t, 0, m)
        row_max(m, 0)

        @pl.loop(0, NU // 2)
        def _(j):
            @pl.when(jnp.logical_and(j % 3 == 0, j < 30))
            def _():
                tick_f((NF + F_SEQ) * l + j // 3)
            for slot in range(2):
                unit(2 * j + slot, slot)

    def out_proj(l):
        @pl.loop(0, NB)
        def _(m):
            rows = span(m * BQ, BQ)
            for nb in range(DM // BQ):
                col = slice(nb * BQ, (nb + 1) * BQ)
                y = jnp.dot(B[0, rows, :GF], wb[0, :, col], preferred_element_type=F32)
                y = y + jnp.dot(B[0, rows, GF:1024], wb[1, :KC, col], preferred_element_type=F32)
                U[rows, col] = (X[rows, col].astype(F32) + y).astype(BF16).astype(F32)

    def load_group(l, g, slot):
        k = NF * l + 3 * g
        to = (B.at[slot, :GF], B.at[slot, GF:2 * GF], wb.at[slot])
        return [local(gf.at[k + i], dst, gs.at[slot]) for i, dst in enumerate(to)]

    def loaded(slot):
        drained(gf.at[:3], gs.at[slot])

    def group_in(l, g):
        drained(gf.at[:3, :4 * FR], mate_f.at[NG * l + g])

    def ffn_step(slot, m):
        rows = span(m * BQ, BQ)
        hm = X[rows, :]
        a = lax.dot_general(hm, B[slot, :GF, :], NT, preferred_element_type=F32)
        b = lax.dot_general(hm, B[slot, GF:2 * GF, :], NT, preferred_element_type=F32)
        g = (gelu(a) * b).astype(BF16)
        U[rows, :] += jnp.dot(g, wb[slot], preferred_element_type=F32)

    def all_sent(l):
        drained(gq.at[l, :7 * QROWS], sent_q.at[l])
        drained(go.at[l, :7 * HROWS], sent_o.at[l])

        @pl.loop(NG * l, NG * (l + 1))
        def _(g):
            drained(gf.at[:3, :7 * FR], sent_f.at[g])

    def block(mi):
        return 2 * ((cy + (mi + 1) % 2) % 2) + (cx + 1 - mi // 2) % 2

    def home(mi, half):
        dev = 2 * block(mi) + half
        return remote(X.at[pl.ds(dev * PART, PART)], out.at[me], ys.at[0], yr.at[0], dev)

    def deliver(mi):
        rows = span(block(mi) * BQ, BQ)
        X[rows, :] = U[rows, :].astype(BF16)
        start(home(mi, half) for half in range(2))

    seen = [(me, own_tok), (mate, tcp[6]), (ny, tcp[4]), (other(ny), tcp[5]), (nd, tcp[0]), (other(nd), tcp[1]),
            (nx, tcp[2]), (other(nx), tcp[3])]
    back = [local(xs, X, vs.at[NDEV])]
    for l in range(LAYERS):
        gain1, gain2 = n1[pl.ds(l, 1), :], n2[pl.ds(l, 1), :]
        if l == 0:
            for i, (d, c) in enumerate(seen):
                if i == 0:
                    c.wait()
                else:
                    c.wait_recv()
                save(d, i).start()
                if i > 0:
                    e = seen[i - 1][0]
                    save(e, i - 1).wait()
                    norm_rows(X, e * PART, PART, gain1)
            save(d, i).wait()
            norm_rows(X, d * PART, PART, gain1)
        else:
            for i in EVERY:
                r = slice(i * PART, (i + 1) * PART)
                X[r, :] = U[r, :].astype(BF16)
                save(i, i).start()
            for i in EVERY:
                save(i, i).wait()
                norm_rows(X, i * PART, PART, gain1)
        qkv(l)
        start(back)
        attention(l)
        wait(back)
        drained(go.at[l, :4 * HROWS], mate_o.at[l])
        load_out = [local(go.at[l, :GF], wb.at[0], ls.at[0]), local(go.at[l, GF:], wb.at[1, :KC], ls.at[1])]
        start(load_out)
        tick((14, NSEQ - 1)[l])
        wait(load_out)
        group_in(l, 0)
        first = load_group(l, 0, 1)
        start(first[:2])
        out_proj(l)
        first[2].start()
        if l == 0:
            tick(NF)
        norm_rows(U, 0, SEQ, gain2)

        if l == 0:
            loaded(1)

            @pl.loop(0, NG * NB)
            def _(s):
                g, m = s // NB, s % NB
                for i in EVERY[:-1]:
                    @pl.when(s == (17 * i) // 6)
                    def _():
                        tick(16 + i)

                @pl.when(jnp.logical_and(m == 0, g > 0))
                def _():
                    loaded((g + 1) % 2)

                @pl.when(s == NB * (NG - 1) - 1)
                def _():
                    for k in LATE[:2]:
                        forward_far('f', k)

                @pl.when(jnp.logical_and(m == NB - 1, g < NG - 1))
                def _():
                    group_in(l, g + 1)
                    start(load_group(l, g + 1, g % 2))
                ffn_step((g + 1) % 2, m)
            all_sent(l)
            continue

        @pl.loop(0, NB * NG)
        def _(s):
            mi, g, slot = s // NG, s % NG, (s + 1) % 2
            loaded(slot)

            @pl.when(s == 2)
            def _():
                for k in LATE[2:4]:
                    forward_far('f', k)

            @pl.when(s == 3)
            def _():
                for k in LATE[4:]:
                    forward_far('f', k)

            @pl.when(s < NG - 1)
            def _():
                group_in(l, g + 1)

            @pl.when(s < NB * NG - 1)
            def _():
                start(load_group(l, (g + 1) % NG, 1 - slot))
            ffn_step(slot, block(mi))

            @pl.when(s == NG)
            def _():
                all_sent(l)

            @pl.when(jnp.logical_and(g == NG - 1, mi < NB - 1))
            def _():
                deliver(mi)

    own = span(chip * BQ, BQ)
    X[own, :] = U[own, :].astype(BF16)
    to_mate = remote(X.at[pl.ds(mate * PART, PART)], out.at[me], ys.at[0], yr.at[0], mate)
    to_self = local(X.at[pl.ds(me * PART, PART)], out.at[me], vs.at[NDEV])
    start((to_mate, to_self))
    drained(tok.at[:NDEV - 1], ts.at[0])
    drained(out.at[:NDEV - 1], ys.at[0])
    drained(out.at[:NDEV - 1], yr.at[0])
    to_self.wait()


def solution(mesh):
    col_spec = P(None, None, 'tp')
    row_spec = P(None, 'tp', None)

    def local_fn(tokens, pad_mask, rel_table, w_query, w_key, w_value, w_out, w_act, w_lin, w_down, norm_attn, norm_mlp):
        hbm = pl.BlockSpec(memory_space=pltpu.MemorySpace.HBM)
        vmem = pl.BlockSpec(memory_space=pltpu.VMEM)
        sem = pltpu.SemaphoreType.DMA
        shapes = [(NDEV, PART, DM), (LAYERS, NDEV * QROWS, DM), (LAYERS, NDEV * HROWS, DM), (LAYERS * NF, GF, DM), (SEQ, DM)]
        chunks = (O_SEQ * LAYERS, LAYERS, LAYERS * NF)
        return pl.pallas_call(
            mega_kernel,
            in_specs=[hbm, vmem, pl.BlockSpec(memory_space=pltpu.SMEM)] + [hbm] * 7 + [vmem] * 2,
            out_specs=[hbm] * 5,
            out_shape=[jax.ShapeDtypeStruct(s, BF16) for s in shapes],
            scratch_shapes=[
                pltpu.VMEM((SEQ, DM), BF16), pltpu.VMEM((SEQ, DM), F32), pltpu.VMEM((2, SEQ, DM), BF16),
                pltpu.VMEM((NH, 3, KC, KC), F32), pltpu.VMEM((2, GF, DM), BF16), pltpu.VMEM((NDEV, NDEV, 4 * KC), F32),
                pltpu.VMEM((NDEV, 4 * KC), F32), pltpu.VMEM((LANES, SEQ), BF16), pltpu.VMEM((NH, NT_K, LANES), F32),
                pltpu.VMEM((2, BQ, LANES), F32), pltpu.VMEM((LAYERS, 3, DM, LANES), BF16),
            ] + [sem((n, 2)) for n in chunks] + [sem((LAYERS,)), sem((LAYERS,)), sem((LAYERS * NF,))] + [
                sem((LAYERS, 4)), sem((LAYERS,)), sem((LAYERS * NG,)), sem((LAYERS,)), sem((LAYERS,)), sem((LAYERS * NG,)),
                sem((1,)), sem((NDEV,))] + [sem((1,))] * 4 + [
                sem((2,)), sem((2,)), sem((NDEV + 1,)), sem((LAYERS, 2)), sem((LAYERS, 2))],
            compiler_params=pltpu.CompilerParams(collective_id=0, has_side_effects=True, vmem_limit_bytes=VMEM_BYTES),
        )(tokens, pad_mask, rel_table.T, w_query, w_key, w_value, w_out, jnp.swapaxes(w_act, 1, 2), jnp.swapaxes(w_lin, 1, 2),
          w_down, norm_attn, norm_mlp)[0]

    in_specs = (P('dp', 'tp', None), P('dp', None), P(None, 'tp'), col_spec, col_spec, col_spec, row_spec,
                col_spec, col_spec, row_spec, P(None, None), P(None, None))
    return jax.shard_map(local_fn, mesh=mesh, in_specs=in_specs, out_specs=P('dp', 'tp', None), check_vma=False)
```

```python
import jax
import jax.numpy as jnp
from jax import lax
from jax.experimental import pallas as pl
from jax.experimental.pallas import tpu as pltpu
from jax.sharding import PartitionSpec as P

LOG2E = 1.4426950408889634
MESH = pl.DeviceIdType.MESH
F32, BF16 = jnp.float32, jnp.bfloat16
NT = (((1,), (1,)), ((), ()))

SEQ, DM, NH, NDEV, LAYERS = 2048, 1536, 16, 8, 2
LANES = 128
HD = 64
PART = SEQ // NDEV
KC = 256
NT_K = SEQ // KC
BQ = 512
NB = SEQ // BQ
NSUB = BQ // KC
HROWS = LANES
QROWS = 3 * HROWS
SHARD = 480
FR = 96
NG = SHARD // FR
GF = NDEV * FR
NF = 3 * NG
LEAD = 5
LAG = 5
VMEM_BYTES = 67043328

SEQUENCE = []
for _l in range(LAYERS):
    SEQUENCE += [('q', 3 * _l + i) for i in range(3)] + [('o', _l)] + [('f', NF * _l + i) for i in range(NF)]
NSEQ = len(SEQUENCE)
PER = NSEQ // LAYERS
ROWS = {'q': HROWS, 'o': HROWS, 'f': FR}
EVERY = tuple(range(NDEV))
LATE = tuple(range(9, 15)) + tuple(range(25, 30))
O_SEQ, F_SEQ = 3, 4


def sent_after(s):
    held = {14: 18, 15: 18, 16: 19, 17: 20, 18: 22, 19: 22, 20: 23}
    return held.get(s, min(s + LEAD, NSEQ - 1))


def split3(x):
    a = x.astype(BF16).astype(F32)
    b = (x - a).astype(BF16).astype(F32)
    return a, b, x - a - b


def gelu(x):
    return 0.5 * x * (1.0 + jnp.tanh(0.7978845608028654 * (x + 0.044715 * (x * x * x))))


def span(start, size, unit=LANES):
    return pl.ds(pl.multiple_of(start, unit), size)


def start(cps):
    for c in cps:
        c.start()


def wait(cps):
    for c in cps:
        c.wait()


def mega_kernel(tok, pad, rel, wq, wk, wv, wo, wa, wl, wd, n1, n2,
                out, gq, go, gf, xs,
                X, U, B, W, wb, wo2, F, Fo, ka_ref, qa_ref, mx, rawq,
                near_q, near_o, near_f, far_q, far_o, far_f, mate_q, mate_o, mate_f, sent_q, sent_o, sent_f,
                ts, tr, fts, ftr, ys, yr, ls, gs, vs, ps, rl):
    me = lax.axis_index('tp')
    core, chip = me % 2, me // 2
    cx, cy = chip % 2, chip // 2
    nx = cy * 4 + (1 - cx) * 2 + core
    ny = (1 - cy) * 4 + cx * 2 + core
    nd = (1 - cy) * 4 + (1 - cx) * 2 + core

    def other(d):
        return d + 1 - 2 * (d % 2)

    mate = other(me)

    def remote(src, dst, ss, rs, dev):
        return pltpu.make_async_remote_copy(src_ref=src, dst_ref=dst, send_sem=ss, recv_sem=rs,
                                            device_id={'tp': dev}, device_id_type=MESH)

    local = pltpu.make_async_copy

    def place(kind, k, owner, r0, r):
        if kind == 'q':
            return gq.at[k // 3, pl.ds(owner * QROWS + (k % 3) * HROWS + r0, r)]
        if kind == 'o':
            return go.at[k, pl.ds(owner * HROWS + r0, r)]
        return gf.at[k, pl.ds(owner * FR + r0, r)]

    def drained(ref, sem):
        local(ref, ref, sem).wait()

    def hop(kind, k, slot):
        r = ROWS[kind]
        owner, r0, rr, dev = ((me, 0, r, nx), (me, 0, r, ny), (me, 0, r, mate), (nx, 0, r // 2, ny),
                              (ny, r // 2, r // 2, nx), (nx, 0, r, mate), (ny, 0, r, mate), (nd, 0, r, mate))[slot]
        ref = place(kind, k, owner, r0, rr)
        near, far, via, sent = {'q': (near_q, far_q, mate_q, sent_q), 'o': (near_o, far_o, mate_o, sent_o),
                                'f': (near_f, far_f, mate_f, sent_f)}[kind]
        if slot < 2:
            got = near.at[k, slot]
        elif slot in (3, 4):
            got = far.at[k // 3 if kind == 'q' else k]
        elif kind == 'q':
            got = via.at[k // 3, max(slot - 4, 0)]
        else:
            got = via.at[k // 3 + k // (LAYERS * NF - 1) if kind == 'f' else k]
        return remote(ref, ref, sent.at[k // 3 if kind != 'o' else k], got, dev)

    def send_own(kind, k):
        start(hop(kind, k, slot) for slot in EVERY[:3])

    def forward(kind, k):
        for near in EVERY[:2]:
            hop(kind, k, near).wait_recv()
            start(hop(kind, k, near + step) for step in (3, 5))

    def forward_far(kind, k):
        if kind == 'q':
            drained(gq.at[k // 3, :QROWS], far_q.at[k // 3])
            start(hop(kind, k + i, EVERY[-1]) for i in range(3))
        else:
            drained(place(kind, k, 0, 0, ROWS[kind]), (far_o if kind == 'o' else far_f).at[k])
            hop(kind, k, EVERY[-1]).start()

    def tick(s):
        forward(*SEQUENCE[s])
        if s >= O_SEQ:
            kind, k = SEQUENCE[max(s - LAG, 0)]
            if kind == 'o' or kind == 'f' and k not in LATE:
                forward_far(kind, k)
            for ahead in range(sent_after(s - 1) + 1, sent_after(s) + 1):
                send_own(*SEQUENCE[ahead])

    def tick_f(l, k):
        forward('f', k)

        @pl.when(k % NF == LAG - 1)
        def _():
            forward_far('o', k // NF)

        @pl.when(k % NF >= LAG)
        def _():
            forward_far('f', k - LAG)

        @pl.when(k < NF * (l + 1) - LEAD)
        def _():
            send_own('f', k + LEAD)

    REST = slice(QROWS, BQ + 3 * SHARD)

    def load_raw(l):
        cps = [local(w.at[l], rawq.at[l, i], rl.at[l, 0]) for i, w in enumerate((wq, wk, wv))]
        cps += [local(wo.at[l], B.at[l, QROWS:BQ], rl.at[l, 1])]
        return cps + [local(w.at[l], B.at[l, BQ + SHARD * i:BQ + SHARD * (i + 1)], rl.at[l, 1])
                      for i, w in enumerate((wa, wl, wd))]

    def store_own(l):
        cps = [local(B.at[l, :QROWS], gq.at[l, pl.ds(me * QROWS, QROWS)], ps.at[l, 0]),
               local(B.at[l, QROWS:BQ], go.at[l, pl.ds(me * HROWS, HROWS)], ps.at[l, 1])]
        for m in range(3):
            for g in range(NG):
                r0 = BQ + SHARD * m + FR * g
                cps.append(local(B.at[l, r0:r0 + FR], gf.at[NF * l + 3 * g + m, pl.ds(me * FR, FR)], ps.at[l, 1]))
        return cps

    barrier = pltpu.get_barrier_semaphore()
    for o in EVERY[1:]:
        pl.semaphore_signal(barrier, inc=1, device_id={'tp': (me + o) % NDEV}, device_id_type=MESH)
    stores = [store_own(l) for l in range(LAYERS)]
    for l in range(LAYERS):
        start(load_raw(l))
    pl.semaphore_wait(barrier, NDEV - 1)

    peers = [nd, other(nd), nx, other(nx), ny, other(ny), mate]
    fcp = [remote(Fo, F.at[me], fts.at[0], ftr.at[0], d) for d in peers]
    tcp = [remote(tok.at[d], X.at[pl.ds(me * PART, PART)], ts.at[0], tr.at[i], d) for i, d in enumerate(peers)]
    own_tok = local(tok.at[me], X.at[pl.ds(me * PART, PART)], vs.at[NDEV])
    start((*tcp[2:], own_tok))

    t = lax.broadcasted_iota(jnp.int32, (1, 4 * KC), 1)
    n = jnp.where(t < 3 * KC, t, t - 4 * KC) - KC
    dist = jnp.minimum(jnp.abs(n), 128)
    steps = sum((dist * dist >= 64 * 2 ** i).astype(jnp.int32) for i in range(1, 8))
    bucket = jnp.where(n > 0, 16, 0) + jnp.where(dist < 8, dist, 8 + steps)
    for h in range(2):
        row = jnp.zeros((1, 4 * KC), F32)
        for b in range(32):
            row = jnp.where(bucket == b, rel[h, b] * LOG2E, row)
        Fo[pl.ds(h, 1), :] = row
    Fo[2:, :] = jnp.zeros((NDEV - 2, 4 * KC), F32)

    for l in range(LAYERS):
        drained(rawq.at[l], rl.at[l, 0])
        for i in range(3):
            for cb in range(DM // LANES):
                at = slice(LANES * cb, LANES * (cb + 1))
                B[l, HROWS * i:HROWS * (i + 1), at] = rawq[l, i, at, :].T
        if l == 0:
            start(fcp)
            start(tcp[:2])
            F[me] = Fo[:, :]
        stores[l][0].start()
        if l == 0:
            stores[l][0].wait()
            for k in range(O_SEQ):
                send_own('q', k)
        drained(B.at[l, REST], rl.at[l, 1])
        start(stores[l][1:])

    m3 = split3(jnp.where(pad[pl.ds(me, 1), :] == 1, 0.0, -1e9).astype(F32) * LOG2E)
    rowi = lax.broadcasted_iota(jnp.int32, (LANES, 1), 0) % HD
    for c in range(NT_K):
        col = slice(c * KC, (c + 1) * KC)
        v = jnp.where(jnp.logical_and(rowi >= 3 * c, rowi < 3 * c + 3), 1.0, jnp.zeros((LANES, KC), F32))
        for p in range(3):
            v = jnp.where(rowi == 3 * NT_K + p, m3[p][:, col], v)
        ka_ref[:, col] = v.astype(BF16)

    drained(F.at[:NDEV - 1], fts.at[0])
    drained(F.at[:NDEV - 1], ftr.at[0])
    lane8 = lax.broadcasted_iota(jnp.int32, (NT_K, LANES), 1) % HD
    qrow8 = lax.broadcasted_iota(jnp.int32, (NT_K, LANES), 0)

    @pl.loop(0, NH)
    def _(h):
        row = F[h // 2, pl.ds(h % 2, 1), :]
        full = pltpu.roll(jnp.broadcast_to(row, (KC, 4 * KC)), 0, 1, stride=1, stride_axis=0)
        for d in range(3):
            W[h, d] = full[:, d * KC:(d + 1) * KC]
        left, right = split3(row[:, :1]), split3(row[:, 2 * KC:2 * KC + 1])
        v = jnp.where(lane8 - 3 * NT_K < 3, 1.0, 0.0)
        for c in range(NT_K):
            for p in range(3):
                far = jnp.where(qrow8 <= c - 2, right[p], jnp.where(qrow8 >= c + 2, left[p], 0.0))
                v = jnp.where(lane8 == 3 * c + p, far, v)
        qa_ref[h] = jnp.where(lane8 < 3 * NT_K + 3, v, 0.0)

    stores[1][0].wait()
    for l in range(LAYERS):
        drained(B.at[l, REST], ps.at[l, 1])

    def norm_rows(src, r0, rows, gain):
        @pl.loop(0, rows // HD)
        def _(i):
            r = span(r0 + i * HD, HD, HD)
            v = src[r, :].astype(F32)
            inv = lax.rsqrt(jnp.mean(v * v, axis=-1, keepdims=True) + 1e-6)
            X[r, :] = (v * inv * gain).astype(BF16)

    def save(d, i):
        r = pl.ds(d * PART, PART)
        return local(X.at[r], xs.at[r], vs.at[i])

    def q_cols(pair):
        return span(pair * LANES, LANES)

    def v_cols(pair):
        return span(1024 * (1 - pair // 4) + LANES * (pair % 4), LANES)

    def k_at(pair, key, size):
        half = SEQ // 2
        return span((key // half) * half + pair * LANES, LANES), span(BQ + key % half, size)

    def qkv_step(p, slot):
        @pl.loop(0, NB)
        def _(m):
            rows = span(m * BQ, BQ)
            res = lax.dot_general(X[rows, :], wb[slot], NT, preferred_element_type=F32)
            for o in range(2):
                pair = 2 * p + o
                q, k, v = (res[:, QROWS * o + LANES * i:QROWS * o + LANES * (i + 1)] for i in range(3))
                B[0, rows, q_cols(pair)] = q.astype(BF16)
                kr, kc = k_at(pair, m * BQ, BQ)
                B[1, kr, kc] = k.T.astype(BF16)
                B[p // 2, rows, v_cols(pair)] = v.astype(BF16)

    def qkv(l):
        order = [chip, nx // 2, ny // 2, nd // 2]
        loads = [local(gq.at[l, pl.ds(p * GF, GF)], wb.at[i % 2], ls.at[i % 2]) for i, p in enumerate(order)]

        def fetch(i):
            if i == 1:
                if l == 0:
                    for s in range(O_SEQ):
                        tick(s)
                    for s in range(O_SEQ, O_SEQ + LEAD):
                        send_own(*SEQUENCE[s])
            if l == 1 and i > 0:
                tick(PER + O_SEQ + i)
            if i == 3 and l == 0:
                forward_far('q', 0)
            drained(gq.at[l, :QROWS], mate_q.at[l, i])
            loads[i].start()

        early = (2,) if l == 0 else (1, 2)
        fetch(0)
        for i, p in enumerate(order):
            loads[i].wait()
            if i + 1 in early:
                fetch(i + 1)
            if i == 2 and l == 1:
                forward_far('q', O_SEQ)
            qkv_step(p, i % 2)
            if i + 1 < NB and i + 1 not in early:
                fetch(i + 1)
        tick((O_SEQ, PER + F_SEQ + 3)[l])

    lane = lax.broadcasted_iota(jnp.int32, (1, LANES), 1)
    krow = lax.broadcasted_iota(jnp.int32, (LANES, 1), 0)
    NU = NH * NB
    ones = jnp.ones((KC, LANES), BF16)

    def sblock(slot, t):
        b = slot * NT_K + t
        wide = DM // KC
        return (b // wide) * BQ, (b % wide) * KC

    def parts(u):
        h = u // NB
        return h, u % NB, h // 2, h % 2

    def tile_at(i, t):
        return (i * NSUB - 1 + t + NT_K) % NT_K

    def q_operand(u):
        h, i, pair, odd = parts(u)
        q32 = B[0, span(i * BQ, BQ), q_cols(pair)].astype(F32) * LOG2E
        hi = q32.astype(BF16).astype(F32)
        mine = (lane // HD) == odd
        qa = jnp.concatenate([jnp.broadcast_to(qa_ref[h, pl.ds(i * NSUB + r, 1), :], (KC, LANES)) for r in range(NSUB)])
        return jnp.concatenate([jnp.where(mine, hi, 0.0).astype(BF16), jnp.where(mine, q32 - hi, qa).astype(BF16)], axis=1)

    def score_tile(u, qv, t, slot, m):
        h, i, pair, odd = parts(u)
        c = tile_at(i, t)
        kr, kc = k_at(pair, c * KC, KC)
        kp = B[1, kr, kc]
        kx = ka_ref[:, span(c * KC, KC)]
        sel = jnp.where((krow // HD) == odd, kp.astype(F32), kx.astype(F32)).astype(BF16)
        s = jnp.dot(qv, jnp.concatenate([kp, sel]), preferred_element_type=F32)
        r0, c0 = sblock(slot, t)
        ms = []
        for r in range(NSUB):
            sr = s[r * KC:(r + 1) * KC]
            d = t - r
            if 0 <= d < 3:
                w = W[h, d]
                if (d, r) in ((0, 0), (2, NSUB - 1)):
                    at = i * NSUB + r - 1 + d
                    w = jnp.where(jnp.logical_and(at >= 0, at < NT_K), w, 0.0)
                sr = sr + w
            U[r0 + r * KC:r0 + (r + 1) * KC, c0:c0 + KC] = sr
            mm = jnp.maximum(sr[:, :LANES], sr[:, LANES:])
            ms.append(jnp.maximum(m[r], mm) if m else mm)
        return ms

    def value_tile(u, t, slot, mr, acc):
        h, i, pair, odd = parts(u)
        r0, c0 = sblock(slot, t)
        p = jnp.exp2(U[r0:r0 + BQ, c0:c0 + KC] - mr).astype(BF16)
        v = B[pair // 4, span(tile_at(i, t) * KC, KC), v_cols(pair)]
        a = jnp.dot(p, jnp.concatenate([v, ones], axis=1), preferred_element_type=F32)
        return a if t == 0 else acc + a

    def row_max(m, slot):
        for r in range(NSUB):
            mx[slot, r * KC:(r + 1) * KC] = jnp.broadcast_to(jnp.max(m[r], axis=1, keepdims=True), (KC, LANES))

    def context(u, acc):
        h, i, pair, odd = parts(u)
        rows, col = span(i * BQ, BQ), q_cols(pair)
        res = acc[:, :LANES] / acc[:, LANES:]
        B[0, rows, col] = jnp.where((lane // HD) == odd, res, B[0, rows, col].astype(F32)).astype(BF16)

    def unit(u, slot):
        nxt = 1 - slot
        un = jnp.minimum(u + 1, NU - 1)
        acc, m = (), ()
        mr = jnp.concatenate([mx[slot], mx[slot]], axis=1)
        qv = q_operand(un)
        for t in range(NT_K):
            m = score_tile(un, qv, t, nxt, m)
            acc = value_tile(u, t, slot, mr, acc)
        row_max(m, nxt)
        context(u, acc)

    def load_out(l):
        return [local(go.at[l, :GF], wb.at[0], ls.at[0]), local(go.at[l, GF:], wo2, ls.at[1])]

    def attention(l):
        qv, m = q_operand(0), ()
        for t in range(NT_K):
            m = score_tile(0, qv, t, 0, m)
        row_max(m, 0)

        @pl.loop(0, NU // 2)
        def _(j):
            due = jnp.logical_and(j % 3 == 0, j < 30) if l == 0 else j % 7 % 4 == 0

            @pl.when(due)
            def _():
                tick_f(l, j // 3 if l == 0 else NF + F_SEQ + (2 * j + 1) // 7)

            @pl.when(j == 30)
            def _():
                drained(go.at[l, :4 * HROWS], mate_o.at[l])
                start(load_out(l))
            for slot in range(2):
                unit(2 * j + slot, slot)

    def norm_block(m, gain, keep=False):
        for i in range(BQ // HD):
            r = span(m * BQ + i * HD, HD, HD)
            v = U[r, :]
            if keep:
                x = v.astype(BF16)
                B[m % 2, 2 * GF + i * HD:2 * GF + (i + 1) * HD, :] = x
                v = x.astype(F32)
            inv = lax.rsqrt(jnp.mean(v * v, axis=-1, keepdims=True) + 1e-6)
            X[r, :] = (v * inv * gain).astype(BF16)

    def kept(m):
        return local(B.at[m % 2, pl.ds(2 * GF, BQ)], xs.at[pl.ds(m * BQ, BQ)], vs.at[m])

    def out_block(m):
        rows = span(m * BQ, BQ)
        for nb in range(DM // BQ):
            col = slice(nb * BQ, (nb + 1) * BQ)
            y = jnp.dot(B[0, rows, :GF], wb[0, :, col], preferred_element_type=F32)
            y = y + jnp.dot(B[0, rows, GF:1024], wo2[:, col], preferred_element_type=F32)
            U[rows, col] = (X[rows, col].astype(F32) + y).astype(BF16).astype(F32)

    def out_proj(gain):
        out_block(0)

        @pl.loop(1, NB)
        def _(m):
            out_block(m)
            norm_block(m - 1, gain)

    def load_group(l, g, slot):
        k = NF * l + 3 * g
        to = (B.at[slot, :GF], B.at[slot, GF:2 * GF], wb.at[slot])
        return [local(gf.at[k + i], dst, gs.at[slot]) for i, dst in enumerate(to)]

    def loaded(slot):
        drained(gf.at[:3], gs.at[slot])

    def group_in(l, g):
        drained(gf.at[:3, :4 * FR], mate_f.at[NG * l + g])

    def gated(slot, devs):
        hm = jnp.concatenate([X[span(d * PART, PART), :] for d in devs])
        a = lax.dot_general(hm, B[slot, :GF, :], NT, preferred_element_type=F32)
        b = lax.dot_general(hm, B[slot, GF:2 * GF, :], NT, preferred_element_type=F32)
        return (gelu(a) * b).astype(BF16)

    def add_down(slot, devs, g):
        y = jnp.dot(g, wb[slot], preferred_element_type=F32)
        for i, d in enumerate(devs):
            U[span(d * PART, PART), :] += y[i * PART:(i + 1) * PART]

    def ffn_step(slot, devs):
        add_down(slot, devs, gated(slot, devs))

    def pair_of(m):
        return 2 * m, 2 * m + 1

    def all_sent(l):
        drained(gq.at[l, :7 * QROWS], sent_q.at[l])
        drained(go.at[l, :7 * HROWS], sent_o.at[l])

        @pl.loop(NG * l, NG * (l + 1))
        def _(g):
            drained(gf.at[:3, :7 * FR], sent_f.at[g])

    far_pair = pair_of(nd // 2)

    def near_pair(mi):
        mine = mi // 3
        return [(1 - mine) * (2 * (near // 2) + mi - 1) + mine * (2 * chip + i) for i, near in enumerate((nx, ny))]

    def home(d):
        return remote(X.at[pl.ds(d * PART, PART)], out.at[me], ys.at[0], yr.at[0], d)

    def deliver(devs):
        for d in devs:
            r = span(d * PART, PART)
            X[r, :] = U[r, :].astype(BF16)
        start(home(d) for d in devs)

    seen = [(me, own_tok)] + [(peers[i], tcp[i]) for i in reversed(range(NDEV - 1))]
    back = [local(xs, X, vs.at[NDEV])]
    for l in range(LAYERS):
        gain1, gain2 = n1[pl.ds(l, 1), :], n2[pl.ds(l, 1), :]
        if l == 0:
            for i, (d, c) in enumerate(seen):
                if i == 0:
                    c.wait()
                else:
                    c.wait_recv()
                save(d, i).start()
                if i > 0:
                    e = seen[i - 1][0]
                    save(e, i - 1).wait()
                    norm_rows(X, e * PART, PART, gain1)
            save(d, i).wait()
            norm_rows(X, d * PART, PART, gain1)
        else:
            kept(2).wait()
            kept(3).wait()
        qkv(l)
        start(back)
        attention(l)
        wait(back)
        wait(load_out(l))
        tick((14, NSEQ - 2)[l])
        group_in(l, 0)
        first = load_group(l, 0, 1)
        start(first)
        out_proj(gain2)
        tick((NF, NSEQ - 1)[l])
        norm_block(NB - 1, gain2)

        if l == 0:
            loaded(1)

            @pl.loop(0, NG * NB - NB + 1)
            def _(s):
                g, m = s // NB, s % NB
                for i in EVERY[:-2]:
                    @pl.when(s == 3 * i + 1)
                    def _():
                        tick(16 + i)

                @pl.when(jnp.logical_and(m == 0, g > 0))
                def _():
                    loaded((g + 1) % 2)

                for i in range(2):
                    @pl.when(s == NB * (3 + i) - 2)
                    def _():
                        for k in LATE[3 * i:3 * i + 3]:
                            forward_far('f', k)

                @pl.when(jnp.logical_and(m == NB - 1, g < NG - 1))
                def _():
                    group_in(l, g + 1)
                    start(load_group(l, g + 1, g % 2))
                ffn_step((g + 1) % 2, pair_of(m))
            tick(22)

            @pl.loop(1, NB)
            def _(m):
                @pl.when(m > 2)
                def _():
                    kept(m - 3).wait()
                ffn_step(1, pair_of(m))
                norm_block(m - 1, n1[1:, :], True)
                kept(m - 1).start()
            kept(1).wait()
            norm_block(NB - 1, n1[1:, :], True)
            kept(NB - 1).start()
            all_sent(l)
            continue

        tail = load_group(l, NG - 1, 1)

        @pl.loop(0, NG - 1)
        def _(s):
            slot = (s + 1) % 2
            loaded(slot)

            @pl.when(s == 2)
            def _():
                for k in LATE[6:-1]:
                    forward_far('f', k)

            @pl.when(s < 3)
            def _():
                group_in(l, s + 1)
                start(load_group(l, s + 1, 1 - slot))

            @pl.when(s == 3)
            def _():
                drained(gf.at[:2, :4 * FR], mate_f.at[LAYERS * NG - 1])
                start(tail[:2])
            ffn_step(slot, far_pair)

        forward_far('f', LATE[-1])
        start(load_group(l, 0, 0))
        drained(gf.at[:2], gs.at[1])
        g = gated(1, far_pair)
        drained(gf.at[0, :4 * FR], mate_f.at[LAYERS * NG])
        tail[2].start()
        tail[2].wait()
        add_down(1, far_pair, g)
        deliver(far_pair)
        all_sent(l)

        @pl.loop(NG, NB * NG)
        def _(s):
            mi, g, slot = s // NG, s % NG, (s + 1) % 2
            loaded(slot)

            @pl.when(s < NB * NG - 1)
            def _():
                start(load_group(l, (g + 1) % NG, 1 - slot))
            ffn_step(slot, near_pair(mi))

            @pl.when(jnp.logical_and(g == NG - 1, mi < NB - 1))
            def _():
                deliver(near_pair(mi))

    for d in (mate, me):
        r = span(d * PART, PART)
        X[r, :] = U[r, :].astype(BF16)
    to_mate = home(mate)
    to_self = local(X.at[pl.ds(me * PART, PART)], out.at[me], vs.at[NDEV])
    start((to_mate, to_self))
    drained(tok.at[:NDEV - 1], ts.at[0])
    drained(out.at[:NDEV - 1], ys.at[0])
    drained(out.at[:NDEV - 1], yr.at[0])
    to_self.wait()


def solution(mesh):
    col_spec = P(None, None, 'tp')
    row_spec = P(None, 'tp', None)

    def local_fn(tokens, pad_mask, rel_table, w_query, w_key, w_value, w_out, w_act, w_lin, w_down, norm_attn, norm_mlp):
        hbm = pl.BlockSpec(memory_space=pltpu.MemorySpace.HBM)
        vmem = pl.BlockSpec(memory_space=pltpu.VMEM)
        sem = pltpu.SemaphoreType.DMA
        shapes = [(NDEV, PART, DM), (LAYERS, NDEV * QROWS, DM), (LAYERS, NDEV * HROWS, DM), (LAYERS * NF, GF, DM), (SEQ, DM)]
        chunks = (O_SEQ * LAYERS, LAYERS, LAYERS * NF)
        return pl.pallas_call(
            mega_kernel,
            in_specs=[hbm, vmem, pl.BlockSpec(memory_space=pltpu.SMEM)] + [hbm] * 7 + [vmem] * 2,
            out_specs=[hbm] * 5,
            out_shape=[jax.ShapeDtypeStruct(s, BF16) for s in shapes],
            scratch_shapes=[
                pltpu.VMEM((SEQ, DM), BF16), pltpu.VMEM((SEQ, DM), F32), pltpu.VMEM((2, SEQ, DM), BF16),
                pltpu.VMEM((NH, 3, KC, KC), F32), pltpu.VMEM((2, GF, DM), BF16), pltpu.VMEM((KC, DM), BF16), pltpu.VMEM((NDEV, NDEV, 4 * KC), F32),
                pltpu.VMEM((NDEV, 4 * KC), F32), pltpu.VMEM((LANES, SEQ), BF16), pltpu.VMEM((NH, NT_K, LANES), F32),
                pltpu.VMEM((2, BQ, LANES), F32), pltpu.VMEM((LAYERS, 3, DM, LANES), BF16),
            ] + [sem((n, 2)) for n in chunks] + [sem((LAYERS,)), sem((LAYERS,)), sem((LAYERS * NF,))] + [
                sem((LAYERS, 4)), sem((LAYERS,)), sem((LAYERS * NG + 1,)), sem((LAYERS,)), sem((LAYERS,)), sem((LAYERS * NG,)),
                sem((1,)), sem((NDEV,))] + [sem((1,))] * 4 + [
                sem((2,)), sem((2,)), sem((NDEV + 1,)), sem((LAYERS, 2)), sem((LAYERS, 2))],
            compiler_params=pltpu.CompilerParams(collective_id=0, has_side_effects=True, vmem_limit_bytes=VMEM_BYTES),
        )(tokens, pad_mask, rel_table.T, w_query, w_key, w_value, w_out, jnp.swapaxes(w_act, 1, 2), jnp.swapaxes(w_lin, 1, 2),
          w_down, norm_attn, norm_mlp)[0]

    in_specs = (P('dp', 'tp', None), P('dp', None), P(None, 'tp'), col_spec, col_spec, col_spec, row_spec,
                col_spec, col_spec, row_spec, P(None, None), P(None, None))
    return jax.shard_map(local_fn, mesh=mesh, in_specs=in_specs, out_specs=P('dp', 'tp', None), check_vma=False)
```

```python
import jax
import jax.numpy as jnp
from jax import lax
from jax.experimental import pallas as pl
from jax.experimental.pallas import tpu as pltpu
from jax.sharding import PartitionSpec as P

LOG2E = 1.4426950408889634
MESH = pl.DeviceIdType.MESH
F32, BF16 = jnp.float32, jnp.bfloat16
NT = (((1,), (1,)), ((), ()))

SEQ, DM, NH, NDEV, LAYERS = 2048, 1536, 16, 8, 2
LANES = 128
HD = 64
PART = SEQ // NDEV
KC = 256
NT_K = SEQ // KC
BQ = 512
NB = SEQ // BQ
NSUB = BQ // KC
HROWS = LANES
QROWS = 3 * HROWS
SHARD = 480
FR = 96
NG = SHARD // FR
GF = NDEV * FR
NF = 3 * NG
LEAD = 5
LAG = 5
VMEM_BYTES = 67043328

SEQUENCE = []
for _l in range(LAYERS):
    SEQUENCE += [('q', 3 * _l + i) for i in range(3)] + [('o', _l)] + [('f', NF * _l + i) for i in range(NF)]
NSEQ = len(SEQUENCE)
PER = NSEQ // LAYERS
ROWS = {'q': HROWS, 'o': HROWS, 'f': FR}
EVERY = tuple(range(NDEV))
LATE = tuple(range(9, 15)) + tuple(range(25, 30))
O_SEQ, F_SEQ = 3, 4


def sent_after(s):
    held = {14: 18, 15: 18, 16: 19, 17: 20, 18: 22, 19: 22, 20: 23}
    return held.get(s, min(s + LEAD, NSEQ - 1))


def split3(x):
    a = x.astype(BF16).astype(F32)
    b = (x - a).astype(BF16).astype(F32)
    return a, b, x - a - b


def gelu(x):
    return 0.5 * x * (1.0 + jnp.tanh(0.7978845608028654 * (x + 0.044715 * (x * x * x))))


def span(start, size, unit=LANES):
    return pl.ds(pl.multiple_of(start, unit), size)


def start(cps):
    for c in cps:
        c.start()


def wait(cps):
    for c in cps:
        c.wait()


def mega_kernel(tok, pad, rel, wq, wk, wv, wo, wa, wl, wd, n1, n2,
                out, gq, go, gf, xs,
                X, U, B, W, wb, wo2, F, Fo, ka_ref, qa_ref, mx, rawq,
                near_q, near_o, near_f, far_q, far_o, far_f, mate_q, mate_o, mate_f, sent_q, sent_o, sent_f,
                ts, tr, fts, ftr, ys, yr, ls, gs, vs, ps, rl):
    me = lax.axis_index('tp')
    core, chip = me % 2, me // 2
    cx, cy = chip % 2, chip // 2
    nx = cy * 4 + (1 - cx) * 2 + core
    ny = (1 - cy) * 4 + cx * 2 + core
    nd = (1 - cy) * 4 + (1 - cx) * 2 + core

    def other(d):
        return d + 1 - 2 * (d % 2)

    mate = other(me)

    def remote(src, dst, ss, rs, dev):
        return pltpu.make_async_remote_copy(src_ref=src, dst_ref=dst, send_sem=ss, recv_sem=rs,
                                            device_id={'tp': dev}, device_id_type=MESH)

    local = pltpu.make_async_copy

    def place(kind, k, owner, r0, r):
        if kind == 'q':
            return gq.at[k // 3, pl.ds(owner * QROWS + (k % 3) * HROWS + r0, r)]
        if kind == 'o':
            return go.at[k, pl.ds(owner * HROWS + r0, r)]
        return gf.at[k, pl.ds(owner * FR + r0, r)]

    def drained(ref, sem):
        local(ref, ref, sem).wait()

    def hop(kind, k, slot):
        r = ROWS[kind]
        owner, r0, rr, dev = ((me, 0, r, nx), (me, 0, r, ny), (me, 0, r, mate), (nx, 0, r // 2, ny),
                              (ny, r // 2, r // 2, nx), (nx, 0, r, mate), (ny, 0, r, mate), (nd, 0, r, mate))[slot]
        ref = place(kind, k, owner, r0, rr)
        near, far, via, sent = {'q': (near_q, far_q, mate_q, sent_q), 'o': (near_o, far_o, mate_o, sent_o),
                                'f': (near_f, far_f, mate_f, sent_f)}[kind]
        if slot < 2:
            got = near.at[k, slot]
        elif slot in (3, 4):
            got = far.at[k // 3 if kind == 'q' else k]
        elif kind == 'q':
            got = via.at[k // 3, max(slot - 4, 0)]
        else:
            got = via.at[k // 3 + k // (LAYERS * NF - 1) if kind == 'f' else k]
        return remote(ref, ref, sent.at[k // 3 if kind != 'o' else k], got, dev)

    def send_own(kind, k):
        start(hop(kind, k, slot) for slot in EVERY[:3])

    def forward(kind, k):
        for near in EVERY[:2]:
            hop(kind, k, near).wait_recv()
            start(hop(kind, k, near + step) for step in (3, 5))

    def forward_far(kind, k):
        if kind == 'q':
            drained(gq.at[k // 3, :QROWS], far_q.at[k // 3])
            start(hop(kind, k + i, EVERY[-1]) for i in range(3))
        else:
            drained(place(kind, k, 0, 0, ROWS[kind]), (far_o if kind == 'o' else far_f).at[k])
            hop(kind, k, EVERY[-1]).start()

    def tick(s):
        forward(*SEQUENCE[s])
        if s >= O_SEQ:
            kind, k = SEQUENCE[max(s - LAG, 0)]
            if kind == 'o' or kind == 'f' and k not in LATE:
                forward_far(kind, k)
            for ahead in range(sent_after(s - 1) + 1, sent_after(s) + 1):
                send_own(*SEQUENCE[ahead])

    def tick_f(l, k):
        forward('f', k)

        @pl.when(k % NF == LAG - 1)
        def _():
            forward_far('o', k // NF)

        @pl.when(k % NF >= LAG)
        def _():
            forward_far('f', k - LAG)

        @pl.when(k < NF * (l + 1) - LEAD)
        def _():
            send_own('f', k + LEAD)

    REST = slice(QROWS, BQ + 3 * SHARD)

    def load_raw(l):
        cps = [local(w.at[l], rawq.at[l, i], rl.at[l, 0]) for i, w in enumerate((wq, wk, wv))]
        cps += [local(wo.at[l], B.at[l, QROWS:BQ], rl.at[l, 1])]
        return cps + [local(w.at[l], B.at[l, BQ + SHARD * i:BQ + SHARD * (i + 1)], rl.at[l, 1])
                      for i, w in enumerate((wa, wl, wd))]

    def store_own(l):
        cps = [local(B.at[l, :QROWS], gq.at[l, pl.ds(me * QROWS, QROWS)], ps.at[l, 0]),
               local(B.at[l, QROWS:BQ], go.at[l, pl.ds(me * HROWS, HROWS)], ps.at[l, 1])]
        for m in range(3):
            for g in range(NG):
                r0 = BQ + SHARD * m + FR * g
                cps.append(local(B.at[l, r0:r0 + FR], gf.at[NF * l + 3 * g + m, pl.ds(me * FR, FR)], ps.at[l, 1]))
        return cps

    barrier = pltpu.get_barrier_semaphore()
    for o in EVERY[1:]:
        pl.semaphore_signal(barrier, inc=1, device_id={'tp': (me + o) % NDEV}, device_id_type=MESH)
    stores = [store_own(l) for l in range(LAYERS)]
    for l in range(LAYERS):
        start(load_raw(l))
    pl.semaphore_wait(barrier, NDEV - 1)

    peers = [nd, other(nd), nx, other(nx), ny, other(ny), mate]
    fcp = [remote(Fo, F.at[me], fts.at[0], ftr.at[0], d) for d in peers]
    tcp = [remote(tok.at[d], X.at[pl.ds(me * PART, PART)], ts.at[0], tr.at[i], d) for i, d in enumerate(peers)]
    own_tok = local(tok.at[me], X.at[pl.ds(me * PART, PART)], vs.at[NDEV])
    start((*tcp[2:], own_tok))

    t = lax.broadcasted_iota(jnp.int32, (1, 4 * KC), 1)
    n = jnp.where(t < 3 * KC, t, t - 4 * KC) - KC
    dist = jnp.minimum(jnp.abs(n), 128)
    steps = sum((dist * dist >= 64 * 2 ** i).astype(jnp.int32) for i in range(1, 8))
    bucket = jnp.where(n > 0, 16, 0) + jnp.where(dist < 8, dist, 8 + steps)
    for h in range(2):
        row = jnp.zeros((1, 4 * KC), F32)
        for b in range(32):
            row = jnp.where(bucket == b, rel[h, b] * LOG2E, row)
        Fo[pl.ds(h, 1), :] = row
    Fo[2:, :] = jnp.zeros((NDEV - 2, 4 * KC), F32)

    for l in range(LAYERS):
        drained(rawq.at[l], rl.at[l, 0])
        for i in range(3):
            for cb in range(DM // LANES):
                at = slice(LANES * cb, LANES * (cb + 1))
                B[l, HROWS * i:HROWS * (i + 1), at] = rawq[l, i, at, :].T
        if l == 0:
            start(fcp)
            start(tcp[:2])
            F[me] = Fo[:, :]
        stores[l][0].start()
        if l == 0:
            stores[l][0].wait()
            for k in range(O_SEQ):
                send_own('q', k)
        drained(B.at[l, REST], rl.at[l, 1])
        start(stores[l][1:])

    m3 = split3(jnp.where(pad[pl.ds(me, 1), :] == 1, 0.0, -1e9).astype(F32) * LOG2E)
    rowi = lax.broadcasted_iota(jnp.int32, (LANES, 1), 0) % HD
    for c in range(NT_K):
        col = slice(c * KC, (c + 1) * KC)
        v = jnp.where(jnp.logical_and(rowi >= 3 * c, rowi < 3 * c + 3), 1.0, jnp.zeros((LANES, KC), F32))
        for p in range(3):
            v = jnp.where(rowi == 3 * NT_K + p, m3[p][:, col], v)
        ka_ref[:, col] = v.astype(BF16)

    drained(F.at[:NDEV - 1], fts.at[0])
    drained(F.at[:NDEV - 1], ftr.at[0])
    lane8 = lax.broadcasted_iota(jnp.int32, (NT_K, LANES), 1) % HD
    qrow8 = lax.broadcasted_iota(jnp.int32, (NT_K, LANES), 0)

    @pl.loop(0, NH)
    def _(h):
        row = F[h // 2, pl.ds(h % 2, 1), :]
        full = pltpu.roll(jnp.broadcast_to(row, (KC, 4 * KC)), 0, 1, stride=1, stride_axis=0)
        for d in range(3):
            W[h, d] = full[:, d * KC:(d + 1) * KC]
        left, right = split3(row[:, :1]), split3(row[:, 2 * KC:2 * KC + 1])
        v = jnp.where(lane8 - 3 * NT_K < 3, 1.0, 0.0)
        for c in range(NT_K):
            for p in range(3):
                far = jnp.where(qrow8 <= c - 2, right[p], jnp.where(qrow8 >= c + 2, left[p], 0.0))
                v = jnp.where(lane8 == 3 * c + p, far, v)
        qa_ref[h] = jnp.where(lane8 < 3 * NT_K + 3, v, 0.0)

    stores[1][0].wait()
    for l in range(LAYERS):
        drained(B.at[l, REST], ps.at[l, 1])

    def norm_rows(src, r0, rows, gain):
        @pl.loop(0, rows // HD)
        def _(i):
            r = span(r0 + i * HD, HD, HD)
            v = src[r, :].astype(F32)
            inv = lax.rsqrt(jnp.mean(v * v, axis=-1, keepdims=True) + 1e-6)
            X[r, :] = (v * inv * gain).astype(BF16)

    def save(d, i):
        r = pl.ds(d * PART, PART)
        return local(X.at[r], xs.at[r], vs.at[i])

    def q_cols(pair):
        return span(pair * LANES, LANES)

    def v_cols(pair):
        return span(1024 * (1 - pair // 4) + LANES * (pair % 4), LANES)

    def k_at(pair, key, size):
        half = SEQ // 2
        return span((key // half) * half + pair * LANES, LANES), span(BQ + key % half, size)

    def qkv_step(p, slot):
        @pl.loop(0, NB)
        def _(m):
            rows = span(m * BQ, BQ)
            res = lax.dot_general(X[rows, :], wb[slot], NT, preferred_element_type=F32)
            for o in range(2):
                pair = 2 * p + o
                q, k, v = (res[:, QROWS * o + LANES * i:QROWS * o + LANES * (i + 1)] for i in range(3))
                B[0, rows, q_cols(pair)] = q.astype(BF16)
                kr, kc = k_at(pair, m * BQ, BQ)
                B[1, kr, kc] = k.T.astype(BF16)
                B[p // 2, rows, v_cols(pair)] = v.astype(BF16)

    def qkv(l):
        def load(i):
            p, slot = 2 * ((cy + i // 2) % 2) + (cx + i % 2) % 2, i % 2
            return p, slot, local(gq.at[l, pl.ds(p * GF, GF)], wb.at[slot], ls.at[slot])

        def fetch(i):
            if i == 1 and l == 0:
                for s in range(O_SEQ):
                    tick(s)
                for s in range(O_SEQ, O_SEQ + LEAD):
                    send_own(*SEQUENCE[s])
            if l == 1:
                tick(PER + O_SEQ + i)
            if i == 3 and l == 0:
                forward_far('q', 0)
            drained(gq.at[l, :QROWS], mate_q.at[l, i])
            load(i)[2].start()

        drained(gq.at[l, :QROWS], mate_q.at[l, 0])
        load(0)[2].start()
        before = ({1: 2}, {0: 1, 1: 2})[l]
        after = ({0: 1, 2: 3}, {2: 3})[l]

        @pl.loop(0, NB)
        def _(i):
            p, slot, cp = load(i)
            cp.wait()
            for at, nxt in before.items():
                @pl.when(i == at)
                def _():
                    fetch(nxt)
            if l == 1:
                @pl.when(i == 2)
                def _():
                    forward_far('q', O_SEQ)
            qkv_step(p, slot)
            for at, nxt in after.items():
                @pl.when(i == at)
                def _():
                    fetch(nxt)
        tick((O_SEQ, PER + F_SEQ + 3)[l])

    lane = lax.broadcasted_iota(jnp.int32, (1, LANES), 1)
    krow = lax.broadcasted_iota(jnp.int32, (LANES, 1), 0)
    NU = NH * NB
    ones = jnp.ones((KC, LANES), BF16)

    def sblock(slot, t):
        b = slot * NT_K + t
        wide = DM // KC
        return (b // wide) * BQ, (b % wide) * KC

    def parts(u):
        h = u // NB
        return h, u % NB, h // 2, h % 2

    def tile_at(i, t):
        return (i * NSUB - 1 + t + NT_K) % NT_K

    def q_operand(u):
        h, i, pair, odd = parts(u)
        q32 = B[0, span(i * BQ, BQ), q_cols(pair)].astype(F32) * LOG2E
        hi = q32.astype(BF16).astype(F32)
        mine = (lane // HD) == odd
        qa = jnp.concatenate([jnp.broadcast_to(qa_ref[h, pl.ds(i * NSUB + r, 1), :], (KC, LANES)) for r in range(NSUB)])
        return jnp.concatenate([jnp.where(mine, hi, 0.0).astype(BF16), jnp.where(mine, q32 - hi, qa).astype(BF16)], axis=1)

    def score_tile(u, qv, t, slot, m):
        h, i, pair, odd = parts(u)
        c = tile_at(i, t)
        kr, kc = k_at(pair, c * KC, KC)
        kp = B[1, kr, kc]
        kx = ka_ref[:, span(c * KC, KC)]
        sel = jnp.where((krow // HD) == odd, kp.astype(F32), kx.astype(F32)).astype(BF16)
        s = jnp.dot(qv, jnp.concatenate([kp, sel]), preferred_element_type=F32)
        r0, c0 = sblock(slot, t)
        ms = []
        for r in range(NSUB):
            sr = s[r * KC:(r + 1) * KC]
            d = t - r
            if 0 <= d < 3:
                w = W[h, d]
                if (d, r) in ((0, 0), (2, NSUB - 1)):
                    at = i * NSUB + r - 1 + d
                    w = jnp.where(jnp.logical_and(at >= 0, at < NT_K), w, 0.0)
                sr = sr + w
            U[r0 + r * KC:r0 + (r + 1) * KC, c0:c0 + KC] = sr
            mm = jnp.maximum(sr[:, :LANES], sr[:, LANES:])
            ms.append(jnp.maximum(m[r], mm) if m else mm)
        return ms

    def value_tile(u, t, slot, mr, acc):
        h, i, pair, odd = parts(u)
        r0, c0 = sblock(slot, t)
        p = jnp.exp2(U[r0:r0 + BQ, c0:c0 + KC] - mr).astype(BF16)
        v = B[pair // 4, span(tile_at(i, t) * KC, KC), v_cols(pair)]
        a = jnp.dot(p, jnp.concatenate([v, ones], axis=1), preferred_element_type=F32)
        return a if t == 0 else acc + a

    def row_max(m, slot):
        for r in range(NSUB):
            mx[slot, r * KC:(r + 1) * KC] = jnp.broadcast_to(jnp.max(m[r], axis=1, keepdims=True), (KC, LANES))

    def context(u, acc):
        h, i, pair, odd = parts(u)
        rows, col = span(i * BQ, BQ), q_cols(pair)
        res = acc[:, :LANES] / acc[:, LANES:]
        B[0, rows, col] = jnp.where((lane // HD) == odd, res, B[0, rows, col].astype(F32)).astype(BF16)

    def unit(u, slot):
        nxt = 1 - slot
        un = jnp.minimum(u + 1, NU - 1)
        acc, m = (), ()
        mr = jnp.concatenate([mx[slot], mx[slot]], axis=1)
        qv = q_operand(un)
        for t in range(NT_K):
            m = score_tile(un, qv, t, nxt, m)
            acc = value_tile(u, t, slot, mr, acc)
        row_max(m, nxt)
        context(u, acc)

    def load_out(l):
        return [local(go.at[l, :GF], wb.at[0], ls.at[0]), local(go.at[l, GF:], wo2, ls.at[1])]

    def attention(l):
        qv, m = q_operand(0), ()
        for t in range(NT_K):
            m = score_tile(0, qv, t, 0, m)
        row_max(m, 0)

        @pl.loop(0, NU // 2)
        def _(j):
            due = jnp.logical_and(j % 3 == 0, j < 30) if l == 0 else j % 7 % 4 == 0

            @pl.when(due)
            def _():
                tick_f(l, j // 3 if l == 0 else NF + F_SEQ + (2 * j + 1) // 7)

            @pl.when(j == 30)
            def _():
                drained(go.at[l, :4 * HROWS], mate_o.at[l])
                start(load_out(l))
            for slot in range(2):
                unit(2 * j + slot, slot)

    def norm_block(m, gain, keep=False):
        for i in range(BQ // HD):
            r = span(m * BQ + i * HD, HD, HD)
            v = U[r, :]
            if keep:
                x = v.astype(BF16)
                B[m % 2, 2 * GF + i * HD:2 * GF + (i + 1) * HD, :] = x
                v = x.astype(F32)
            inv = lax.rsqrt(jnp.mean(v * v, axis=-1, keepdims=True) + 1e-6)
            X[r, :] = (v * inv * gain).astype(BF16)

    def kept(m):
        return local(B.at[m % 2, pl.ds(2 * GF, BQ)], xs.at[pl.ds(m * BQ, BQ)], vs.at[m])

    def out_block(m):
        rows = span(m * BQ, BQ)
        for nb in range(DM // BQ):
            col = slice(nb * BQ, (nb + 1) * BQ)
            y = jnp.dot(B[0, rows, :GF], wb[0, :, col], preferred_element_type=F32)
            y = y + jnp.dot(B[0, rows, GF:1024], wo2[:, col], preferred_element_type=F32)
            U[rows, col] = (X[rows, col].astype(F32) + y).astype(BF16).astype(F32)

    def out_proj(gain):
        out_block(0)

        @pl.loop(1, NB)
        def _(m):
            out_block(m)
            norm_block(m - 1, gain)

    def load_group(l, g, slot):
        k = NF * l + 3 * g
        to = (B.at[slot, :GF], B.at[slot, GF:2 * GF], wb.at[slot])
        return [local(gf.at[k + i], dst, gs.at[slot]) for i, dst in enumerate(to)]

    def loaded(slot):
        drained(gf.at[:3], gs.at[slot])

    def group_in(l, g):
        drained(gf.at[:3, :4 * FR], mate_f.at[NG * l + g])

    def gated(slot, devs):
        hm = jnp.concatenate([X[span(d * PART, PART), :] for d in devs])
        a = lax.dot_general(hm, B[slot, :GF, :], NT, preferred_element_type=F32)
        b = lax.dot_general(hm, B[slot, GF:2 * GF, :], NT, preferred_element_type=F32)
        return (gelu(a) * b).astype(BF16)

    def add_down(slot, devs, g):
        y = jnp.dot(g, wb[slot], preferred_element_type=F32)
        for i, d in enumerate(devs):
            U[span(d * PART, PART), :] += y[i * PART:(i + 1) * PART]

    def ffn_step(slot, devs):
        add_down(slot, devs, gated(slot, devs))

    def pair_of(m):
        return 2 * m, 2 * m + 1

    def all_sent(l):
        drained(gq.at[l, :7 * QROWS], sent_q.at[l])
        drained(go.at[l, :7 * HROWS], sent_o.at[l])

        @pl.loop(NG * l, NG * (l + 1))
        def _(g):
            drained(gf.at[:3, :7 * FR], sent_f.at[g])

    far_pair = pair_of(nd // 2)

    def near_pair(mi):
        mine = mi // 3
        return [(1 - mine) * (2 * (near // 2) + mi - 1) + mine * (2 * chip + i) for i, near in enumerate((nx, ny))]

    def home(d):
        return remote(X.at[pl.ds(d * PART, PART)], out.at[me], ys.at[0], yr.at[0], d)

    def deliver(devs):
        for d in devs:
            r = span(d * PART, PART)
            X[r, :] = U[r, :].astype(BF16)
        start(home(d) for d in devs)

    seen = [(me, own_tok)] + [(peers[i], tcp[i]) for i in reversed(range(NDEV - 1))]
    back = [local(xs, X, vs.at[NDEV])]
    for l in range(LAYERS):
        gain1, gain2 = n1[pl.ds(l, 1), :], n2[pl.ds(l, 1), :]
        if l == 0:
            for i, (d, c) in enumerate(seen):
                if i == 0:
                    c.wait()
                else:
                    c.wait_recv()
                save(d, i).start()
                if i > 0:
                    e = seen[i - 1][0]
                    save(e, i - 1).wait()
                    norm_rows(X, e * PART, PART, gain1)
            save(d, i).wait()
            norm_rows(X, d * PART, PART, gain1)
        else:
            kept(2).wait()
            kept(3).wait()
        qkv(l)
        start(back)
        attention(l)
        wait(back)
        wait(load_out(l))
        tick((14, NSEQ - 2)[l])
        group_in(l, 0)
        first = load_group(l, 0, 1)
        start(first)
        out_proj(gain2)
        tick((NF, NSEQ - 1)[l])
        norm_block(NB - 1, gain2)

        if l == 0:
            loaded(1)

            @pl.loop(0, NG * NB - NB + 1)
            def _(s):
                g, m = s // NB, s % NB
                for i in EVERY[:-2]:
                    @pl.when(s == 3 * i + 1)
                    def _():
                        tick(16 + i)

                @pl.when(jnp.logical_and(m == 0, g > 0))
                def _():
                    loaded((g + 1) % 2)

                for i in range(2):
                    @pl.when(s == NB * (3 + i) - 2)
                    def _():
                        for k in LATE[3 * i:3 * i + 3]:
                            forward_far('f', k)

                @pl.when(jnp.logical_and(m == NB - 1, g < NG - 1))
                def _():
                    group_in(l, g + 1)
                    start(load_group(l, g + 1, g % 2))
                ffn_step((g + 1) % 2, pair_of(m))
            tick(22)

            @pl.loop(1, NB)
            def _(m):
                @pl.when(m > 2)
                def _():
                    kept(m - 3).wait()
                ffn_step(1, pair_of(m))
                norm_block(m - 1, n1[1:, :], True)
                kept(m - 1).start()
            kept(1).wait()
            norm_block(NB - 1, n1[1:, :], True)
            kept(NB - 1).start()
            all_sent(l)
            continue

        tail = load_group(l, NG - 1, 1)

        @pl.loop(0, NG - 1)
        def _(s):
            slot = (s + 1) % 2
            loaded(slot)

            @pl.when(s == 2)
            def _():
                for k in LATE[6:-1]:
                    forward_far('f', k)

            @pl.when(s < 3)
            def _():
                group_in(l, s + 1)
                start(load_group(l, s + 1, 1 - slot))

            @pl.when(s == 3)
            def _():
                drained(gf.at[:2, :4 * FR], mate_f.at[LAYERS * NG - 1])
                start(tail[:2])
            ffn_step(slot, far_pair)

        forward_far('f', LATE[-1])
        start(load_group(l, 0, 0))
        drained(gf.at[:2], gs.at[1])
        g = gated(1, far_pair)
        drained(gf.at[0, :4 * FR], mate_f.at[LAYERS * NG])
        tail[2].start()
        tail[2].wait()
        add_down(1, far_pair, g)
        deliver(far_pair)
        all_sent(l)

        @pl.loop(NG, NB * NG)
        def _(s):
            mi, g, slot = s // NG, s % NG, (s + 1) % 2
            loaded(slot)

            @pl.when(s < NB * NG - 1)
            def _():
                start(load_group(l, (g + 1) % NG, 1 - slot))
            ffn_step(slot, near_pair(mi))

            @pl.when(jnp.logical_and(g == NG - 1, mi < NB - 1))
            def _():
                deliver(near_pair(mi))

    for d in (mate, me):
        r = span(d * PART, PART)
        X[r, :] = U[r, :].astype(BF16)
    to_mate = home(mate)
    to_self = local(X.at[pl.ds(me * PART, PART)], out.at[me], vs.at[NDEV])
    start((to_mate, to_self))
    drained(tok.at[:NDEV - 1], ts.at[0])
    drained(out.at[:NDEV - 1], ys.at[0])
    drained(out.at[:NDEV - 1], yr.at[0])
    to_self.wait()


def solution(mesh):
    col_spec = P(None, None, 'tp')
    row_spec = P(None, 'tp', None)

    def local_fn(tokens, pad_mask, rel_table, w_query, w_key, w_value, w_out, w_act, w_lin, w_down, norm_attn, norm_mlp):
        hbm = pl.BlockSpec(memory_space=pltpu.MemorySpace.HBM)
        vmem = pl.BlockSpec(memory_space=pltpu.VMEM)
        sem = pltpu.SemaphoreType.DMA
        shapes = [(NDEV, PART, DM), (LAYERS, NDEV * QROWS, DM), (LAYERS, NDEV * HROWS, DM), (LAYERS * NF, GF, DM), (SEQ, DM)]
        chunks = (O_SEQ * LAYERS, LAYERS, LAYERS * NF)
        return pl.pallas_call(
            mega_kernel,
            in_specs=[hbm, vmem, pl.BlockSpec(memory_space=pltpu.SMEM)] + [hbm] * 7 + [vmem] * 2,
            out_specs=[hbm] * 5,
            out_shape=[jax.ShapeDtypeStruct(s, BF16) for s in shapes],
            scratch_shapes=[
                pltpu.VMEM((SEQ, DM), BF16), pltpu.VMEM((SEQ, DM), F32), pltpu.VMEM((2, SEQ, DM), BF16),
                pltpu.VMEM((NH, 3, KC, KC), F32), pltpu.VMEM((2, GF, DM), BF16), pltpu.VMEM((KC, DM), BF16), pltpu.VMEM((NDEV, NDEV, 4 * KC), F32),
                pltpu.VMEM((NDEV, 4 * KC), F32), pltpu.VMEM((LANES, SEQ), BF16), pltpu.VMEM((NH, NT_K, LANES), F32),
                pltpu.VMEM((2, BQ, LANES), F32), pltpu.VMEM((LAYERS, 3, DM, LANES), BF16),
            ] + [sem((n, 2)) for n in chunks] + [sem((LAYERS,)), sem((LAYERS,)), sem((LAYERS * NF,))] + [
                sem((LAYERS, 4)), sem((LAYERS,)), sem((LAYERS * NG + 1,)), sem((LAYERS,)), sem((LAYERS,)), sem((LAYERS * NG,)),
                sem((1,)), sem((NDEV,))] + [sem((1,))] * 4 + [
                sem((2,)), sem((2,)), sem((NDEV + 1,)), sem((LAYERS, 2)), sem((LAYERS, 2))],
            compiler_params=pltpu.CompilerParams(collective_id=0, has_side_effects=True, vmem_limit_bytes=VMEM_BYTES),
        )(tokens, pad_mask, rel_table.T, w_query, w_key, w_value, w_out, jnp.swapaxes(w_act, 1, 2), jnp.swapaxes(w_lin, 1, 2),
          w_down, norm_attn, norm_mlp)[0]

    in_specs = (P('dp', 'tp', None), P('dp', None), P(None, 'tp'), col_spec, col_spec, col_spec, row_spec,
                col_spec, col_spec, row_spec, P(None, None), P(None, None))
    return jax.shard_map(local_fn, mesh=mesh, in_specs=in_specs, out_specs=P('dp', 'tp', None), check_vma=False)
```

```python
import jax
import jax.numpy as jnp
from jax import lax
from jax.experimental import pallas as pl
from jax.experimental.pallas import tpu as pltpu
from jax.sharding import PartitionSpec as P

LOG2E = 1.4426950408889634
MESH = pl.DeviceIdType.MESH
F32, BF16 = jnp.float32, jnp.bfloat16
NT = (((1,), (1,)), ((), ()))

SEQ, DM, NH, NDEV, LAYERS = 2048, 1536, 16, 8, 2
LANES = 128
HD = 64
PART = SEQ // NDEV
KC = 256
NT_K = SEQ // KC
BQ = 512
NB = SEQ // BQ
NSUB = BQ // KC
HROWS = LANES
QROWS = 3 * HROWS
SHARD = 480
FR = 96
NG = SHARD // FR
GF = NDEV * FR
NF = 3 * NG
LEAD = 5
LAG = 5
SWAP = 48
KEEP = PART - SWAP
VMEM_BYTES = 67043328

SEQUENCE = []
for _l in range(LAYERS):
    SEQUENCE += [('q', 3 * _l + i) for i in range(3)] + [('o', _l)] + [('f', NF * _l + i) for i in range(NF)]
NSEQ = len(SEQUENCE)
PER = NSEQ // LAYERS
ROWS = {'q': HROWS, 'o': HROWS, 'f': FR}
EVERY = tuple(range(NDEV))
LATE = tuple(range(9, 15)) + tuple(range(25, 30))
O_SEQ, F_SEQ = 3, 4


def sent_after(s):
    held = {14: 18, 15: 18, 16: 19, 17: 20, 18: 22, 19: 22, 20: 23}
    return held.get(s, min(s + LEAD, NSEQ - 1))


def split3(x):
    a = x.astype(BF16).astype(F32)
    b = (x - a).astype(BF16).astype(F32)
    return a, b, x - a - b


def gelu(x):
    return 0.5 * x * (1.0 + jnp.tanh(0.7978845608028654 * (x + 0.044715 * (x * x * x))))


def span(start, size, unit=LANES):
    return pl.ds(pl.multiple_of(start, unit), size)


def start(cps):
    for c in cps:
        c.start()


def wait(cps):
    for c in cps:
        c.wait()


def mega_kernel(tok, pad, rel, wq, wk, wv, wo, wa, wl, wd, n1, n2,
                out, gq, go, gf, xs,
                X, U, B, W, wb, wo2, away, here, Hx, Ux, F, Fo, ka_ref, qa_ref, mx, rawq,
                near_q, near_o, near_f, far_q, far_o, far_f, mate_q, mate_o, mate_f, sent_q, sent_o, sent_f,
                ts, tr, fts, ftr, ys, yr, ss, sr, ls, gs, vs, ps, rl):
    me = lax.axis_index('tp')
    core, chip = me % 2, me // 2
    cx, cy = chip % 2, chip // 2
    nx = cy * 4 + (1 - cx) * 2 + core
    ny = (1 - cy) * 4 + cx * 2 + core
    nd = (1 - cy) * 4 + (1 - cx) * 2 + core

    def other(d):
        return d + 1 - 2 * (d % 2)

    mate = other(me)

    def remote(src, dst, ss, rs, dev):
        return pltpu.make_async_remote_copy(src_ref=src, dst_ref=dst, send_sem=ss, recv_sem=rs,
                                            device_id={'tp': dev}, device_id_type=MESH)

    local = pltpu.make_async_copy

    def place(kind, k, owner, r0, r):
        if kind == 'q':
            return gq.at[k // 3, pl.ds(owner * QROWS + (k % 3) * HROWS + r0, r)]
        if kind == 'o':
            return go.at[k, pl.ds(owner * HROWS + r0, r)]
        return gf.at[k, pl.ds(owner * FR + r0, r)]

    def drained(ref, sem):
        local(ref, ref, sem).wait()

    def hop(kind, k, slot):
        r = ROWS[kind]
        owner, r0, rr, dev = ((me, 0, r, nx), (me, 0, r, ny), (me, 0, r, mate), (nx, 0, r // 2, ny),
                              (ny, r // 2, r // 2, nx), (nx, 0, r, mate), (ny, 0, r, mate), (nd, 0, r, mate))[slot]
        ref = place(kind, k, owner, r0, rr)
        near, far, via, sent = {'q': (near_q, far_q, mate_q, sent_q), 'o': (near_o, far_o, mate_o, sent_o),
                                'f': (near_f, far_f, mate_f, sent_f)}[kind]
        if slot < 2:
            got = near.at[k, slot]
        elif slot in (3, 4):
            got = far.at[k // 3 if kind == 'q' else k]
        elif kind == 'q':
            got = via.at[k // 3, max(slot - 4, 0)]
        else:
            got = via.at[k // 3 + k // (LAYERS * NF - 1) if kind == 'f' else k]
        return remote(ref, ref, sent.at[k // 3 if kind != 'o' else k], got, dev)

    def send_own(kind, k):
        start(hop(kind, k, slot) for slot in EVERY[:3])

    def forward(kind, k):
        for near in EVERY[:2]:
            hop(kind, k, near).wait_recv()
            start(hop(kind, k, near + step) for step in (3, 5))

    def forward_far(kind, k):
        if kind == 'q':
            drained(gq.at[k // 3, :QROWS], far_q.at[k // 3])
            start(hop(kind, k + i, EVERY[-1]) for i in range(3))
        else:
            drained(place(kind, k, 0, 0, ROWS[kind]), (far_o if kind == 'o' else far_f).at[k])
            hop(kind, k, EVERY[-1]).start()

    def tick(s):
        forward(*SEQUENCE[s])
        if s >= O_SEQ:
            kind, k = SEQUENCE[max(s - LAG, 0)]
            if kind == 'o' or kind == 'f' and k not in LATE:
                forward_far(kind, k)
            for ahead in range(sent_after(s - 1) + 1, sent_after(s) + 1):
                send_own(*SEQUENCE[ahead])

    def tick_f(l, k):
        forward('f', k)

        @pl.when(k % NF == LAG - 1)
        def _():
            forward_far('o', k // NF)

        @pl.when(k % NF >= LAG)
        def _():
            forward_far('f', k - LAG)

        @pl.when(k < NF * (l + 1) - LEAD)
        def _():
            send_own('f', k + LEAD)

    REST = slice(QROWS, BQ + 3 * SHARD)

    def load_raw(l):
        cps = [local(w.at[l], rawq.at[l, i], rl.at[l, 0]) for i, w in enumerate((wq, wk, wv))]
        cps += [local(wo.at[l], B.at[l, QROWS:BQ], rl.at[l, 1])]
        return cps + [local(w.at[l], B.at[l, BQ + SHARD * i:BQ + SHARD * (i + 1)], rl.at[l, 1])
                      for i, w in enumerate((wa, wl, wd))]

    def store_own(l):
        cps = [local(B.at[l, :QROWS], gq.at[l, pl.ds(me * QROWS, QROWS)], ps.at[l, 0]),
               local(B.at[l, QROWS:BQ], go.at[l, pl.ds(me * HROWS, HROWS)], ps.at[l, 1])]
        for m in range(3):
            for g in range(NG):
                r0 = BQ + SHARD * m + FR * g
                cps.append(local(B.at[l, r0:r0 + FR], gf.at[NF * l + 3 * g + m, pl.ds(me * FR, FR)], ps.at[l, 1]))
        return cps

    barrier = pltpu.get_barrier_semaphore()
    for o in EVERY[1:]:
        pl.semaphore_signal(barrier, inc=1, device_id={'tp': (me + o) % NDEV}, device_id_type=MESH)
    stores = [store_own(l) for l in range(LAYERS)]
    for l in range(LAYERS):
        start(load_raw(l))
    pl.semaphore_wait(barrier, NDEV - 1)

    peers = [nd, other(nd), nx, other(nx), ny, other(ny), mate]
    fcp = [remote(Fo, F.at[me], fts.at[0], ftr.at[0], d) for d in peers]
    tcp = [remote(tok.at[d], X.at[pl.ds(me * PART, PART)], ts.at[0], tr.at[i], d) for i, d in enumerate(peers)]
    own_tok = local(tok.at[me], X.at[pl.ds(me * PART, PART)], vs.at[NDEV])
    start((*tcp[2:], own_tok))

    t = lax.broadcasted_iota(jnp.int32, (1, 4 * KC), 1)
    n = jnp.where(t < 3 * KC, t, t - 4 * KC) - KC
    dist = jnp.minimum(jnp.abs(n), 128)
    steps = sum((dist * dist >= 64 * 2 ** i).astype(jnp.int32) for i in range(1, 8))
    bucket = jnp.where(n > 0, 16, 0) + jnp.where(dist < 8, dist, 8 + steps)
    for h in range(2):
        row = jnp.zeros((1, 4 * KC), F32)
        for b in range(32):
            row = jnp.where(bucket == b, rel[h, b] * LOG2E, row)
        Fo[pl.ds(h, 1), :] = row
    Fo[2:, :] = jnp.zeros((NDEV - 2, 4 * KC), F32)

    for l in range(LAYERS):
        drained(rawq.at[l], rl.at[l, 0])
        for i in range(3):
            for cb in range(DM // LANES):
                at = slice(LANES * cb, LANES * (cb + 1))
                B[l, HROWS * i:HROWS * (i + 1), at] = rawq[l, i, at, :].T
        if l == 0:
            start(fcp)
            start(tcp[:2])
            F[me] = Fo[:, :]
        stores[l][0].start()
        if l == 0:
            stores[l][0].wait()
            for k in range(O_SEQ):
                send_own('q', k)
        drained(B.at[l, REST], rl.at[l, 1])
        start(stores[l][1:])

    m3 = split3(jnp.where(pad[pl.ds(me, 1), :] == 1, 0.0, -1e9).astype(F32) * LOG2E)
    rowi = lax.broadcasted_iota(jnp.int32, (LANES, 1), 0) % HD
    for c in range(NT_K):
        col = slice(c * KC, (c + 1) * KC)
        v = jnp.where(jnp.logical_and(rowi >= 3 * c, rowi < 3 * c + 3), 1.0, jnp.zeros((LANES, KC), F32))
        for p in range(3):
            v = jnp.where(rowi == 3 * NT_K + p, m3[p][:, col], v)
        ka_ref[:, col] = v.astype(BF16)

    drained(F.at[:NDEV - 1], fts.at[0])
    drained(F.at[:NDEV - 1], ftr.at[0])
    lane8 = lax.broadcasted_iota(jnp.int32, (NT_K, LANES), 1) % HD
    qrow8 = lax.broadcasted_iota(jnp.int32, (NT_K, LANES), 0)

    @pl.loop(0, NH)
    def _(h):
        row = F[h // 2, pl.ds(h % 2, 1), :]
        full = pltpu.roll(jnp.broadcast_to(row, (KC, 4 * KC)), 0, 1, stride=1, stride_axis=0)
        for d in range(3):
            W[h, d] = full[:, d * KC:(d + 1) * KC]
        left, right = split3(row[:, :1]), split3(row[:, 2 * KC:2 * KC + 1])
        v = jnp.where(lane8 - 3 * NT_K < 3, 1.0, 0.0)
        for c in range(NT_K):
            for p in range(3):
                far = jnp.where(qrow8 <= c - 2, right[p], jnp.where(qrow8 >= c + 2, left[p], 0.0))
                v = jnp.where(lane8 == 3 * c + p, far, v)
        qa_ref[h] = jnp.where(lane8 < 3 * NT_K + 3, v, 0.0)

    stores[1][0].wait()
    for l in range(LAYERS):
        drained(B.at[l, REST], ps.at[l, 1])

    def norm_rows(src, r0, rows, gain):
        @pl.loop(0, rows // HD)
        def _(i):
            r = span(r0 + i * HD, HD, HD)
            v = src[r, :].astype(F32)
            inv = lax.rsqrt(jnp.mean(v * v, axis=-1, keepdims=True) + 1e-6)
            X[r, :] = (v * inv * gain).astype(BF16)

    def save(d, i):
        r = pl.ds(d * PART, PART)
        return local(X.at[r], xs.at[r], vs.at[i])

    def q_cols(pair):
        return span(pair * LANES, LANES)

    def v_cols(pair):
        return span(1024 * (1 - pair // 4) + LANES * (pair % 4), LANES)

    def k_at(pair, key, size):
        half = SEQ // 2
        return span((key // half) * half + pair * LANES, LANES), span(BQ + key % half, size)

    def qkv_step(p, slot):
        @pl.loop(0, NB)
        def _(m):
            rows = span(m * BQ, BQ)
            res = lax.dot_general(X[rows, :], wb[slot], NT, preferred_element_type=F32)
            for o in range(2):
                pair = 2 * p + o
                q, k, v = (res[:, QROWS * o + LANES * i:QROWS * o + LANES * (i + 1)] for i in range(3))
                B[0, rows, q_cols(pair)] = q.astype(BF16)
                kr, kc = k_at(pair, m * BQ, BQ)
                B[1, kr, kc] = k.T.astype(BF16)
                B[p // 2, rows, v_cols(pair)] = v.astype(BF16)

    def qkv(l):
        def load(i):
            p, slot = 2 * ((cy + i // 2) % 2) + (cx + i % 2) % 2, i % 2
            return p, slot, local(gq.at[l, pl.ds(p * GF, GF)], wb.at[slot], ls.at[slot])

        def fetch(i):
            if i == 1 and l == 0:
                for s in range(O_SEQ):
                    tick(s)
                for s in range(O_SEQ, O_SEQ + LEAD):
                    send_own(*SEQUENCE[s])
            if l == 1:
                tick(PER + O_SEQ + i)
            if i == 3 and l == 0:
                forward_far('q', 0)
            drained(gq.at[l, :QROWS], mate_q.at[l, i])
            load(i)[2].start()

        drained(gq.at[l, :QROWS], mate_q.at[l, 0])
        load(0)[2].start()
        before = ({1: 2}, {0: 1, 1: 2})[l]
        after = ({0: 1, 2: 3}, {2: 3})[l]

        @pl.loop(0, NB)
        def _(i):
            p, slot, cp = load(i)
            cp.wait()
            for at, nxt in before.items():
                @pl.when(i == at)
                def _():
                    fetch(nxt)
            if l == 1:
                @pl.when(i == 2)
                def _():
                    forward_far('q', O_SEQ)
            qkv_step(p, slot)
            for at, nxt in after.items():
                @pl.when(i == at)
                def _():
                    fetch(nxt)
        tick((O_SEQ, PER + F_SEQ + 3)[l])

    lane = lax.broadcasted_iota(jnp.int32, (1, LANES), 1)
    krow = lax.broadcasted_iota(jnp.int32, (LANES, 1), 0)
    NU = NH * NB
    ones = jnp.ones((KC, LANES), BF16)

    def sblock(slot, t):
        b = slot * NT_K + t
        wide = DM // KC
        return (b // wide) * BQ, (b % wide) * KC

    def parts(u):
        h = u // NB
        return h, u % NB, h // 2, h % 2

    def tile_at(i, t):
        return (i * NSUB - 1 + t + NT_K) % NT_K

    def q_operand(u):
        h, i, pair, odd = parts(u)
        q32 = B[0, span(i * BQ, BQ), q_cols(pair)].astype(F32) * LOG2E
        hi = q32.astype(BF16).astype(F32)
        mine = (lane // HD) == odd
        qa = jnp.concatenate([jnp.broadcast_to(qa_ref[h, pl.ds(i * NSUB + r, 1), :], (KC, LANES)) for r in range(NSUB)])
        return jnp.concatenate([jnp.where(mine, hi, 0.0).astype(BF16), jnp.where(mine, q32 - hi, qa).astype(BF16)], axis=1)

    def score_tile(u, qv, t, slot, m):
        h, i, pair, odd = parts(u)
        c = tile_at(i, t)
        kr, kc = k_at(pair, c * KC, KC)
        kp = B[1, kr, kc]
        kx = ka_ref[:, span(c * KC, KC)]
        sel = jnp.where((krow // HD) == odd, kp.astype(F32), kx.astype(F32)).astype(BF16)
        s = jnp.dot(qv, jnp.concatenate([kp, sel]), preferred_element_type=F32)
        r0, c0 = sblock(slot, t)
        ms = []
        for r in range(NSUB):
            sr = s[r * KC:(r + 1) * KC]
            d = t - r
            if 0 <= d < 3:
                w = W[h, d]
                if (d, r) in ((0, 0), (2, NSUB - 1)):
                    at = i * NSUB + r - 1 + d
                    w = jnp.where(jnp.logical_and(at >= 0, at < NT_K), w, 0.0)
                sr = sr + w
            U[r0 + r * KC:r0 + (r + 1) * KC, c0:c0 + KC] = sr
            mm = jnp.maximum(sr[:, :LANES], sr[:, LANES:])
            ms.append(jnp.maximum(m[r], mm) if m else mm)
        return ms

    def value_tile(u, t, slot, mr, acc):
        h, i, pair, odd = parts(u)
        r0, c0 = sblock(slot, t)
        p = jnp.exp2(U[r0:r0 + BQ, c0:c0 + KC] - mr).astype(BF16)
        v = B[pair // 4, span(tile_at(i, t) * KC, KC), v_cols(pair)]
        a = jnp.dot(p, jnp.concatenate([v, ones], axis=1), preferred_element_type=F32)
        return a if t == 0 else acc + a

    def row_max(m, slot):
        for r in range(NSUB):
            mx[slot, r * KC:(r + 1) * KC] = jnp.broadcast_to(jnp.max(m[r], axis=1, keepdims=True), (KC, LANES))

    def context(u, acc):
        h, i, pair, odd = parts(u)
        rows, col = span(i * BQ, BQ), q_cols(pair)
        res = acc[:, :LANES] / acc[:, LANES:]
        B[0, rows, col] = jnp.where((lane // HD) == odd, res, B[0, rows, col].astype(F32)).astype(BF16)

    def unit(u, slot):
        nxt = 1 - slot
        un = jnp.minimum(u + 1, NU - 1)
        acc, m = (), ()
        mr = jnp.concatenate([mx[slot], mx[slot]], axis=1)
        qv = q_operand(un)
        for t in range(NT_K):
            m = score_tile(un, qv, t, nxt, m)
            acc = value_tile(u, t, slot, mr, acc)
        row_max(m, nxt)
        context(u, acc)

    def load_out(l):
        return [local(go.at[l, :GF], wb.at[0], ls.at[0]), local(go.at[l, GF:], wo2, ls.at[1])]

    def attention(l):
        qv, m = q_operand(0), ()
        for t in range(NT_K):
            m = score_tile(0, qv, t, 0, m)
        row_max(m, 0)

        @pl.loop(0, NU // 2)
        def _(j):
            due = jnp.logical_and(j % 3 == 0, j < 30) if l == 0 else j % 7 % 4 == 0

            @pl.when(due)
            def _():
                tick_f(l, j // 3 if l == 0 else NF + F_SEQ + (2 * j + 1) // 7)

            @pl.when(j == 30)
            def _():
                drained(go.at[l, :4 * HROWS], mate_o.at[l])
                start(load_out(l))
            for slot in range(2):
                unit(2 * j + slot, slot)

    def norm_block(m, gain, keep=False):
        for i in range(BQ // HD):
            r = span(m * BQ + i * HD, HD, HD)
            v = U[r, :]
            if keep:
                x = v.astype(BF16)
                B[m % 2, 2 * GF + i * HD:2 * GF + (i + 1) * HD, :] = x
                v = x.astype(F32)
            inv = lax.rsqrt(jnp.mean(v * v, axis=-1, keepdims=True) + 1e-6)
            X[r, :] = (v * inv * gain).astype(BF16)

    def kept(m):
        return local(B.at[m % 2, pl.ds(2 * GF, BQ)], xs.at[pl.ds(m * BQ, BQ)], vs.at[m])

    def out_block(m):
        rows = span(m * BQ, BQ)
        for nb in range(DM // BQ):
            col = slice(nb * BQ, (nb + 1) * BQ)
            y = jnp.dot(B[0, rows, :GF], wb[0, :, col], preferred_element_type=F32)
            y = y + jnp.dot(B[0, rows, GF:1024], wo2[:, col], preferred_element_type=F32)
            U[rows, col] = (X[rows, col].astype(F32) + y).astype(BF16).astype(F32)

    def out_proj(gain):
        out_block(0)

        @pl.loop(1, NB)
        def _(m):
            out_block(m)
            norm_block(m - 1, gain)

    def load_group(l, g, slot):
        k = NF * l + 3 * g
        to = (B.at[slot, :GF], B.at[slot, GF:2 * GF], wb.at[slot])
        return [local(gf.at[k + i], dst, gs.at[slot]) for i, dst in enumerate(to)]

    def loaded(slot):
        drained(gf.at[:3], gs.at[slot])

    def group_in(l, g):
        drained(gf.at[:3, :4 * FR], mate_f.at[NG * l + g])

    def gated(slot, parts):
        hm = jnp.concatenate([h[r, :] for h, _, r in parts])
        a = lax.dot_general(hm, B[slot, :GF, :], NT, preferred_element_type=F32)
        b = lax.dot_general(hm, B[slot, GF:2 * GF, :], NT, preferred_element_type=F32)
        return (gelu(a) * b).astype(BF16)

    def add_down(slot, parts, g):
        y = jnp.dot(g, wb[slot], preferred_element_type=F32)
        at = 0
        for _, total, r in parts:
            total[r, :] += y[at:at + r.size]
            at += r.size

    def ffn_step(slot, parts):
        add_down(slot, parts, gated(slot, parts))

    def rows_of(devs, size=PART):
        return [(X, U, span(d * PART, size)) for d in devs]

    def pair_of(m):
        return 2 * m, 2 * m + 1

    def all_sent(l):
        drained(gq.at[l, :7 * QROWS], sent_q.at[l])
        drained(go.at[l, :7 * HROWS], sent_o.at[l])

        @pl.loop(NG * l, NG * (l + 1))
        def _(g):
            drained(gf.at[:3, :7 * FR], sent_f.at[g])

    far_pair = pair_of(nd // 2)

    def near_pair(mi):
        return [2 * (near // 2) + mi - 1 for near in (nx, ny)]

    def home(d, rows=PART):
        i = rows // PART
        return remote(X.at[pl.ds(d * PART, rows)], out.at[me, :rows], ys.at[i], yr.at[i], d)

    def deliver(devs, rows=PART):
        for d in devs:
            r = span(d * PART, rows)
            X[r, :] = U[r, :].astype(BF16)
        start(home(d, rows) for d in devs)

    seen = [(me, own_tok)] + [(peers[i], tcp[i]) for i in reversed(range(NDEV - 1))]
    back = [local(xs, X, vs.at[NDEV])]
    for l in range(LAYERS):
        gain1, gain2 = n1[pl.ds(l, 1), :], n2[pl.ds(l, 1), :]
        if l == 0:
            for i, (d, c) in enumerate(seen):
                if i == 0:
                    c.wait()
                else:
                    c.wait_recv()
                save(d, i).start()
                if i > 0:
                    e = seen[i - 1][0]
                    save(e, i - 1).wait()
                    norm_rows(X, e * PART, PART, gain1)
            save(d, i).wait()
            norm_rows(X, d * PART, PART, gain1)
        else:
            kept(2).wait()
            kept(3).wait()
        qkv(l)
        start(back)
        attention(l)
        wait(back)
        wait(load_out(l))
        tick((14, NSEQ - 2)[l])
        group_in(l, 0)
        first = load_group(l, 0, 1)
        start(first)
        out_proj(gain2)
        tick((NF, NSEQ - 1)[l])
        if l == 1:
            for i, d in enumerate(far_pair):
                away[i] = U[span(d * PART + KEEP, SWAP, HD // 4), :].astype(BF16)
                remote(away.at[i], here.at[core], ss.at[0], sr.at[0], d).start()
        norm_block(NB - 1, gain2)

        if l == 0:
            loaded(1)

            @pl.loop(0, NG * NB - NB + 1)
            def _(s):
                g, m = s // NB, s % NB
                for i in EVERY[:-2]:
                    @pl.when(s == 3 * i + 1)
                    def _():
                        tick(16 + i)

                @pl.when(jnp.logical_and(m == 0, g > 0))
                def _():
                    loaded((g + 1) % 2)

                for i in range(2):
                    @pl.when(s == NB * (3 + i) - 2)
                    def _():
                        for k in LATE[3 * i:3 * i + 3]:
                            forward_far('f', k)

                @pl.when(jnp.logical_and(m == NB - 1, g < NG - 1))
                def _():
                    group_in(l, g + 1)
                    start(load_group(l, g + 1, g % 2))
                ffn_step((g + 1) % 2, rows_of(pair_of(m)))
            tick(22)

            @pl.loop(1, NB)
            def _(m):
                @pl.when(m > 2)
                def _():
                    kept(m - 3).wait()
                ffn_step(1, rows_of(pair_of(m)))
                norm_block(m - 1, n1[1:, :], True)
                kept(m - 1).start()
            kept(1).wait()
            norm_block(NB - 1, n1[1:, :], True)
            kept(NB - 1).start()
            all_sent(l)
            continue

        tail = load_group(l, NG - 1, 1)
        far_rows = rows_of(far_pair, KEEP)

        @pl.loop(0, NG - 1)
        def _(s):
            slot = (s + 1) % 2
            loaded(slot)

            @pl.when(s == 2)
            def _():
                for k in LATE[6:-1]:
                    forward_far('f', k)

            @pl.when(s < 3)
            def _():
                group_in(l, s + 1)
                start(load_group(l, s + 1, 1 - slot))

            @pl.when(s == 3)
            def _():
                drained(gf.at[:2, :4 * FR], mate_f.at[LAYERS * NG - 1])
                start(tail[:2])
            ffn_step(slot, far_rows)

        forward_far('f', LATE[-1])
        start(load_group(l, 0, 0))
        drained(gf.at[:2], gs.at[1])
        g = gated(1, far_rows)
        drained(gf.at[0, :4 * FR], mate_f.at[LAYERS * NG])
        tail[2].start()
        tail[2].wait()
        add_down(1, far_rows, g)
        deliver(far_pair, KEEP)
        all_sent(l)

        def last_steps(s, body):
            g, slot = s % NG, (s + 1) % 2
            loaded(slot)

            @pl.when(s < NB * NG - 1)
            def _():
                start(load_group(l, (g + 1) % NG, 1 - slot))
            body(slot)

        @pl.loop(NG, 3 * NG)
        def _(s):
            devs = near_pair(s // NG)
            last_steps(s, lambda slot: ffn_step(slot, rows_of(devs)))

            @pl.when(s % NG == NG - 1)
            def _():
                deliver(devs)

        drained(here, sr.at[0])
        for i in range(2):
            r = pl.ds(i * SWAP, SWAP)
            v = here[i].astype(F32)
            inv = lax.rsqrt(jnp.mean(v * v, axis=-1, keepdims=True) + 1e-6)
            Hx[r, :] = (v * inv * gain2).astype(BF16)
            Ux[r, :] = v
        own_rows = rows_of(pair_of(chip)) + [(Hx, Ux, pl.ds(0, 2 * SWAP))]

        @pl.loop(3 * NG, NB * NG)
        def _(s):
            last_steps(s, lambda slot: ffn_step(slot, own_rows))

    for d in (mate, me):
        r = span(d * PART, PART)
        X[r, :] = U[r, :].astype(BF16)
    Hx[:, :] = Ux[:, :].astype(BF16)
    to_mate = home(mate)
    to_self = local(X.at[pl.ds(me * PART, PART)], out.at[me], vs.at[NDEV])
    swapped = [local(Hx.at[pl.ds(i * SWAP, SWAP)], out.at[d, KEEP:], vs.at[i]) for i, d in enumerate(far_pair)]
    start(swapped)
    start((to_mate, to_self))
    drained(tok.at[:NDEV - 1], ts.at[0])
    drained(away, ss.at[0])
    for sems in (ys, yr):
        drained(out.at[:2, :KEEP], sems.at[0])
        drained(out.at[:NDEV - 3], sems.at[1])
    to_self.wait()
    wait(swapped)


def solution(mesh):
    col_spec = P(None, None, 'tp')
    row_spec = P(None, 'tp', None)

    def local_fn(tokens, pad_mask, rel_table, w_query, w_key, w_value, w_out, w_act, w_lin, w_down, norm_attn, norm_mlp):
        hbm = pl.BlockSpec(memory_space=pltpu.MemorySpace.HBM)
        vmem = pl.BlockSpec(memory_space=pltpu.VMEM)
        sem = pltpu.SemaphoreType.DMA
        shapes = [(NDEV, PART, DM), (LAYERS, NDEV * QROWS, DM), (LAYERS, NDEV * HROWS, DM), (LAYERS * NF, GF, DM), (SEQ, DM)]
        chunks = (O_SEQ * LAYERS, LAYERS, LAYERS * NF)
        return pl.pallas_call(
            mega_kernel,
            in_specs=[hbm, vmem, pl.BlockSpec(memory_space=pltpu.SMEM)] + [hbm] * 7 + [vmem] * 2,
            out_specs=[hbm] * 5,
            out_shape=[jax.ShapeDtypeStruct(s, BF16) for s in shapes],
            scratch_shapes=[
                pltpu.VMEM((SEQ, DM), BF16), pltpu.VMEM((SEQ, DM), F32), pltpu.VMEM((2, SEQ, DM), BF16),
                pltpu.VMEM((NH, 3, KC, KC), F32), pltpu.VMEM((2, GF, DM), BF16), pltpu.VMEM((KC, DM), BF16), pltpu.VMEM((2, SWAP, DM), BF16),
                pltpu.VMEM((2, SWAP, DM), BF16), pltpu.VMEM((2 * SWAP, DM), BF16), pltpu.VMEM((2 * SWAP, DM), F32), pltpu.VMEM((NDEV, NDEV, 4 * KC), F32),
                pltpu.VMEM((NDEV, 4 * KC), F32), pltpu.VMEM((LANES, SEQ), BF16), pltpu.VMEM((NH, NT_K, LANES), F32),
                pltpu.VMEM((2, BQ, LANES), F32), pltpu.VMEM((LAYERS, 3, DM, LANES), BF16),
            ] + [sem((n, 2)) for n in chunks] + [sem((LAYERS,)), sem((LAYERS,)), sem((LAYERS * NF,))] + [
                sem((LAYERS, 4)), sem((LAYERS,)), sem((LAYERS * NG + 1,)), sem((LAYERS,)), sem((LAYERS,)), sem((LAYERS * NG,)),
                sem((1,)), sem((NDEV,))] + [sem((1,))] * 2 + [sem((2,))] * 2 + [sem((1,))] * 2 + [
                sem((2,)), sem((2,)), sem((NDEV + 1,)), sem((LAYERS, 2)), sem((LAYERS, 2))],
            compiler_params=pltpu.CompilerParams(collective_id=0, has_side_effects=True, vmem_limit_bytes=VMEM_BYTES),
        )(tokens, pad_mask, rel_table.T, w_query, w_key, w_value, w_out, jnp.swapaxes(w_act, 1, 2), jnp.swapaxes(w_lin, 1, 2),
          w_down, norm_attn, norm_mlp)[0]

    in_specs = (P('dp', 'tp', None), P('dp', None), P(None, 'tp'), col_spec, col_spec, col_spec, row_spec,
                col_spec, col_spec, row_spec, P(None, None), P(None, None))
    return jax.shard_map(local_fn, mesh=mesh, in_specs=in_specs, out_specs=P('dp', 'tp', None), check_vma=False)
```

```python
import jax
import jax.numpy as jnp
from jax import lax
from jax.experimental import pallas as pl
from jax.experimental.pallas import tpu as pltpu
from jax.sharding import PartitionSpec as P

LOG2E = 1.4426950408889634
MESH = pl.DeviceIdType.MESH
F32, BF16 = jnp.float32, jnp.bfloat16
NT = (((1,), (1,)), ((), ()))

SEQ, DM, NH, NDEV, LAYERS = 2048, 1536, 16, 8, 2
LANES = 128
HD = 64
PART = SEQ // NDEV
KC = 256
NT_K = SEQ // KC
BQ = 512
NB = SEQ // BQ
NSUB = BQ // KC
HROWS = LANES
QROWS = 3 * HROWS
SHARD = 480
FR = 96
NG = SHARD // FR
GF = NDEV * FR
NF = 3 * NG
LEAD = 5
LAG = 5
SWAP = 48
KEEP = PART - SWAP
VMEM_BYTES = 67043328

SEQUENCE = []
for _l in range(LAYERS):
    SEQUENCE += [('q', 3 * _l + i) for i in range(3)] + [('o', _l)] + [('f', NF * _l + i) for i in range(NF)]
NSEQ = len(SEQUENCE)
PER = NSEQ // LAYERS
ROWS = {'q': HROWS, 'o': HROWS, 'f': FR}
EVERY = tuple(range(NDEV))
LATE = tuple(range(9, 15)) + tuple(range(25, 30))
O_SEQ, F_SEQ = 3, 4


def sent_after(s):
    held = {14: 18, 15: 18, 16: 19, 17: 20, 18: 22, 19: 22, 20: 23}
    return held.get(s, min(s + LEAD, NSEQ - 1))


def split3(x):
    a = x.astype(BF16).astype(F32)
    b = (x - a).astype(BF16).astype(F32)
    return a, b, x - a - b


def gelu(x):
    return 0.5 * x * (1.0 + jnp.tanh(0.7978845608028654 * (x + 0.044715 * (x * x * x))))


def span(start, size, unit=LANES):
    return pl.ds(pl.multiple_of(start, unit), size)


def start(cps):
    for c in cps:
        c.start()


def wait(cps):
    for c in cps:
        c.wait()


def mega_kernel(tok, pad, rel, wq, wk, wv, wo, wa, wl, wd, n1, n2,
                out, gq, go, gf, xs,
                X, U, B, W, wb, wo2, away, here, Hx, Ux, F, Fo, ka_ref, qa_ref, mx, rawq,
                near_q, near_o, near_f, far_q, far_o, far_f, mate_q, mate_o, mate_f, sent_q, sent_o, sent_f,
                ts, tr, fts, ftr, ys, yr, ss, sr, ls, gs, vs, ps, rl):
    me = lax.axis_index('tp')
    core, chip = me % 2, me // 2
    cx, cy = chip % 2, chip // 2
    nx = cy * 4 + (1 - cx) * 2 + core
    ny = (1 - cy) * 4 + cx * 2 + core
    nd = (1 - cy) * 4 + (1 - cx) * 2 + core

    def other(d):
        return d + 1 - 2 * (d % 2)

    mate = other(me)

    def remote(src, dst, ss, rs, dev):
        return pltpu.make_async_remote_copy(src_ref=src, dst_ref=dst, send_sem=ss, recv_sem=rs,
                                            device_id={'tp': dev}, device_id_type=MESH)

    local = pltpu.make_async_copy

    def place(kind, k, owner, r0, r):
        if kind == 'q':
            return gq.at[k // 3, pl.ds(owner * QROWS + (k % 3) * HROWS + r0, r)]
        if kind == 'o':
            return go.at[k, pl.ds(owner * HROWS + r0, r)]
        return gf.at[k, pl.ds(owner * FR + r0, r)]

    def drained(ref, sem):
        local(ref, ref, sem).wait()

    def hop(kind, k, slot):
        r = ROWS[kind]
        owner, r0, rr, dev = ((me, 0, r, nx), (me, 0, r, ny), (me, 0, r, mate), (nx, 0, r // 2, ny),
                              (ny, r // 2, r // 2, nx), (nx, 0, r, mate), (ny, 0, r, mate), (nd, 0, r, mate))[slot]
        ref = place(kind, k, owner, r0, rr)
        near, far, via, sent = {'q': (near_q, far_q, mate_q, sent_q), 'o': (near_o, far_o, mate_o, sent_o),
                                'f': (near_f, far_f, mate_f, sent_f)}[kind]
        if slot < 2:
            got = near.at[k, slot]
        elif slot in (3, 4):
            got = far.at[k // 3 if kind == 'q' else k]
        elif kind == 'q':
            got = via.at[k // 3, max(slot - 4, 0)]
        else:
            got = via.at[k // 3 + k // (LAYERS * NF - 1) if kind == 'f' else k]
        return remote(ref, ref, sent.at[k // 3 if kind != 'o' else k], got, dev)

    def send_own(kind, k):
        start(hop(kind, k, slot) for slot in EVERY[:3])

    def forward(kind, k):
        for near in EVERY[:2]:
            hop(kind, k, near).wait_recv()
            start(hop(kind, k, near + step) for step in (3, 5))

    def forward_far(kind, k):
        if kind == 'q':
            drained(gq.at[k // 3, :QROWS], far_q.at[k // 3])
            start(hop(kind, k + i, EVERY[-1]) for i in range(3))
        else:
            drained(place(kind, k, 0, 0, ROWS[kind]), (far_o if kind == 'o' else far_f).at[k])
            hop(kind, k, EVERY[-1]).start()

    def tick(s):
        forward(*SEQUENCE[s])
        if s >= O_SEQ:
            kind, k = SEQUENCE[max(s - LAG, 0)]
            if kind == 'o' or kind == 'f' and k not in LATE:
                forward_far(kind, k)
            for ahead in range(sent_after(s - 1) + 1, sent_after(s) + 1):
                send_own(*SEQUENCE[ahead])

    def tick_f(l, k):
        forward('f', k)

        @pl.when(k % NF == LAG - 1)
        def _():
            forward_far('o', k // NF)

        @pl.when(k % NF >= LAG)
        def _():
            forward_far('f', k - LAG)

        @pl.when(k < NF * (l + 1) - LEAD)
        def _():
            send_own('f', k + LEAD)

    REST = slice(QROWS, BQ + 3 * SHARD)

    def load_raw(l):
        cps = [local(w.at[l], rawq.at[l, i], rl.at[l, 0]) for i, w in enumerate((wq, wk, wv))]
        cps += [local(wo.at[l], B.at[l, QROWS:BQ], rl.at[l, 1])]
        return cps + [local(w.at[l], B.at[l, BQ + SHARD * i:BQ + SHARD * (i + 1)], rl.at[l, 1])
                      for i, w in enumerate((wa, wl, wd))]

    def store_own(l):
        cps = [local(B.at[l, :QROWS], gq.at[l, pl.ds(me * QROWS, QROWS)], ps.at[l, 0]),
               local(B.at[l, QROWS:BQ], go.at[l, pl.ds(me * HROWS, HROWS)], ps.at[l, 1])]
        for m in range(3):
            for g in range(NG):
                r0 = BQ + SHARD * m + FR * g
                cps.append(local(B.at[l, r0:r0 + FR], gf.at[NF * l + 3 * g + m, pl.ds(me * FR, FR)], ps.at[l, 1]))
        return cps

    barrier = pltpu.get_barrier_semaphore()
    for o in EVERY[1:]:
        pl.semaphore_signal(barrier, inc=1, device_id={'tp': (me + o) % NDEV}, device_id_type=MESH)
    stores = [store_own(l) for l in range(LAYERS)]
    for l in range(LAYERS):
        start(load_raw(l))
    pl.semaphore_wait(barrier, NDEV - 1)

    peers = [nd, other(nd), nx, other(nx), ny, other(ny), mate]
    fcp = [remote(Fo, F.at[me], fts.at[0], ftr.at[0], d) for d in peers]
    tcp = [remote(tok.at[d], X.at[pl.ds(me * PART, PART)], ts.at[0], tr.at[i], d) for i, d in enumerate(peers)]
    own_tok = local(tok.at[me], X.at[pl.ds(me * PART, PART)], vs.at[NDEV])
    start((*tcp[2:], own_tok))

    t = lax.broadcasted_iota(jnp.int32, (1, 4 * KC), 1)
    n = jnp.where(t < 3 * KC, t, t - 4 * KC) - KC
    dist = jnp.minimum(jnp.abs(n), 128)
    steps = sum((dist * dist >= 64 * 2 ** i).astype(jnp.int32) for i in range(1, 8))
    bucket = jnp.where(n > 0, 16, 0) + jnp.where(dist < 8, dist, 8 + steps)
    for h in range(2):
        row = jnp.zeros((1, 4 * KC), F32)
        for b in range(32):
            row = jnp.where(bucket == b, rel[h, b] * LOG2E, row)
        Fo[pl.ds(h, 1), :] = row
    Fo[2:, :] = jnp.zeros((NDEV - 2, 4 * KC), F32)

    for l in range(LAYERS):
        drained(rawq.at[l], rl.at[l, 0])
        for i in range(3):
            for cb in range(DM // LANES):
                at = slice(LANES * cb, LANES * (cb + 1))
                B[l, HROWS * i:HROWS * (i + 1), at] = rawq[l, i, at, :].T
        if l == 0:
            start(fcp)
            start(tcp[:2])
            F[me] = Fo[:, :]
        stores[l][0].start()
        if l == 0:
            stores[l][0].wait()
            for k in range(O_SEQ):
                send_own('q', k)
        drained(B.at[l, REST], rl.at[l, 1])
        start(stores[l][1:])

    m3 = split3(jnp.where(pad[pl.ds(me, 1), :] == 1, 0.0, -1e9).astype(F32) * LOG2E)
    rowi = lax.broadcasted_iota(jnp.int32, (HD, 1), 0)
    for c in range(NT_K):
        col = slice(c * KC, (c + 1) * KC)
        v = jnp.where(jnp.logical_and(rowi >= 3 * c, rowi < 3 * c + 3), 1.0, jnp.zeros((HD, KC), F32))
        for p in range(3):
            v = jnp.where(rowi == 3 * NT_K + p, m3[p][:, col], v)
        ka_ref[:, col] = v.astype(BF16)

    drained(F.at[:NDEV - 1], fts.at[0])
    drained(F.at[:NDEV - 1], ftr.at[0])
    lane8 = lax.broadcasted_iota(jnp.int32, (NT_K, LANES), 1) % HD
    qrow8 = lax.broadcasted_iota(jnp.int32, (NT_K, LANES), 0)

    @pl.loop(0, NH)
    def _(h):
        row = F[h // 2, pl.ds(h % 2, 1), :]
        full = pltpu.roll(jnp.broadcast_to(row, (KC, 4 * KC)), 0, 1, stride=1, stride_axis=0)
        for d in range(3):
            W[h, d] = full[:, d * KC:(d + 1) * KC]
        left, right = split3(row[:, :1]), split3(row[:, 2 * KC:2 * KC + 1])
        v = jnp.where(lane8 - 3 * NT_K < 3, 1.0, 0.0)
        for c in range(NT_K):
            for p in range(3):
                far = jnp.where(qrow8 <= c - 2, right[p], jnp.where(qrow8 >= c + 2, left[p], 0.0))
                v = jnp.where(lane8 == 3 * c + p, far, v)
        qa_ref[h] = jnp.where(lane8 < 3 * NT_K + 3, v, 0.0)

    stores[1][0].wait()
    for l in range(LAYERS):
        drained(B.at[l, REST], ps.at[l, 1])

    def norm_rows(src, r0, rows, gain):
        @pl.loop(0, rows // HD)
        def _(i):
            r = span(r0 + i * HD, HD, HD)
            v = src[r, :].astype(F32)
            inv = lax.rsqrt(jnp.mean(v * v, axis=-1, keepdims=True) + 1e-6)
            X[r, :] = (v * inv * gain).astype(BF16)

    def save(d, i):
        r = pl.ds(d * PART, PART)
        return local(X.at[r], xs.at[r], vs.at[i])

    def q_cols(pair):
        return span(pair * LANES, LANES)

    def v_cols(pair):
        return span(1024 * (1 - pair // 4) + LANES * (pair % 4), LANES)

    def k_at(i, key, size, rows=LANES):
        half = SEQ // 2
        return span((key // half) * half + i * rows, rows, rows), span(BQ + key % half, size)

    def qkv_step(p, slot):
        @pl.loop(0, NB)
        def _(m):
            rows = span(m * BQ, BQ)
            res = lax.dot_general(X[rows, :], wb[slot], NT, preferred_element_type=F32)
            for o in range(2):
                pair = 2 * p + o
                q, k, v = (res[:, QROWS * o + LANES * i:QROWS * o + LANES * (i + 1)] for i in range(3))
                B[0, rows, q_cols(pair)] = q.astype(BF16)
                kr, kc = k_at(pair, m * BQ, BQ)
                B[1, kr, kc] = k.T.astype(BF16)
                B[p // 2, rows, v_cols(pair)] = v.astype(BF16)

    def qkv(l):
        def load(i):
            p, slot = 2 * ((cy + i // 2) % 2) + (cx + i % 2) % 2, i % 2
            return p, slot, local(gq.at[l, pl.ds(p * GF, GF)], wb.at[slot], ls.at[slot])

        def fetch(i):
            if i == 1 and l == 0:
                for s in range(O_SEQ):
                    tick(s)
                for s in range(O_SEQ, O_SEQ + LEAD):
                    send_own(*SEQUENCE[s])
            if l == 1:
                tick(PER + O_SEQ + i)
            if i == 3 and l == 0:
                forward_far('q', 0)
            drained(gq.at[l, :QROWS], mate_q.at[l, i])
            load(i)[2].start()

        drained(gq.at[l, :QROWS], mate_q.at[l, 0])
        load(0)[2].start()
        before = ({1: 2}, {0: 1, 1: 2})[l]
        after = ({0: 1, 2: 3}, {2: 3})[l]

        @pl.loop(0, NB)
        def _(i):
            p, slot, cp = load(i)
            cp.wait()
            for at, nxt in before.items():
                @pl.when(i == at)
                def _():
                    fetch(nxt)
            if l == 1:
                @pl.when(i == 2)
                def _():
                    forward_far('q', O_SEQ)
            qkv_step(p, slot)
            for at, nxt in after.items():
                @pl.when(i == at)
                def _():
                    fetch(nxt)
        tick((O_SEQ, PER + F_SEQ + 3)[l])

    lane = lax.broadcasted_iota(jnp.int32, (1, LANES), 1)
    NU = NH * NB
    ones = jnp.ones((KC, LANES), BF16)

    def sblock(slot, t):
        b = slot * NT_K + t
        wide = DM // KC
        return (b // wide) * BQ, (b % wide) * KC

    def parts(u):
        h = u // NB
        return h, u % NB, h // 2, h % 2

    def tile_at(i, t):
        return (i * NSUB - 1 + t + NT_K) % NT_K

    def q_operand(u):
        h, i, pair, odd = parts(u)
        q32 = B[0, span(i * BQ, BQ), q_cols(pair)].astype(F32) * LOG2E
        q32 = jnp.where((lane // HD) == odd, q32, pltpu.roll(q32, HD, 1))
        hi, mid, low = split3(q32)
        qa = jnp.concatenate([jnp.broadcast_to(qa_ref[h, pl.ds(i * NSUB + r, 1), :], (KC, LANES)) for r in range(NSUB)])
        both = jnp.where(lane < HD, hi, low), jnp.where(lane < HD, mid, qa)
        return jnp.concatenate([v.astype(BF16) for v in both], axis=1)

    def score_tile(u, qv, t, slot, m):
        h, i, pair, odd = parts(u)
        c = tile_at(i, t)
        kr, kc = k_at(h, c * KC, KC, HD)
        kh = B[1, kr, kc]
        s = jnp.dot(qv, jnp.concatenate([kh, kh, kh, ka_ref[:, span(c * KC, KC)]]), preferred_element_type=F32)
        r0, c0 = sblock(slot, t)
        ms = []
        for r in range(NSUB):
            sr = s[r * KC:(r + 1) * KC]
            d = t - r
            if 0 <= d < 3:
                w = W[h, d]
                if (d, r) in ((0, 0), (2, NSUB - 1)):
                    at = i * NSUB + r - 1 + d
                    w = jnp.where(jnp.logical_and(at >= 0, at < NT_K), w, 0.0)
                sr = sr + w
            U[r0 + r * KC:r0 + (r + 1) * KC, c0:c0 + KC] = sr
            mm = jnp.maximum(sr[:, :LANES], sr[:, LANES:])
            ms.append(jnp.maximum(m[r], mm) if m else mm)
        return ms

    def value_tile(u, t, slot, mr, acc):
        h, i, pair, odd = parts(u)
        r0, c0 = sblock(slot, t)
        p = jnp.exp2(U[r0:r0 + BQ, c0:c0 + KC] - mr).astype(BF16)
        v = B[pair // 4, span(tile_at(i, t) * KC, KC), v_cols(pair)]
        a = jnp.dot(p, jnp.concatenate([v, ones], axis=1), preferred_element_type=F32)
        return a if t == 0 else acc + a

    def row_max(m, slot):
        for r in range(NSUB):
            mx[slot, r * KC:(r + 1) * KC] = jnp.broadcast_to(jnp.max(m[r], axis=1, keepdims=True), (KC, LANES))

    def context(u, acc):
        h, i, pair, odd = parts(u)
        rows, col = span(i * BQ, BQ), q_cols(pair)
        res = acc[:, :LANES] / acc[:, LANES:]
        B[0, rows, col] = jnp.where((lane // HD) == odd, res, B[0, rows, col].astype(F32)).astype(BF16)

    def unit(u, slot):
        nxt = 1 - slot
        un = jnp.minimum(u + 1, NU - 1)
        acc, m = (), ()
        mr = jnp.concatenate([mx[slot], mx[slot]], axis=1)
        qv = q_operand(un)
        for t in range(NT_K):
            m = score_tile(un, qv, t, nxt, m)
            acc = value_tile(u, t, slot, mr, acc)
        row_max(m, nxt)
        context(u, acc)

    def load_out(l):
        return [local(go.at[l, :GF], wb.at[0], ls.at[0]), local(go.at[l, GF:], wo2, ls.at[1])]

    def attention(l):
        qv, m = q_operand(0), ()
        for t in range(NT_K):
            m = score_tile(0, qv, t, 0, m)
        row_max(m, 0)

        @pl.loop(0, NU // 2)
        def _(j):
            due = jnp.logical_and(j % 3 == 0, j < 30) if l == 0 else j % 7 % 4 == 0

            @pl.when(due)
            def _():
                tick_f(l, j // 3 if l == 0 else NF + F_SEQ + (2 * j + 1) // 7)

            @pl.when(j == 30)
            def _():
                drained(go.at[l, :4 * HROWS], mate_o.at[l])
                start(load_out(l))
            for slot in range(2):
                unit(2 * j + slot, slot)

    def norm_block(m, gain, keep=False):
        for i in range(BQ // HD):
            r = span(m * BQ + i * HD, HD, HD)
            v = U[r, :]
            if keep:
                x = v.astype(BF16)
                B[m % 2, 2 * GF + i * HD:2 * GF + (i + 1) * HD, :] = x
                v = x.astype(F32)
            inv = lax.rsqrt(jnp.mean(v * v, axis=-1, keepdims=True) + 1e-6)
            X[r, :] = (v * inv * gain).astype(BF16)

    def kept(m):
        return local(B.at[m % 2, pl.ds(2 * GF, BQ)], xs.at[pl.ds(m * BQ, BQ)], vs.at[m])

    def out_block(m):
        rows = span(m * BQ, BQ)
        for nb in range(DM // BQ):
            col = slice(nb * BQ, (nb + 1) * BQ)
            y = jnp.dot(B[0, rows, :GF], wb[0, :, col], preferred_element_type=F32)
            y = y + jnp.dot(B[0, rows, GF:1024], wo2[:, col], preferred_element_type=F32)
            U[rows, col] = (X[rows, col].astype(F32) + y).astype(BF16).astype(F32)

    def out_proj(gain):
        out_block(0)

        @pl.loop(1, NB)
        def _(m):
            out_block(m)
            norm_block(m - 1, gain)

    def load_group(l, g, slot):
        k = NF * l + 3 * g
        to = (B.at[slot, :GF], B.at[slot, GF:2 * GF], wb.at[slot])
        return [local(gf.at[k + i], dst, gs.at[slot]) for i, dst in enumerate(to)]

    def loaded(slot):
        drained(gf.at[:3], gs.at[slot])

    def group_in(l, g):
        drained(gf.at[:3, :4 * FR], mate_f.at[NG * l + g])

    def gated(slot, parts):
        hm = jnp.concatenate([h[r, :] for h, _, r in parts])
        a = lax.dot_general(hm, B[slot, :GF, :], NT, preferred_element_type=F32)
        b = lax.dot_general(hm, B[slot, GF:2 * GF, :], NT, preferred_element_type=F32)
        return (gelu(a) * b).astype(BF16)

    def add_down(slot, parts, g):
        y = jnp.dot(g, wb[slot], preferred_element_type=F32)
        at = 0
        for _, total, r in parts:
            total[r, :] += y[at:at + r.size]
            at += r.size

    def ffn_step(slot, parts):
        add_down(slot, parts, gated(slot, parts))

    def rows_of(devs, size=PART):
        return [(X, U, span(d * PART, size)) for d in devs]

    def pair_of(m):
        return 2 * m, 2 * m + 1

    def all_sent(l):
        drained(gq.at[l, :7 * QROWS], sent_q.at[l])
        drained(go.at[l, :7 * HROWS], sent_o.at[l])

        @pl.loop(NG * l, NG * (l + 1))
        def _(g):
            drained(gf.at[:3, :7 * FR], sent_f.at[g])

    far_pair = pair_of(nd // 2)

    def near_pair(mi):
        return [2 * (near // 2) + mi - 1 for near in (nx, ny)]

    def home(d, rows=PART):
        i = rows // PART
        return remote(X.at[pl.ds(d * PART, rows)], out.at[me, :rows], ys.at[i], yr.at[i], d)

    def deliver(devs, rows=PART):
        for d in devs:
            r = span(d * PART, rows)
            X[r, :] = U[r, :].astype(BF16)
        start(home(d, rows) for d in devs)

    seen = [(me, own_tok)] + [(peers[i], tcp[i]) for i in reversed(range(NDEV - 1))]
    back = [local(xs, X, vs.at[NDEV])]
    for l in range(LAYERS):
        gain1, gain2 = n1[pl.ds(l, 1), :], n2[pl.ds(l, 1), :]
        if l == 0:
            for i, (d, c) in enumerate(seen):
                if i == 0:
                    c.wait()
                else:
                    c.wait_recv()
                save(d, i).start()
                if i > 0:
                    e = seen[i - 1][0]
                    save(e, i - 1).wait()
                    norm_rows(X, e * PART, PART, gain1)
            save(d, i).wait()
            norm_rows(X, d * PART, PART, gain1)
        else:
            kept(2).wait()
            kept(3).wait()
        qkv(l)
        start(back)
        attention(l)
        wait(back)
        wait(load_out(l))
        tick((14, NSEQ - 2)[l])
        group_in(l, 0)
        first = load_group(l, 0, 1)
        start(first)
        out_proj(gain2)
        tick((NF, NSEQ - 1)[l])
        if l == 1:
            for i, d in enumerate(far_pair):
                away[i] = U[span(d * PART + KEEP, SWAP, HD // 4), :].astype(BF16)
                remote(away.at[i], here.at[core], ss.at[0], sr.at[0], d).start()
        norm_block(NB - 1, gain2)

        if l == 0:
            loaded(1)

            @pl.loop(0, NG * NB - NB + 1)
            def _(s):
                g, m = s // NB, s % NB
                for i in EVERY[:-2]:
                    @pl.when(s == 3 * i + 1)
                    def _():
                        tick(16 + i)

                @pl.when(jnp.logical_and(m == 0, g > 0))
                def _():
                    loaded((g + 1) % 2)

                for i in range(2):
                    @pl.when(s == NB * (3 + i) - 2)
                    def _():
                        for k in LATE[3 * i:3 * i + 3]:
                            forward_far('f', k)

                @pl.when(jnp.logical_and(m == NB - 1, g < NG - 1))
                def _():
                    group_in(l, g + 1)
                    start(load_group(l, g + 1, g % 2))
                ffn_step((g + 1) % 2, rows_of(pair_of(m)))
            tick(22)

            @pl.loop(1, NB)
            def _(m):
                @pl.when(m > 2)
                def _():
                    kept(m - 3).wait()
                ffn_step(1, rows_of(pair_of(m)))
                norm_block(m - 1, n1[1:, :], True)
                kept(m - 1).start()
            kept(1).wait()
            norm_block(NB - 1, n1[1:, :], True)
            kept(NB - 1).start()
            all_sent(l)
            continue

        tail = load_group(l, NG - 1, 1)
        far_rows = rows_of(far_pair, KEEP)

        @pl.loop(0, NG - 1)
        def _(s):
            slot = (s + 1) % 2
            loaded(slot)

            @pl.when(s == 2)
            def _():
                for k in LATE[6:-1]:
                    forward_far('f', k)

            @pl.when(s < 3)
            def _():
                group_in(l, s + 1)
                start(load_group(l, s + 1, 1 - slot))

            @pl.when(s == 3)
            def _():
                drained(gf.at[:2, :4 * FR], mate_f.at[LAYERS * NG - 1])
                start(tail[:2])
            ffn_step(slot, far_rows)

        forward_far('f', LATE[-1])
        start(load_group(l, 0, 0))
        drained(gf.at[:2], gs.at[1])
        g = gated(1, far_rows)
        drained(gf.at[0, :4 * FR], mate_f.at[LAYERS * NG])
        tail[2].start()
        tail[2].wait()
        add_down(1, far_rows, g)
        deliver(far_pair, KEEP)
        all_sent(l)

        def last_steps(s, body):
            g, slot = s % NG, (s + 1) % 2
            loaded(slot)

            @pl.when(s < NB * NG - 1)
            def _():
                start(load_group(l, (g + 1) % NG, 1 - slot))
            body(slot)

        @pl.loop(NG, 3 * NG)
        def _(s):
            devs = near_pair(s // NG)
            last_steps(s, lambda slot: ffn_step(slot, rows_of(devs)))

            @pl.when(s % NG == NG - 1)
            def _():
                deliver(devs)

        drained(here, sr.at[0])
        for i in range(2):
            r = pl.ds(i * SWAP, SWAP)
            v = here[i].astype(F32)
            inv = lax.rsqrt(jnp.mean(v * v, axis=-1, keepdims=True) + 1e-6)
            Hx[r, :] = (v * inv * gain2).astype(BF16)
            Ux[r, :] = v
        own_rows = rows_of(pair_of(chip)) + [(Hx, Ux, pl.ds(0, 2 * SWAP))]

        @pl.loop(3 * NG, NB * NG)
        def _(s):
            last_steps(s, lambda slot: ffn_step(slot, own_rows))

    for d in (mate, me):
        r = span(d * PART, PART)
        X[r, :] = U[r, :].astype(BF16)
    Hx[:, :] = Ux[:, :].astype(BF16)
    to_mate = home(mate)
    to_self = local(X.at[pl.ds(me * PART, PART)], out.at[me], vs.at[NDEV])
    swapped = [local(Hx.at[pl.ds(i * SWAP, SWAP)], out.at[d, KEEP:], vs.at[i]) for i, d in enumerate(far_pair)]
    start(swapped)
    start((to_mate, to_self))
    drained(tok.at[:NDEV - 1], ts.at[0])
    drained(away, ss.at[0])
    for sems in (ys, yr):
        drained(out.at[:2, :KEEP], sems.at[0])
        drained(out.at[:NDEV - 3], sems.at[1])
    to_self.wait()
    wait(swapped)


def solution(mesh):
    col_spec = P(None, None, 'tp')
    row_spec = P(None, 'tp', None)

    def local_fn(tokens, pad_mask, rel_table, w_query, w_key, w_value, w_out, w_act, w_lin, w_down, norm_attn, norm_mlp):
        hbm = pl.BlockSpec(memory_space=pltpu.MemorySpace.HBM)
        vmem = pl.BlockSpec(memory_space=pltpu.VMEM)
        sem = pltpu.SemaphoreType.DMA
        shapes = [(NDEV, PART, DM), (LAYERS, NDEV * QROWS, DM), (LAYERS, NDEV * HROWS, DM), (LAYERS * NF, GF, DM), (SEQ, DM)]
        chunks = (O_SEQ * LAYERS, LAYERS, LAYERS * NF)
        return pl.pallas_call(
            mega_kernel,
            in_specs=[hbm, vmem, pl.BlockSpec(memory_space=pltpu.SMEM)] + [hbm] * 7 + [vmem] * 2,
            out_specs=[hbm] * 5,
            out_shape=[jax.ShapeDtypeStruct(s, BF16) for s in shapes],
            scratch_shapes=[
                pltpu.VMEM((SEQ, DM), BF16), pltpu.VMEM((SEQ, DM), F32), pltpu.VMEM((2, SEQ, DM), BF16),
                pltpu.VMEM((NH, 3, KC, KC), F32), pltpu.VMEM((2, GF, DM), BF16), pltpu.VMEM((KC, DM), BF16), pltpu.VMEM((2, SWAP, DM), BF16),
                pltpu.VMEM((2, SWAP, DM), BF16), pltpu.VMEM((2 * SWAP, DM), BF16), pltpu.VMEM((2 * SWAP, DM), F32), pltpu.VMEM((NDEV, NDEV, 4 * KC), F32),
                pltpu.VMEM((NDEV, 4 * KC), F32), pltpu.VMEM((HD, SEQ), BF16), pltpu.VMEM((NH, NT_K, LANES), F32),
                pltpu.VMEM((2, BQ, LANES), F32), pltpu.VMEM((LAYERS, 3, DM, LANES), BF16),
            ] + [sem((n, 2)) for n in chunks] + [sem((LAYERS,)), sem((LAYERS,)), sem((LAYERS * NF,))] + [
                sem((LAYERS, 4)), sem((LAYERS,)), sem((LAYERS * NG + 1,)), sem((LAYERS,)), sem((LAYERS,)), sem((LAYERS * NG,)),
                sem((1,)), sem((NDEV,))] + [sem((1,))] * 2 + [sem((2,))] * 2 + [sem((1,))] * 2 + [
                sem((2,)), sem((2,)), sem((NDEV + 1,)), sem((LAYERS, 2)), sem((LAYERS, 2))],
            compiler_params=pltpu.CompilerParams(collective_id=0, has_side_effects=True, vmem_limit_bytes=VMEM_BYTES),
        )(tokens, pad_mask, rel_table.T, w_query, w_key, w_value, w_out, jnp.swapaxes(w_act, 1, 2), jnp.swapaxes(w_lin, 1, 2),
          w_down, norm_attn, norm_mlp)[0]

    in_specs = (P('dp', 'tp', None), P('dp', None), P(None, 'tp'), col_spec, col_spec, col_spec, row_spec,
                col_spec, col_spec, row_spec, P(None, None), P(None, None))
    return jax.shard_map(local_fn, mesh=mesh, in_specs=in_specs, out_specs=P('dp', 'tp', None), check_vma=False)
```

```python
import jax
import jax.numpy as jnp
from jax import lax
from jax.experimental import pallas as pl
from jax.experimental.pallas import tpu as pltpu
from jax.sharding import PartitionSpec as P

LOG2E = 1.4426950408889634
MESH = pl.DeviceIdType.MESH
F32, BF16 = jnp.float32, jnp.bfloat16
NT = (((1,), (1,)), ((), ()))

SEQ, DM, NH, NDEV, LAYERS = 2048, 1536, 16, 8, 2
LANES = 128
HD = 64
PART = SEQ // NDEV
KC = 256
NT_K = SEQ // KC
BQ = 512
NB = SEQ // BQ
NSUB = BQ // KC
HROWS = LANES
QROWS = 3 * HROWS
SHARD = 480
FR = 96
NG = SHARD // FR
GF = NDEV * FR
NF = 3 * NG
POOL = NF - NG
LEAD = 5
LAG = 5
SWAP = 32
KEEP = PART - SWAP
VMEM_BYTES = 67043328

SEQUENCE = []
for _l in range(LAYERS):
    SEQUENCE += [('q', 3 * _l + i) for i in range(3)] + [('o', _l)] + [('f', NF * _l + i) for i in range(NF)]
NSEQ = len(SEQUENCE)
PER = NSEQ // LAYERS
ROWS = {'q': HROWS, 'o': HROWS, 'f': FR}
EVERY = tuple(range(NDEV))
LATE = tuple(range(9, 15)) + tuple(range(25, 30))
O_SEQ, F_SEQ = 3, 4


def sent_after(s):
    held = {14: 18, 15: 18, 16: 19, 17: 20, 18: 22, 19: 22, 20: 23}
    return held.get(s, min(s + LEAD, NSEQ - 1))


def split3(x):
    a = x.astype(BF16).astype(F32)
    b = (x - a).astype(BF16).astype(F32)
    return a, b, x - a - b


def gelu(x):
    return 0.5 * x * (1.0 + jnp.tanh(0.7978845608028654 * (x + 0.044715 * (x * x * x))))


def span(start, size, unit=LANES):
    return pl.ds(pl.multiple_of(start, unit), size)


def start(cps):
    for c in cps:
        c.start()


def wait(cps):
    for c in cps:
        c.wait()


def mega_kernel(tok, pad_in, rel_in, wq, wk, wv, wo, wa, wl, wd, n1_in, n2_in,
                out, gq, go, gf, xs,
                X, U, B, W, wb, wo2, away, here, Hx, Ux, F, Fo, ka_ref, qa_ref, mx, rawq, pad, rel, n1, n2,
                near_q, near_o, near_f, far_q, far_o, far_f, mate_q, mate_o, mate_f, sent_q, sent_o, sent_f,
                ts, tr, fts, ftr, ys, yr, ss, sr, ls, gs, vs, ps, rl):
    me = lax.axis_index('tp')
    core, chip = me % 2, me // 2
    cx, cy = chip % 2, chip // 2
    nx = cy * 4 + (1 - cx) * 2 + core
    ny = (1 - cy) * 4 + cx * 2 + core
    nd = (1 - cy) * 4 + (1 - cx) * 2 + core

    def other(d):
        return d + 1 - 2 * (d % 2)

    mate = other(me)

    def remote(src, dst, ss, rs, dev):
        return pltpu.make_async_remote_copy(src_ref=src, dst_ref=dst, send_sem=ss, recv_sem=rs,
                                            device_id={'tp': dev}, device_id_type=MESH)

    local = pltpu.make_async_copy

    def place(kind, k, owner, r0, r):
        if kind == 'q':
            return gq.at[k // 3, pl.ds(owner * QROWS + (k % 3) * HROWS + r0, r)]
        if kind == 'o':
            return go.at[k, pl.ds(owner * HROWS + r0, r)]
        return gf.at[k, pl.ds(owner * FR + r0, r)]

    def drained(ref, sem):
        local(ref, ref, sem).wait()

    def hop(kind, k, slot):
        r = ROWS[kind]
        owner, r0, rr, dev = ((me, 0, r, nx), (me, 0, r, ny), (me, 0, r, mate), (nx, 0, r // 2, ny),
                              (ny, r // 2, r // 2, nx), (nx, 0, r, mate), (ny, 0, r, mate), (nd, 0, r, mate))[slot]
        ref = place(kind, k, owner, r0, rr)
        near, far, via, sent = {'q': (near_q, far_q, mate_q, sent_q), 'o': (near_o, far_o, mate_o, sent_o),
                                'f': (near_f, far_f, mate_f, sent_f)}[kind]
        if slot < 2:
            got = near.at[k % POOL if kind == 'f' else k, slot]
        elif slot in (3, 4):
            got = far.at[k // 3 if kind == 'q' else k % NF]
        elif kind == 'q':
            got = via.at[k // 3, max(slot - 4, 0)]
        else:
            got = via.at[k // 3 + k // (LAYERS * NF - 1) if kind == 'f' else k]
        return remote(ref, ref, sent.at[k // 3 if kind != 'o' else k], got, dev)

    def send_own(kind, k):
        start(hop(kind, k, slot) for slot in EVERY[:3])

    def forward(kind, k):
        for near in EVERY[:2]:
            hop(kind, k, near).wait_recv()
            start(hop(kind, k, near + step) for step in (3, 5))

    def forward_far(kind, k):
        if kind == 'q':
            drained(gq.at[k // 3, :QROWS], far_q.at[k // 3])
            start(hop(kind, k + i, EVERY[-1]) for i in range(3))
        else:
            drained(place(kind, k, 0, 0, ROWS[kind]), (far_o if kind == 'o' else far_f).at[k % NF])
            hop(kind, k, EVERY[-1]).start()

    def tick(s):
        forward(*SEQUENCE[s])
        if s >= O_SEQ:
            kind, k = SEQUENCE[max(s - LAG, 0)]
            if kind == 'o' or kind == 'f' and k not in LATE:
                forward_far(kind, k)
            for ahead in range(sent_after(s - 1) + 1, sent_after(s) + 1):
                send_own(*SEQUENCE[ahead])

    def tick_f(l, k):
        forward('f', k)

        @pl.when(k % NF == LAG - 1)
        def _():
            forward_far('o', k // NF)

        @pl.when(k % NF >= LAG)
        def _():
            forward_far('f', k - LAG)

        @pl.when(k < NF * (l + 1) - LEAD)
        def _():
            send_own('f', k + LEAD)

    REST = slice(QROWS, BQ + 3 * SHARD)

    def load_raw(l):
        cps = [local(w.at[l], rawq.at[l, i], rl.at[l, 0]) for i, w in enumerate((wq, wk, wv))]
        cps += [local(wo.at[l], B.at[l, QROWS:BQ], rl.at[l, 1])]
        return cps + [local(w.at[l], B.at[l, BQ + SHARD * i:BQ + SHARD * (i + 1)], rl.at[l, 1])
                      for i, w in enumerate((wa, wl, wd))]

    def store_own(l):
        cps = [local(B.at[l, :QROWS], gq.at[l, pl.ds(me * QROWS, QROWS)], ps.at[l, 0]),
               local(B.at[l, QROWS:BQ], go.at[l, pl.ds(me * HROWS, HROWS)], ps.at[l, 1])]
        for m in range(3):
            for g in range(NG):
                r0 = BQ + SHARD * m + FR * g
                cps.append(local(B.at[l, r0:r0 + FR], gf.at[NF * l + 3 * g + m, pl.ds(me * FR, FR)], ps.at[l, 1]))
        return cps

    barrier = pltpu.get_barrier_semaphore()
    for o in EVERY[1:]:
        pl.semaphore_signal(barrier, inc=1, device_id={'tp': (me + o) % NDEV}, device_id_type=MESH)
    small = [local(a, b, vs.at[i]) for i, (a, b) in enumerate(((rel_in, rel), (pad_in, pad), (n1_in, n1), (n2_in, n2)))]
    start(small)
    stores = [store_own(l) for l in range(LAYERS)]
    for l in range(LAYERS):
        start(load_raw(l))
    pl.semaphore_wait(barrier, NDEV - 1)

    peers = [nd, other(nd), nx, other(nx), ny, other(ny), mate]
    fcp = [remote(Fo, F.at[me], fts.at[0], ftr.at[0], d) for d in peers]
    tcp = [remote(tok.at[d], X.at[pl.ds(me * PART, PART)], ts.at[0], tr.at[i], d) for i, d in enumerate(peers)]
    own_tok = local(tok.at[me], X.at[pl.ds(me * PART, PART)], vs.at[NDEV])
    start((*tcp[2:], own_tok))
    wait(small)
    table = rel[:, :] * LOG2E

    t = lax.broadcasted_iota(jnp.int32, (1, 4 * KC), 1)
    n = jnp.where(t < 3 * KC, t, t - 4 * KC) - KC
    dist = jnp.minimum(jnp.abs(n), 128)
    steps = sum((dist * dist >= 64 * 2 ** i).astype(jnp.int32) for i in range(1, 8))
    bucket = jnp.where(n > 0, 16, 0) + jnp.where(dist < 8, dist, 8 + steps)
    for h in range(2):
        row = jnp.zeros((1, 4 * KC), F32)
        for b in range(32):
            row = jnp.where(bucket == b, table[h:h + 1, b:b + 1], row)
        Fo[pl.ds(h, 1), :] = row
    Fo[2:, :] = jnp.zeros((NDEV - 2, 4 * KC), F32)

    for l in range(LAYERS):
        drained(rawq.at[l], rl.at[l, 0])
        for i in range(3):
            for cb in range(DM // LANES):
                at = slice(LANES * cb, LANES * (cb + 1))
                B[l, HROWS * i:HROWS * (i + 1), at] = rawq[l, i, at, :].T
        if l == 0:
            start(fcp)
            start(tcp[:2])
            F[me] = Fo[:, :]
        stores[l][0].start()
        if l == 0:
            stores[l][0].wait()
            for k in range(O_SEQ):
                send_own('q', k)
        drained(B.at[l, REST], rl.at[l, 1])
        start(stores[l][1:])

    m3 = split3(jnp.where(pad[pl.ds(me, 1), :] == 1, 0.0, -1e9).astype(F32) * LOG2E)
    rowi = lax.broadcasted_iota(jnp.int32, (HD, 1), 0)
    for c in range(NT_K):
        col = slice(c * KC, (c + 1) * KC)
        v = jnp.where(jnp.logical_and(rowi >= 3 * c, rowi < 3 * c + 3), 1.0, jnp.zeros((HD, KC), F32))
        for p in range(3):
            v = jnp.where(rowi == 3 * NT_K + p, m3[p][:, col], v)
        ka_ref[:, col] = v.astype(BF16)

    drained(F.at[:NDEV - 1], fts.at[0])
    drained(F.at[:NDEV - 1], ftr.at[0])
    lane8 = lax.broadcasted_iota(jnp.int32, (NT_K, LANES), 1) % HD
    qrow8 = lax.broadcasted_iota(jnp.int32, (NT_K, LANES), 0)

    @pl.loop(0, NH)
    def _(h):
        row = F[h // 2, pl.ds(h % 2, 1), :]
        full = pltpu.roll(jnp.broadcast_to(row, (KC, 4 * KC)), 0, 1, stride=1, stride_axis=0)
        for d in range(3):
            W[h, d] = full[:, d * KC:(d + 1) * KC]
        left, right = split3(row[:, :1]), split3(row[:, 2 * KC:2 * KC + 1])
        v = jnp.where(lane8 - 3 * NT_K < 3, 1.0, 0.0)
        for c in range(NT_K):
            for p in range(3):
                far = jnp.where(qrow8 <= c - 2, right[p], jnp.where(qrow8 >= c + 2, left[p], 0.0))
                v = jnp.where(lane8 == 3 * c + p, far, v)
        qa_ref[h] = jnp.where(lane8 < 3 * NT_K + 3, v, 0.0)

    stores[1][0].wait()
    for l in range(LAYERS):
        drained(B.at[l, REST], ps.at[l, 1])

    def norm_rows(src, r0, rows, gain):
        @pl.loop(0, rows // HD)
        def _(i):
            r = span(r0 + i * HD, HD, HD)
            v = src[r, :].astype(F32)
            inv = lax.rsqrt(jnp.mean(v * v, axis=-1, keepdims=True) + 1e-6)
            X[r, :] = (v * inv * gain).astype(BF16)

    def save(d, i):
        r = pl.ds(d * PART, PART)
        return local(X.at[r], xs.at[r], vs.at[i])

    def q_cols(pair):
        return span(pair * LANES, LANES)

    def v_cols(pair):
        return span(1024 * (1 - pair // 4) + LANES * (pair % 4), LANES)

    def k_at(i, key, size, rows=LANES):
        half = SEQ // 2
        return span((key // half) * half + i * rows, rows, rows), span(BQ + key % half, size)

    def qkv_step(p, slot):
        @pl.loop(0, NB)
        def _(m):
            rows = span(m * BQ, BQ)
            res = lax.dot_general(X[rows, :], wb[slot], NT, preferred_element_type=F32)
            for o in range(2):
                pair = 2 * p + o
                q, k, v = (res[:, QROWS * o + LANES * i:QROWS * o + LANES * (i + 1)] for i in range(3))
                B[0, rows, q_cols(pair)] = q.astype(BF16)
                kr, kc = k_at(pair, m * BQ, BQ)
                B[1, kr, kc] = k.T.astype(BF16)
                B[p // 2, rows, v_cols(pair)] = v.astype(BF16)

    def qkv(l):
        def load(i):
            p, slot = 2 * ((cy + i // 2) % 2) + (cx + i % 2) % 2, i % 2
            return p, slot, local(gq.at[l, pl.ds(p * GF, GF)], wb.at[slot], ls.at[slot])

        def fetch(i):
            if i == 1 and l == 0:
                for s in range(O_SEQ):
                    tick(s)
                for s in range(O_SEQ, O_SEQ + LEAD):
                    send_own(*SEQUENCE[s])
            if l == 1:
                tick(PER + O_SEQ + i)
            if i == 3 and l == 0:
                forward_far('q', 0)
            drained(gq.at[l, :QROWS], mate_q.at[l, i])
            load(i)[2].start()

        drained(gq.at[l, :QROWS], mate_q.at[l, 0])
        load(0)[2].start()
        before = ({1: 2}, {0: 1, 1: 2})[l]
        after = ({0: 1, 2: 3}, {2: 3})[l]

        @pl.loop(0, NB)
        def _(i):
            p, slot, cp = load(i)
            cp.wait()
            for at, nxt in before.items():
                @pl.when(i == at)
                def _():
                    fetch(nxt)
            if l == 1:
                @pl.when(i == 2)
                def _():
                    forward_far('q', O_SEQ)
            qkv_step(p, slot)
            for at, nxt in after.items():
                @pl.when(i == at)
                def _():
                    fetch(nxt)
        tick((O_SEQ, PER + F_SEQ + 3)[l])

    lane = lax.broadcasted_iota(jnp.int32, (1, LANES), 1)
    NU = NH * NB
    ones = jnp.ones((KC, LANES), BF16)

    def sblock(slot, t):
        b = slot * NT_K + t
        wide = DM // KC
        return (b // wide) * BQ, (b % wide) * KC

    def parts(u):
        h = u // NB
        return h, u % NB, h // 2, h % 2

    def tile_at(i, t):
        return (i * NSUB - 1 + t + NT_K) % NT_K

    def q_operand(u):
        h, i, pair, odd = parts(u)
        q32 = B[0, span(i * BQ, BQ), q_cols(pair)].astype(F32) * LOG2E
        q32 = jnp.where((lane // HD) == odd, q32, pltpu.roll(q32, HD, 1))
        hi, mid, low = split3(q32)
        qa = jnp.concatenate([jnp.broadcast_to(qa_ref[h, pl.ds(i * NSUB + r, 1), :], (KC, LANES)) for r in range(NSUB)])
        both = jnp.where(lane < HD, hi, low), jnp.where(lane < HD, mid, qa)
        return jnp.concatenate([v.astype(BF16) for v in both], axis=1)

    def score_tile(u, qv, t, slot, m):
        h, i, pair, odd = parts(u)
        c = tile_at(i, t)
        kr, kc = k_at(h, c * KC, KC, HD)
        kh = B[1, kr, kc]
        s = jnp.dot(qv, jnp.concatenate([kh, kh, kh, ka_ref[:, span(c * KC, KC)]]), preferred_element_type=F32)
        r0, c0 = sblock(slot, t)
        ms = []
        for r in range(NSUB):
            sr = s[r * KC:(r + 1) * KC]
            d = t - r
            if 0 <= d < 3:
                w = W[h, d]
                if (d, r) in ((0, 0), (2, NSUB - 1)):
                    at = i * NSUB + r - 1 + d
                    w = jnp.where(jnp.logical_and(at >= 0, at < NT_K), w, 0.0)
                sr = sr + w
            U[r0 + r * KC:r0 + (r + 1) * KC, c0:c0 + KC] = sr
            mm = jnp.maximum(sr[:, :LANES], sr[:, LANES:])
            ms.append(jnp.maximum(m[r], mm) if m else mm)
        return ms

    def value_tile(u, t, slot, mr, acc):
        h, i, pair, odd = parts(u)
        r0, c0 = sblock(slot, t)
        p = jnp.exp2(U[r0:r0 + BQ, c0:c0 + KC] - mr).astype(BF16)
        v = B[pair // 4, span(tile_at(i, t) * KC, KC), v_cols(pair)]
        a = jnp.dot(p, jnp.concatenate([v, ones], axis=1), preferred_element_type=F32)
        return a if t == 0 else acc + a

    def row_max(m, slot):
        for r in range(NSUB):
            mx[slot, r * KC:(r + 1) * KC] = jnp.broadcast_to(jnp.max(m[r], axis=1, keepdims=True), (KC, LANES))

    def context(u, acc):
        h, i, pair, odd = parts(u)
        rows, col = span(i * BQ, BQ), q_cols(pair)
        res = acc[:, :LANES] / acc[:, LANES:]
        B[0, rows, col] = jnp.where((lane // HD) == odd, res, B[0, rows, col].astype(F32)).astype(BF16)

    def unit(u, slot):
        nxt = 1 - slot
        un = jnp.minimum(u + 1, NU - 1)
        acc, m = (), ()
        mr = jnp.concatenate([mx[slot], mx[slot]], axis=1)
        qv = q_operand(un)
        for t in range(NT_K):
            m = score_tile(un, qv, t, nxt, m)
            acc = value_tile(u, t, slot, mr, acc)
        row_max(m, nxt)
        context(u, acc)

    def load_out(l):
        return [local(go.at[l, :GF], wb.at[0], ls.at[0]), local(go.at[l, GF:], wo2, ls.at[1])]

    def attention(l):
        qv, m = q_operand(0), ()
        for t in range(NT_K):
            m = score_tile(0, qv, t, 0, m)
        row_max(m, 0)

        @pl.loop(0, NU // 2)
        def _(j):
            due = jnp.logical_and(j % 3 == 0, j < 30) if l == 0 else j % 7 % 4 == 0

            @pl.when(due)
            def _():
                tick_f(l, j // 3 if l == 0 else NF + F_SEQ + (2 * j + 1) // 7)

            @pl.when(j == 30)
            def _():
                drained(go.at[l, :4 * HROWS], mate_o.at[l])
                start(load_out(l))
            for slot in range(2):
                unit(2 * j + slot, slot)

    def norm_block(m, gain, keep=False):
        for i in range(BQ // HD):
            r = span(m * BQ + i * HD, HD, HD)
            v = U[r, :]
            if keep:
                x = v.astype(BF16)
                B[m % 2, 2 * GF + i * HD:2 * GF + (i + 1) * HD, :] = x
                v = x.astype(F32)
            inv = lax.rsqrt(jnp.mean(v * v, axis=-1, keepdims=True) + 1e-6)
            X[r, :] = (v * inv * gain).astype(BF16)

    def kept(m):
        return local(B.at[m % 2, pl.ds(2 * GF, BQ)], xs.at[pl.ds(m * BQ, BQ)], vs.at[m])

    def out_block(m):
        rows = span(m * BQ, BQ)
        for nb in range(DM // BQ):
            col = slice(nb * BQ, (nb + 1) * BQ)
            y = jnp.dot(B[0, rows, :GF], wb[0, :, col], preferred_element_type=F32)
            y = y + jnp.dot(B[0, rows, GF:1024], wo2[:, col], preferred_element_type=F32)
            U[rows, col] = (X[rows, col].astype(F32) + y).astype(BF16).astype(F32)

    def out_proj(gain):
        out_block(0)

        @pl.loop(1, NB)
        def _(m):
            out_block(m)
            norm_block(m - 1, gain)

    def load_group(l, g, slot):
        k = NF * l + 3 * g
        to = (B.at[slot, :GF], B.at[slot, GF:2 * GF], wb.at[slot])
        return [local(gf.at[k + i], dst, gs.at[slot]) for i, dst in enumerate(to)]

    def loaded(slot):
        drained(gf.at[:3], gs.at[slot])

    def group_in(l, g):
        drained(gf.at[:3, :4 * FR], mate_f.at[NG * l + g])

    def gated(slot, parts):
        hm = jnp.concatenate([h[r, :] for h, _, r in parts])
        a = lax.dot_general(hm, B[slot, :GF, :], NT, preferred_element_type=F32)
        b = lax.dot_general(hm, B[slot, GF:2 * GF, :], NT, preferred_element_type=F32)
        return (gelu(a) * b).astype(BF16)

    def add_down(slot, parts, g):
        y = jnp.dot(g, wb[slot], preferred_element_type=F32)
        at = 0
        for _, total, r in parts:
            total[r, :] += y[at:at + r.size]
            at += r.size

    def ffn_step(slot, parts):
        add_down(slot, parts, gated(slot, parts))

    def rows_of(devs, size=PART):
        return [(X, U, span(d * PART, size)) for d in devs]

    def pair_of(m):
        return 2 * m, 2 * m + 1

    def all_sent(l):
        drained(gq.at[l, :7 * QROWS], sent_q.at[l])
        drained(go.at[l, :7 * HROWS], sent_o.at[l])

        @pl.loop(NG * l, NG * (l + 1))
        def _(g):
            drained(gf.at[:3, :7 * FR], sent_f.at[g])

    far_pair = pair_of(nd // 2)

    def near_pair(mi):
        return [2 * (near // 2) + mi - 1 for near in (nx, ny)]

    def home(d, rows=PART):
        i = rows // PART
        return remote(X.at[pl.ds(d * PART, rows)], out.at[me, :rows], ys.at[i], yr.at[i], d)

    def deliver(devs, rows=PART):
        for d in devs:
            r = span(d * PART, rows)
            X[r, :] = U[r, :].astype(BF16)
        start(home(d, rows) for d in devs)

    seen = [(me, own_tok)] + [(peers[i], tcp[i]) for i in reversed(range(NDEV - 1))]
    back = [local(xs, X, vs.at[NDEV])]
    for l in range(LAYERS):
        gain1, gain2 = n1[pl.ds(l, 1), :], n2[pl.ds(l, 1), :]
        if l == 0:
            for i, (d, c) in enumerate(seen):
                if i == 0:
                    c.wait()
                else:
                    c.wait_recv()
                save(d, i).start()
                if i > 0:
                    e = seen[i - 1][0]
                    save(e, i - 1).wait()
                    norm_rows(X, e * PART, PART, gain1)
            save(d, i).wait()
            norm_rows(X, d * PART, PART, gain1)
        else:
            kept(2).wait()
            kept(3).wait()
        qkv(l)
        start(back)
        attention(l)
        wait(back)
        wait(load_out(l))
        tick((14, NSEQ - 2)[l])
        group_in(l, 0)
        first = load_group(l, 0, 1)
        start(first)
        out_proj(gain2)
        tick((NF, NSEQ - 1)[l])
        if l == 1:
            for i, d in enumerate(far_pair):
                away[i] = U[span(d * PART + KEEP, SWAP, HD // 4), :].astype(BF16)
                remote(away.at[i], here.at[core], ss.at[0], sr.at[0], d).start()
        norm_block(NB - 1, gain2)

        if l == 0:
            loaded(1)

            @pl.loop(0, NG * NB - NB + 1)
            def _(s):
                g, m = s // NB, s % NB
                for i in EVERY[:-2]:
                    @pl.when(s == 3 * i + 1)
                    def _():
                        tick(16 + i)

                @pl.when(jnp.logical_and(m == 0, g > 0))
                def _():
                    loaded((g + 1) % 2)

                for i in range(2):
                    @pl.when(s == NB * (3 + i) - 2)
                    def _():
                        for k in LATE[3 * i:3 * i + 3]:
                            forward_far('f', k)

                @pl.when(jnp.logical_and(m == NB - 1, g < NG - 1))
                def _():
                    group_in(l, g + 1)
                    start(load_group(l, g + 1, g % 2))
                ffn_step((g + 1) % 2, rows_of(pair_of(m)))
            tick(22)

            @pl.loop(1, NB)
            def _(m):
                @pl.when(m > 2)
                def _():
                    kept(m - 3).wait()
                ffn_step(1, rows_of(pair_of(m)))
                norm_block(m - 1, n1[1:, :], True)
                kept(m - 1).start()
            kept(1).wait()
            norm_block(NB - 1, n1[1:, :], True)
            kept(NB - 1).start()
            all_sent(l)
            continue

        tail = load_group(l, NG - 1, 1)
        far_rows = rows_of(far_pair, KEEP)

        @pl.loop(0, NG - 1)
        def _(s):
            slot = (s + 1) % 2
            loaded(slot)

            @pl.when(s == 2)
            def _():
                for k in LATE[6:-1]:
                    forward_far('f', k)

            @pl.when(s < 3)
            def _():
                group_in(l, s + 1)
                start(load_group(l, s + 1, 1 - slot))

            @pl.when(s == 3)
            def _():
                drained(gf.at[:2, :4 * FR], mate_f.at[LAYERS * NG - 1])
                start(tail[:2])
            ffn_step(slot, far_rows)

        forward_far('f', LATE[-1])
        start(load_group(l, 0, 0))
        drained(gf.at[:2], gs.at[1])
        g = gated(1, far_rows)
        drained(gf.at[0, :4 * FR], mate_f.at[LAYERS * NG])
        tail[2].start()
        tail[2].wait()
        add_down(1, far_rows, g)
        deliver(far_pair, KEEP)
        all_sent(l)

        def last_steps(s, body):
            g, slot = s % NG, (s + 1) % 2
            loaded(slot)

            @pl.when(s < NB * NG - 1)
            def _():
                start(load_group(l, (g + 1) % NG, 1 - slot))
            body(slot)

        @pl.loop(NG, 3 * NG)
        def _(s):
            devs = near_pair(s // NG)
            last_steps(s, lambda slot: ffn_step(slot, rows_of(devs)))

            @pl.when(s % NG == NG - 1)
            def _():
                deliver(devs)

        drained(here, sr.at[0])
        for i in range(2):
            r = pl.ds(i * SWAP, SWAP)
            v = here[i].astype(F32)
            inv = lax.rsqrt(jnp.mean(v * v, axis=-1, keepdims=True) + 1e-6)
            Hx[r, :] = (v * inv * gain2).astype(BF16)
            Ux[r, :] = v
        own_rows = rows_of(pair_of(chip)) + [(Hx, Ux, pl.ds(0, 2 * SWAP))]

        @pl.loop(3 * NG, NB * NG)
        def _(s):
            last_steps(s, lambda slot: ffn_step(slot, own_rows))

    for d in (mate, me):
        r = span(d * PART, PART)
        X[r, :] = U[r, :].astype(BF16)
    Hx[:, :] = Ux[:, :].astype(BF16)
    to_mate = home(mate)
    to_self = local(X.at[pl.ds(me * PART, PART)], out.at[me], vs.at[NDEV])
    swapped = [local(Hx.at[pl.ds(i * SWAP, SWAP)], out.at[d, KEEP:], vs.at[i]) for i, d in enumerate(far_pair)]
    start(swapped)
    start((to_mate, to_self))
    drained(tok.at[:NDEV - 1], ts.at[0])
    drained(away, ss.at[0])
    for sems in (ys, yr):
        drained(out.at[:2, :KEEP], sems.at[0])
        drained(out.at[:NDEV - 3], sems.at[1])
    to_self.wait()
    wait(swapped)


def solution(mesh):
    col_spec = P(None, None, 'tp')
    row_spec = P(None, 'tp', None)

    def local_fn(tokens, pad_mask, rel_table, w_query, w_key, w_value, w_out, w_act, w_lin, w_down, norm_attn, norm_mlp):
        hbm = pl.BlockSpec(memory_space=pltpu.MemorySpace.HBM)
        sem = pltpu.SemaphoreType.DMA
        shapes = [(NDEV, PART, DM), (LAYERS, NDEV * QROWS, DM), (LAYERS, NDEV * HROWS, DM), (LAYERS * NF, GF, DM), (SEQ, DM)]
        chunks = (O_SEQ * LAYERS, LAYERS, POOL)
        return pl.pallas_call(
            mega_kernel,
            in_specs=[hbm] * 12,
            out_specs=[hbm] * 5,
            out_shape=[jax.ShapeDtypeStruct(s, BF16) for s in shapes],
            scratch_shapes=[
                pltpu.VMEM((SEQ, DM), BF16), pltpu.VMEM((SEQ, DM), F32), pltpu.VMEM((2, SEQ, DM), BF16),
                pltpu.VMEM((NH, 3, KC, KC), F32), pltpu.VMEM((2, GF, DM), BF16), pltpu.VMEM((KC, DM), BF16), pltpu.VMEM((2, SWAP, DM), BF16),
                pltpu.VMEM((2, SWAP, DM), BF16), pltpu.VMEM((2 * SWAP, DM), BF16), pltpu.VMEM((2 * SWAP, DM), F32), pltpu.VMEM((NDEV, NDEV, 4 * KC), F32),
                pltpu.VMEM((NDEV, 4 * KC), F32), pltpu.VMEM((HD, SEQ), BF16), pltpu.VMEM((NH, NT_K, LANES), F32),
                pltpu.VMEM((2, BQ, LANES), F32), pltpu.VMEM((LAYERS, 3, DM, LANES), BF16),
                pltpu.VMEM((NDEV, SEQ), jnp.int32), pltpu.VMEM((2, 32), F32), pltpu.VMEM((LAYERS, DM), F32), pltpu.VMEM((LAYERS, DM), F32),
            ] + [sem((n, 2)) for n in chunks] + [sem((LAYERS,)), sem((LAYERS,)), sem((NF,))] + [
                sem((LAYERS, 4)), sem((LAYERS,)), sem((LAYERS * NG + 1,)), sem((LAYERS,)), sem((LAYERS,)), sem((LAYERS * NG,)),
                sem((1,)), sem((NDEV,))] + [sem((1,))] * 2 + [sem((2,))] * 2 + [sem((1,))] * 2 + [
                sem((2,)), sem((2,)), sem((NDEV + 1,)), sem((LAYERS, 2)), sem((LAYERS, 2))],
            compiler_params=pltpu.CompilerParams(collective_id=0, has_side_effects=True, vmem_limit_bytes=VMEM_BYTES),
        )(tokens, pad_mask, rel_table.T, w_query, w_key, w_value, w_out, jnp.swapaxes(w_act, 1, 2), jnp.swapaxes(w_lin, 1, 2),
          w_down, norm_attn, norm_mlp)[0]

    in_specs = (P('dp', 'tp', None), P('dp', None), P(None, 'tp'), col_spec, col_spec, col_spec, row_spec,
                col_spec, col_spec, row_spec, P(None, None), P(None, None))
    return jax.shard_map(local_fn, mesh=mesh, in_specs=in_specs, out_specs=P('dp', 'tp', None), check_vma=False)
```

```python
import jax
import jax.numpy as jnp
from jax import lax
from jax.experimental import pallas as pl
from jax.experimental.pallas import tpu as pltpu
from jax.sharding import PartitionSpec as P

LOG2E = 1.4426950408889634
MESH = pl.DeviceIdType.MESH
F32, BF16 = jnp.float32, jnp.bfloat16
NT = (((1,), (1,)), ((), ()))

SEQ, DM, NH, NDEV, LAYERS = 2048, 1536, 16, 8, 2
LANES = 128
HD = 64
PART = SEQ // NDEV
KC = 256
NT_K = SEQ // KC
BQ = 512
NB = SEQ // BQ
NSUB = BQ // KC
HROWS = LANES
QROWS = 3 * HROWS
SHARD = 480
FR = 96
NG = SHARD // FR
GF = NDEV * FR
NF = 3 * NG
POOL = NF - NG
LEAD = 5
LAG = 5
SWAP = 16
KEEP = PART - SWAP
VMEM_BYTES = 67043328

SEQUENCE = []
for _l in range(LAYERS):
    SEQUENCE += [('q', 3 * _l + i) for i in range(3)] + [('o', _l)] + [('f', NF * _l + i) for i in range(NF)]
NSEQ = len(SEQUENCE)
PER = NSEQ // LAYERS
ROWS = {'q': HROWS, 'o': HROWS, 'f': FR}
EVERY = tuple(range(NDEV))
LATE = tuple(range(9, 15)) + tuple(range(25, 30))
O_SEQ, F_SEQ = 3, 4


def sent_after(s):
    held = {14: 18, 15: 18, 16: 19, 17: 20, 18: 22, 19: 22, 20: 23}
    return held.get(s, min(s + LEAD, NSEQ - 1))


def split3(x):
    a = x.astype(BF16).astype(F32)
    b = (x - a).astype(BF16).astype(F32)
    return a, b, x - a - b


def gelu(x):
    return 0.5 * x * (1.0 + jnp.tanh(0.7978845608028654 * (x + 0.044715 * (x * x * x))))


def span(start, size, unit=LANES):
    return pl.ds(pl.multiple_of(start, unit), size)


def start(cps):
    for c in cps:
        c.start()


def wait(cps):
    for c in cps:
        c.wait()


def mega_kernel(tok, pad_in, rel_in, wq, wk, wv, wo, wa, wl, wd, n1_in, n2_in,
                out, gq, go, gf, xs,
                X, U, B, W, wb, wo2, away, here, Hx, Ux, F, Fo, ka_ref, qa_ref, mx, rawq, pad, rel, n1, n2,
                near_q, near_o, near_f, far_q, far_o, far_f, mate_q, mate_o, mate_f, sent_q, sent_o, sent_f,
                ts, tr, fts, ftr, ys, yr, ss, sr, ls, gs, vs, ps, rl):
    me = lax.axis_index('tp')
    core, chip = me % 2, me // 2
    cx, cy = chip % 2, chip // 2
    nx = cy * 4 + (1 - cx) * 2 + core
    ny = (1 - cy) * 4 + cx * 2 + core
    nd = (1 - cy) * 4 + (1 - cx) * 2 + core

    def other(d):
        return d + 1 - 2 * (d % 2)

    mate = other(me)

    def remote(src, dst, ss, rs, dev):
        return pltpu.make_async_remote_copy(src_ref=src, dst_ref=dst, send_sem=ss, recv_sem=rs,
                                            device_id={'tp': dev}, device_id_type=MESH)

    local = pltpu.make_async_copy

    def place(kind, k, owner, r0, r):
        if kind == 'q':
            return gq.at[k // 3, pl.ds(owner * QROWS + (k % 3) * HROWS + r0, r)]
        if kind == 'o':
            return go.at[k, pl.ds(owner * HROWS + r0, r)]
        return gf.at[k, pl.ds(owner * FR + r0, r)]

    def drained(ref, sem):
        local(ref, ref, sem).wait()

    def hop(kind, k, slot):
        r = ROWS[kind]
        owner, r0, rr, dev = ((me, 0, r, nx), (me, 0, r, ny), (me, 0, r, mate), (nx, 0, r // 2, ny),
                              (ny, r // 2, r // 2, nx), (nx, 0, r, mate), (ny, 0, r, mate), (nd, 0, r, mate))[slot]
        ref = place(kind, k, owner, r0, rr)
        near, far, via, sent = {'q': (near_q, far_q, mate_q, sent_q), 'o': (near_o, far_o, mate_o, sent_o),
                                'f': (near_f, far_f, mate_f, sent_f)}[kind]
        if slot < 2:
            got = near.at[k % POOL if kind == 'f' else k, slot]
        elif slot in (3, 4):
            got = far.at[k // 3 if kind == 'q' else k % NF]
        elif kind == 'q':
            got = via.at[k // 3, max(slot - 4, 0)]
        else:
            got = via.at[k // 3 + k // (LAYERS * NF - 1) if kind == 'f' else k]
        return remote(ref, ref, sent.at[k // 3 if kind != 'o' else k], got, dev)

    def send_own(kind, k):
        start(hop(kind, k, slot) for slot in EVERY[:3])

    def forward(kind, k):
        for near in EVERY[:2]:
            hop(kind, k, near).wait_recv()
            start(hop(kind, k, near + step) for step in (3, 5))

    def forward_far(kind, k):
        if kind == 'q':
            drained(gq.at[k // 3, :QROWS], far_q.at[k // 3])
            start(hop(kind, k + i, EVERY[-1]) for i in range(3))
        else:
            drained(place(kind, k, 0, 0, ROWS[kind]), (far_o if kind == 'o' else far_f).at[k % NF])
            hop(kind, k, EVERY[-1]).start()

    def tick(s):
        forward(*SEQUENCE[s])
        if s >= O_SEQ:
            kind, k = SEQUENCE[max(s - LAG, 0)]
            if kind == 'o' or kind == 'f' and k not in LATE:
                forward_far(kind, k)
            for ahead in range(sent_after(s - 1) + 1, sent_after(s) + 1):
                send_own(*SEQUENCE[ahead])

    def tick_f(l, k):
        forward('f', k)

        @pl.when(k % NF == LAG - 1)
        def _():
            forward_far('o', k // NF)

        @pl.when(k % NF >= LAG)
        def _():
            forward_far('f', k - LAG)

        @pl.when(k < NF * (l + 1) - LEAD)
        def _():
            send_own('f', k + LEAD)

    REST = slice(QROWS, BQ + 3 * SHARD)

    def load_raw(l):
        cps = [local(w.at[l], rawq.at[l, i], rl.at[l, 0]) for i, w in enumerate((wq, wk, wv))]
        cps += [local(wo.at[l], B.at[l, QROWS:BQ], rl.at[l, 1])]
        return cps + [local(w.at[l], B.at[l, BQ + SHARD * i:BQ + SHARD * (i + 1)], rl.at[l, 1])
                      for i, w in enumerate((wa, wl, wd))]

    def store_own(l):
        cps = [local(B.at[l, :QROWS], gq.at[l, pl.ds(me * QROWS, QROWS)], ps.at[l, 0]),
               local(B.at[l, QROWS:BQ], go.at[l, pl.ds(me * HROWS, HROWS)], ps.at[l, 1])]
        for m in range(3):
            for g in range(NG):
                r0 = BQ + SHARD * m + FR * g
                cps.append(local(B.at[l, r0:r0 + FR], gf.at[NF * l + 3 * g + m, pl.ds(me * FR, FR)], ps.at[l, 1]))
        return cps

    barrier = pltpu.get_barrier_semaphore()
    for o in EVERY[1:]:
        pl.semaphore_signal(barrier, inc=1, device_id={'tp': (me + o) % NDEV}, device_id_type=MESH)
    small = [local(a, b, vs.at[i]) for i, (a, b) in enumerate(((rel_in, rel), (pad_in, pad), (n1_in, n1), (n2_in, n2)))]
    start(small)
    stores = [store_own(l) for l in range(LAYERS)]
    for l in range(LAYERS):
        start(load_raw(l))
    pl.semaphore_wait(barrier, NDEV - 1)

    peers = [nd, other(nd), nx, other(nx), ny, other(ny), mate]
    fcp = [remote(Fo, F.at[me], fts.at[0], ftr.at[0], d) for d in peers]
    tcp = [remote(tok.at[d], X.at[pl.ds(me * PART, PART)], ts.at[0], tr.at[i], d) for i, d in enumerate(peers)]
    own_tok = local(tok.at[me], X.at[pl.ds(me * PART, PART)], vs.at[NDEV])
    start((*tcp[2:], own_tok))
    wait(small)
    table = rel[:, :] * LOG2E

    t = lax.broadcasted_iota(jnp.int32, (1, 4 * KC), 1)
    n = jnp.where(t < 3 * KC, t, t - 4 * KC) - KC
    dist = jnp.minimum(jnp.abs(n), 128)
    steps = sum((dist * dist >= 64 * 2 ** i).astype(jnp.int32) for i in range(1, 8))
    bucket = jnp.where(n > 0, 16, 0) + jnp.where(dist < 8, dist, 8 + steps)
    for h in range(2):
        row = jnp.zeros((1, 4 * KC), F32)
        for b in range(32):
            row = jnp.where(bucket == b, table[h:h + 1, b:b + 1], row)
        Fo[pl.ds(h, 1), :] = row
    Fo[2:, :] = jnp.zeros((NDEV - 2, 4 * KC), F32)

    for l in range(LAYERS):
        drained(rawq.at[l], rl.at[l, 0])
        for i in range(3):
            for cb in range(DM // LANES):
                at = slice(LANES * cb, LANES * (cb + 1))
                B[l, HROWS * i:HROWS * (i + 1), at] = rawq[l, i, at, :].T
        if l == 0:
            start(fcp)
            start(tcp[:2])
            F[me] = Fo[:, :]
        stores[l][0].start()
        if l == 0:
            stores[l][0].wait()
            for k in range(O_SEQ):
                send_own('q', k)
        drained(B.at[l, REST], rl.at[l, 1])
        start(stores[l][1:])

    m3 = split3(jnp.where(pad[pl.ds(me, 1), :] == 1, 0.0, -1e9).astype(F32) * LOG2E)
    rowi = lax.broadcasted_iota(jnp.int32, (HD, 1), 0)
    for c in range(NT_K):
        col = slice(c * KC, (c + 1) * KC)
        v = jnp.where(jnp.logical_and(rowi >= 3 * c, rowi < 3 * c + 3), 1.0, jnp.zeros((HD, KC), F32))
        for p in range(3):
            v = jnp.where(rowi == 3 * NT_K + p, m3[p][:, col], v)
        ka_ref[:, col] = v.astype(BF16)

    drained(F.at[:NDEV - 1], fts.at[0])
    drained(F.at[:NDEV - 1], ftr.at[0])
    lane8 = lax.broadcasted_iota(jnp.int32, (NT_K, LANES), 1) % HD
    qrow8 = lax.broadcasted_iota(jnp.int32, (NT_K, LANES), 0)

    @pl.loop(0, NH)
    def _(h):
        row = F[h // 2, pl.ds(h % 2, 1), :]
        full = pltpu.roll(jnp.broadcast_to(row, (KC, 4 * KC)), 0, 1, stride=1, stride_axis=0)
        for d in range(3):
            W[h, d] = full[:, d * KC:(d + 1) * KC]
        left, right = split3(row[:, :1]), split3(row[:, 2 * KC:2 * KC + 1])
        v = jnp.where(lane8 - 3 * NT_K < 3, 1.0, 0.0)
        for c in range(NT_K):
            for p in range(3):
                far = jnp.where(qrow8 <= c - 2, right[p], jnp.where(qrow8 >= c + 2, left[p], 0.0))
                v = jnp.where(lane8 == 3 * c + p, far, v)
        qa_ref[h] = jnp.where(lane8 < 3 * NT_K + 3, v, 0.0)

    stores[1][0].wait()
    for l in range(LAYERS):
        drained(B.at[l, REST], ps.at[l, 1])

    def norm_rows(src, r0, rows, gain):
        @pl.loop(0, rows // HD)
        def _(i):
            r = span(r0 + i * HD, HD, HD)
            v = src[r, :].astype(F32)
            inv = lax.rsqrt(jnp.mean(v * v, axis=-1, keepdims=True) + 1e-6)
            X[r, :] = (v * inv * gain).astype(BF16)

    def save(d, i):
        r = pl.ds(d * PART, PART)
        return local(X.at[r], xs.at[r], vs.at[i])

    def q_cols(pair):
        return span(pair * LANES, LANES)

    def v_cols(pair):
        return span(1024 * (1 - pair // 4) + LANES * (pair % 4), LANES)

    def k_at(i, key, size, rows=LANES):
        half = SEQ // 2
        return span((key // half) * half + i * rows, rows, rows), span(BQ + key % half, size)

    def qkv_step(p, slot):
        @pl.loop(0, NB)
        def _(m):
            rows = span(m * BQ, BQ)
            res = lax.dot_general(X[rows, :], wb[slot], NT, preferred_element_type=F32)
            for o in range(2):
                pair = 2 * p + o
                q, k, v = (res[:, QROWS * o + LANES * i:QROWS * o + LANES * (i + 1)] for i in range(3))
                B[0, rows, q_cols(pair)] = q.astype(BF16)
                kr, kc = k_at(pair, m * BQ, BQ)
                B[1, kr, kc] = k.T.astype(BF16)
                B[p // 2, rows, v_cols(pair)] = v.astype(BF16)

    def qkv(l):
        def load(i):
            p, slot = 2 * ((cy + i // 2) % 2) + (cx + i % 2) % 2, i % 2
            return p, slot, local(gq.at[l, pl.ds(p * GF, GF)], wb.at[slot], ls.at[slot])

        def fetch(i):
            if i == 1 and l == 0:
                for s in range(O_SEQ):
                    tick(s)
                for s in range(O_SEQ, O_SEQ + LEAD):
                    send_own(*SEQUENCE[s])
            if l == 1:
                tick(PER + O_SEQ + i)
            if i == 3 and l == 0:
                forward_far('q', 0)
            drained(gq.at[l, :QROWS], mate_q.at[l, i])
            load(i)[2].start()

        drained(gq.at[l, :QROWS], mate_q.at[l, 0])
        load(0)[2].start()
        before = ({1: 2}, {0: 1, 1: 2})[l]
        after = ({0: 1, 2: 3}, {2: 3})[l]

        @pl.loop(0, NB)
        def _(i):
            p, slot, cp = load(i)
            cp.wait()
            for at, nxt in before.items():
                @pl.when(i == at)
                def _():
                    fetch(nxt)
            if l == 1:
                @pl.when(i == 2)
                def _():
                    forward_far('q', O_SEQ)
            qkv_step(p, slot)
            for at, nxt in after.items():
                @pl.when(i == at)
                def _():
                    fetch(nxt)
        tick((O_SEQ, PER + F_SEQ + 3)[l])

    lane = lax.broadcasted_iota(jnp.int32, (1, LANES), 1)
    NU = NH * NB
    ones = jnp.ones((KC, LANES), BF16)

    def sblock(slot, t):
        b = slot * NT_K + t
        wide = DM // KC
        return (b // wide) * BQ, (b % wide) * KC

    def parts(u):
        h = u // NB
        return h, u % NB, h // 2, h % 2

    def tile_at(i, t):
        return (i * NSUB - 1 + t + NT_K) % NT_K

    def q_operand(u):
        h, i, pair, odd = parts(u)
        q32 = B[0, span(i * BQ, BQ), q_cols(pair)].astype(F32) * LOG2E
        q32 = jnp.where((lane // HD) == odd, q32, pltpu.roll(q32, HD, 1))
        hi, mid, low = split3(q32)
        qa = jnp.concatenate([jnp.broadcast_to(qa_ref[h, pl.ds(i * NSUB + r, 1), :], (KC, LANES)) for r in range(NSUB)])
        both = jnp.where(lane < HD, hi, low), jnp.where(lane < HD, mid, qa)
        return jnp.concatenate([v.astype(BF16) for v in both], axis=1)

    def score_tile(u, qv, t, slot, m):
        h, i, pair, odd = parts(u)
        c = tile_at(i, t)
        kr, kc = k_at(h, c * KC, KC, HD)
        kh = B[1, kr, kc]
        s = jnp.dot(qv, jnp.concatenate([kh, kh, kh, ka_ref[:, span(c * KC, KC)]]), preferred_element_type=F32)
        r0, c0 = sblock(slot, t)
        ms = []
        for r in range(NSUB):
            sr = s[r * KC:(r + 1) * KC]
            d = t - r
            if 0 <= d < 3:
                w = W[h, d]
                if (d, r) in ((0, 0), (2, NSUB - 1)):
                    at = i * NSUB + r - 1 + d
                    w = jnp.where(jnp.logical_and(at >= 0, at < NT_K), w, 0.0)
                sr = sr + w
            U[r0 + r * KC:r0 + (r + 1) * KC, c0:c0 + KC] = sr
            mm = jnp.maximum(sr[:, :LANES], sr[:, LANES:])
            ms.append(jnp.maximum(m[r], mm) if m else mm)
        return ms

    def value_tile(u, t, slot, mr, acc):
        h, i, pair, odd = parts(u)
        r0, c0 = sblock(slot, t)
        p = jnp.exp2(U[r0:r0 + BQ, c0:c0 + KC] - mr).astype(BF16)
        v = B[pair // 4, span(tile_at(i, t) * KC, KC), v_cols(pair)]
        a = jnp.dot(p, jnp.concatenate([v, ones], axis=1), preferred_element_type=F32)
        return a if t == 0 else acc + a

    def row_max(m, slot):
        for r in range(NSUB):
            mx[slot, r * KC:(r + 1) * KC] = jnp.broadcast_to(jnp.max(m[r], axis=1, keepdims=True), (KC, LANES))

    def context(u, acc):
        h, i, pair, odd = parts(u)
        rows, col = span(i * BQ, BQ), q_cols(pair)
        res = acc[:, :LANES] / acc[:, LANES:]
        B[0, rows, col] = jnp.where((lane // HD) == odd, res, B[0, rows, col].astype(F32)).astype(BF16)

    def unit(u, slot):
        nxt = 1 - slot
        un = jnp.minimum(u + 1, NU - 1)
        acc, m = (), ()
        mr = jnp.concatenate([mx[slot], mx[slot]], axis=1)
        qv = q_operand(un)
        for t in range(NT_K):
            m = score_tile(un, qv, t, nxt, m)
            acc = value_tile(u, t, slot, mr, acc)
        row_max(m, nxt)
        context(u, acc)

    def load_out(l):
        return [local(go.at[l, :GF], wb.at[0], ls.at[0]), local(go.at[l, GF:], wo2, ls.at[1])]

    def attention(l):
        qv, m = q_operand(0), ()
        for t in range(NT_K):
            m = score_tile(0, qv, t, 0, m)
        row_max(m, 0)

        @pl.loop(0, NU // 2)
        def _(j):
            due = jnp.logical_and(j % 3 == 0, j < 30) if l == 0 else j % 7 % 4 == 0

            @pl.when(due)
            def _():
                tick_f(l, j // 3 if l == 0 else NF + F_SEQ + (2 * j + 1) // 7)

            @pl.when(j == 30)
            def _():
                drained(go.at[l, :4 * HROWS], mate_o.at[l])
                start(load_out(l))
            for slot in range(2):
                unit(2 * j + slot, slot)

    def norm_block(m, gain, keep=False):
        for i in range(BQ // HD):
            r = span(m * BQ + i * HD, HD, HD)
            v = U[r, :]
            if keep:
                x = v.astype(BF16)
                B[m % 2, 2 * GF + i * HD:2 * GF + (i + 1) * HD, :] = x
                v = x.astype(F32)
            inv = lax.rsqrt(jnp.mean(v * v, axis=-1, keepdims=True) + 1e-6)
            X[r, :] = (v * inv * gain).astype(BF16)

    def kept(m):
        return local(B.at[m % 2, pl.ds(2 * GF, BQ)], xs.at[pl.ds(m * BQ, BQ)], vs.at[m])

    def out_block(m):
        rows = span(m * BQ, BQ)
        for nb in range(DM // BQ):
            col = slice(nb * BQ, (nb + 1) * BQ)
            y = jnp.dot(B[0, rows, :GF], wb[0, :, col], preferred_element_type=F32)
            y = y + jnp.dot(B[0, rows, GF:1024], wo2[:, col], preferred_element_type=F32)
            U[rows, col] = (X[rows, col].astype(F32) + y).astype(BF16).astype(F32)

    def out_proj(gain):
        out_block(0)

        @pl.loop(1, NB)
        def _(m):
            out_block(m)
            norm_block(m - 1, gain)

    def load_group(l, g, slot):
        k = NF * l + 3 * g
        to = (B.at[slot, :GF], B.at[slot, GF:2 * GF], wb.at[slot])
        return [local(gf.at[k + i], dst, gs.at[slot]) for i, dst in enumerate(to)]

    def loaded(slot):
        drained(gf.at[:3], gs.at[slot])

    def group_in(l, g):
        drained(gf.at[:3, :4 * FR], mate_f.at[NG * l + g])

    def gated(slot, parts):
        hm = jnp.concatenate([h[r, :] for h, _, r in parts])
        a = lax.dot_general(hm, B[slot, :GF, :], NT, preferred_element_type=F32)
        b = lax.dot_general(hm, B[slot, GF:2 * GF, :], NT, preferred_element_type=F32)
        return (gelu(a) * b).astype(BF16)

    def add_down(slot, parts, g):
        y = jnp.dot(g, wb[slot], preferred_element_type=F32)
        at = 0
        for _, total, r in parts:
            total[r, :] += y[at:at + r.size]
            at += r.size

    def ffn_step(slot, parts):
        add_down(slot, parts, gated(slot, parts))

    def rows_of(devs, size=PART):
        return [(X, U, span(d * PART, size)) for d in devs]

    def pair_of(m):
        return 2 * m, 2 * m + 1

    def all_sent(l):
        drained(gq.at[l, :7 * QROWS], sent_q.at[l])
        drained(go.at[l, :7 * HROWS], sent_o.at[l])

        @pl.loop(NG * l, NG * (l + 1))
        def _(g):
            drained(gf.at[:3, :7 * FR], sent_f.at[g])

    far_pair = pair_of(nd // 2)

    def near_pair(mi):
        return [2 * (near // 2) + mi - 1 for near in (nx, ny)]

    def home(d, rows=PART):
        i = rows // PART
        return remote(X.at[pl.ds(d * PART, rows)], out.at[me, :rows], ys.at[i], yr.at[i], d)

    def deliver(devs, rows=PART):
        for d in devs:
            r = span(d * PART, rows)
            X[r, :] = U[r, :].astype(BF16)
        start(home(d, rows) for d in devs)

    seen = [(me, own_tok)] + [(peers[i], tcp[i]) for i in reversed(range(NDEV - 1))]
    back = [local(xs, X, vs.at[NDEV])]
    for l in range(LAYERS):
        gain1, gain2 = n1[pl.ds(l, 1), :], n2[pl.ds(l, 1), :]
        if l == 0:
            for i, (d, c) in enumerate(seen):
                if i == 0:
                    c.wait()
                else:
                    c.wait_recv()
                save(d, i).start()
                if i > 0:
                    e = seen[i - 1][0]
                    save(e, i - 1).wait()
                    norm_rows(X, e * PART, PART, gain1)
            save(d, i).wait()
            norm_rows(X, d * PART, PART, gain1)
        else:
            kept(2).wait()
            kept(3).wait()
        qkv(l)
        start(back)
        attention(l)
        wait(back)
        wait(load_out(l))
        tick((14, NSEQ - 2)[l])
        group_in(l, 0)
        first = load_group(l, 0, 1)
        start(first)
        out_proj(gain2)
        tick((NF, NSEQ - 1)[l])
        if l == 1:
            for i, d in enumerate(far_pair):
                away[i] = U[span(d * PART + KEEP, SWAP, HD // 4), :].astype(BF16)
                remote(away.at[i], here.at[core], ss.at[0], sr.at[0], d).start()
        norm_block(NB - 1, gain2)

        if l == 0:
            loaded(1)

            @pl.loop(0, NG * NB - NB + 1)
            def _(s):
                g, m = s // NB, s % NB
                for i in EVERY[:-2]:
                    @pl.when(s == 3 * i + 1)
                    def _():
                        tick(16 + i)

                @pl.when(jnp.logical_and(m == 0, g > 0))
                def _():
                    loaded((g + 1) % 2)

                for i in range(2):
                    @pl.when(s == NB * (3 + i) - 2)
                    def _():
                        for k in LATE[3 * i:3 * i + 3]:
                            forward_far('f', k)

                @pl.when(jnp.logical_and(m == NB - 1, g < NG - 1))
                def _():
                    group_in(l, g + 1)
                    start(load_group(l, g + 1, g % 2))
                ffn_step((g + 1) % 2, rows_of(pair_of(m)))
            tick(22)

            @pl.loop(1, NB)
            def _(m):
                @pl.when(m > 2)
                def _():
                    kept(m - 3).wait()
                ffn_step(1, rows_of(pair_of(m)))
                norm_block(m - 1, n1[1:, :], True)
                kept(m - 1).start()
            kept(1).wait()
            norm_block(NB - 1, n1[1:, :], True)
            kept(NB - 1).start()
            all_sent(l)
            continue

        tail = load_group(l, NG - 1, 1)
        far_rows = rows_of(far_pair, KEEP)

        @pl.loop(0, NG - 1)
        def _(s):
            slot = (s + 1) % 2
            loaded(slot)

            @pl.when(s == 2)
            def _():
                for k in LATE[6:-1]:
                    forward_far('f', k)

            @pl.when(s < 3)
            def _():
                group_in(l, s + 1)
                start(load_group(l, s + 1, 1 - slot))

            @pl.when(s == 3)
            def _():
                drained(gf.at[:2, :4 * FR], mate_f.at[LAYERS * NG - 1])
                start(tail[:2])
            ffn_step(slot, far_rows)

        forward_far('f', LATE[-1])
        start(load_group(l, 0, 0))
        drained(gf.at[:2], gs.at[1])
        g = gated(1, far_rows)
        drained(gf.at[0, :4 * FR], mate_f.at[LAYERS * NG])
        tail[2].start()
        tail[2].wait()
        add_down(1, far_rows, g)
        deliver(far_pair, KEEP)
        all_sent(l)

        def last_steps(s, body):
            g, slot = s % NG, (s + 1) % 2
            loaded(slot)

            @pl.when(s < NB * NG - 1)
            def _():
                start(load_group(l, (g + 1) % NG, 1 - slot))
            body(slot)

        @pl.loop(NG, 3 * NG)
        def _(s):
            devs = near_pair(s // NG)
            last_steps(s, lambda slot: ffn_step(slot, rows_of(devs)))

            @pl.when(s % NG == NG - 1)
            def _():
                deliver(devs)

        drained(here, sr.at[0])
        for i in range(2):
            r = pl.ds(i * SWAP, SWAP)
            v = here[i].astype(F32)
            inv = lax.rsqrt(jnp.mean(v * v, axis=-1, keepdims=True) + 1e-6)
            Hx[r, :] = (v * inv * gain2).astype(BF16)
            Ux[r, :] = v
        own_rows = rows_of(pair_of(chip)) + [(Hx, Ux, pl.ds(0, 2 * SWAP))]

        @pl.loop(3 * NG, NB * NG)
        def _(s):
            last_steps(s, lambda slot: ffn_step(slot, own_rows))

    for d in (mate, me):
        r = span(d * PART, PART)
        X[r, :] = U[r, :].astype(BF16)
    Hx[:, :] = Ux[:, :].astype(BF16)
    to_mate = home(mate)
    to_self = local(X.at[pl.ds(me * PART, PART)], out.at[me], vs.at[NDEV])
    swapped = [local(Hx.at[pl.ds(i * SWAP, SWAP)], out.at[d, KEEP:], vs.at[i]) for i, d in enumerate(far_pair)]
    start(swapped)
    start((to_mate, to_self))
    drained(tok.at[:NDEV - 1], ts.at[0])
    drained(away, ss.at[0])
    for sems in (ys, yr):
        drained(out.at[:2, :KEEP], sems.at[0])
        drained(out.at[:NDEV - 3], sems.at[1])
    to_self.wait()
    wait(swapped)


def solution(mesh):
    col_spec = P(None, None, 'tp')
    row_spec = P(None, 'tp', None)

    def local_fn(tokens, pad_mask, rel_table, w_query, w_key, w_value, w_out, w_act, w_lin, w_down, norm_attn, norm_mlp):
        hbm = pl.BlockSpec(memory_space=pltpu.MemorySpace.HBM)
        sem = pltpu.SemaphoreType.DMA
        shapes = [(NDEV, PART, DM), (LAYERS, NDEV * QROWS, DM), (LAYERS, NDEV * HROWS, DM), (LAYERS * NF, GF, DM), (SEQ, DM)]
        chunks = (O_SEQ * LAYERS, LAYERS, POOL)
        return pl.pallas_call(
            mega_kernel,
            in_specs=[hbm] * 12,
            out_specs=[hbm] * 5,
            out_shape=[jax.ShapeDtypeStruct(s, BF16) for s in shapes],
            scratch_shapes=[
                pltpu.VMEM((SEQ, DM), BF16), pltpu.VMEM((SEQ, DM), F32), pltpu.VMEM((2, SEQ, DM), BF16),
                pltpu.VMEM((NH, 3, KC, KC), F32), pltpu.VMEM((2, GF, DM), BF16), pltpu.VMEM((KC, DM), BF16), pltpu.VMEM((2, SWAP, DM), BF16),
                pltpu.VMEM((2, SWAP, DM), BF16), pltpu.VMEM((2 * SWAP, DM), BF16), pltpu.VMEM((2 * SWAP, DM), F32), pltpu.VMEM((NDEV, NDEV, 4 * KC), F32),
                pltpu.VMEM((NDEV, 4 * KC), F32), pltpu.VMEM((HD, SEQ), BF16), pltpu.VMEM((NH, NT_K, LANES), F32),
                pltpu.VMEM((2, BQ, LANES), F32), pltpu.VMEM((LAYERS, 3, DM, LANES), BF16),
                pltpu.VMEM((NDEV, SEQ), jnp.int32), pltpu.VMEM((2, 32), F32), pltpu.VMEM((LAYERS, DM), F32), pltpu.VMEM((LAYERS, DM), F32),
            ] + [sem((n, 2)) for n in chunks] + [sem((LAYERS,)), sem((LAYERS,)), sem((NF,))] + [
                sem((LAYERS, 4)), sem((LAYERS,)), sem((LAYERS * NG + 1,)), sem((LAYERS,)), sem((LAYERS,)), sem((LAYERS * NG,)),
                sem((1,)), sem((NDEV,))] + [sem((1,))] * 2 + [sem((2,))] * 2 + [sem((1,))] * 2 + [
                sem((2,)), sem((2,)), sem((NDEV + 1,)), sem((LAYERS, 2)), sem((LAYERS, 2))],
            compiler_params=pltpu.CompilerParams(collective_id=0, has_side_effects=True, vmem_limit_bytes=VMEM_BYTES),
        )(tokens, pad_mask, rel_table.T, w_query, w_key, w_value, w_out, jnp.swapaxes(w_act, 1, 2), jnp.swapaxes(w_lin, 1, 2),
          w_down, norm_attn, norm_mlp)[0]

    in_specs = (P('dp', 'tp', None), P('dp', None), P(None, 'tp'), col_spec, col_spec, col_spec, row_spec,
                col_spec, col_spec, row_spec, P(None, None), P(None, None))
    return jax.shard_map(local_fn, mesh=mesh, in_specs=in_specs, out_specs=P('dp', 'tp', None), check_vma=False)
```
